32 devices in a mesh: dp: 8 (over y, x, core), mp: 4 (over z).
Axes of the slice: x: 2, y: 2, z: 4, core: 2. Of those that a mesh axis runs over, the one named last changes fastest.
Arguments:
- hidden: bfloat16 [8192, 2048], P('dp'), may hold values from -6 to 6
- cotangent: bfloat16 [8192, 2048], P('dp'), may hold values from -6 to 6
- lengths: int32 [16], P('dp'), may hold values from 64 to 512, as said below
- input_gain: bfloat16 [2048], P('dp'), may hold values from 0.5 to 1.5
- input_shift: bfloat16 [2048], P('dp'), may hold values from -1.25 to 1.25
- triple_weight: bfloat16 [2048, 3, 2048], P('dp', None, 'mp'), may hold values from -0.125 to 0.125
- triple_bias: bfloat16 [2, 2048], P(None, 'mp'), may hold values from -1.25 to 1.25
- merge_weight: bfloat16 [2048, 2048], P('mp', 'dp'), may hold values from -0.5 to 0.5
- merge_bias: bfloat16 [2048], P('dp'), may hold values from -1.25 to 1.25
- middle_gain: bfloat16 [2048], P('dp'), may hold values from 0.5 to 1.5
- middle_shift: bfloat16 [2048], P('dp'), may hold values from -1.25 to 1.25
- expand_weight: bfloat16 [2048, 8192], P('dp', 'mp'), may hold values from -0.125 to 0.125
- expand_bias: bfloat16 [8192], P('mp'), may hold values from -1.25 to 1.25
- reduce_weight: bfloat16 [8192, 2048], P('mp', 'dp'), may hold values from -0.0625 to 0.0625
- reduce_bias: bfloat16 [2048], P('dp'), may hold values from -1.25 to 1.25
Outputs:
- layer_output: bfloat16 [8192, 2048], P('dp')
- hidden_grad: bfloat16 [8192, 2048], P('dp')
- input_gain_grad: float32 [2048], P('dp')
- input_shift_grad: float32 [2048], P('dp')
- triple_weight_grad: float32 [2048, 3, 2048], P('dp', None, 'mp')
- triple_bias_grad: float32 [2, 2048], P(None, 'mp')
- merge_weight_grad: float32 [2048, 2048], P('mp', 'dp')
- merge_bias_grad: float32 [2048], P('dp')
- middle_gain_grad: float32 [2048], P('dp')
- middle_shift_grad: float32 [2048], P('dp')
- expand_weight_grad: float32 [2048, 8192], P('dp', 'mp')
- expand_bias_grad: float32 [8192], P('mp')
- reduce_weight_grad: float32 [8192, 2048], P('mp', 'dp')
- reduce_bias_grad: float32 [2048], P('dp')
- branch_rms: float32 [3], replicated
The draws below stay inside these ranges and needn't reach their ends.
Inputs may be any that keep to these rules, and one draw needn't show every extreme that they name: `lengths`: each slot's valid tokens stand at its start; in every draw some slot is full (512 valid tokens).
All inputs are finite; a program needn't handle non-finite values.
Results may differ from the reference program's by a relative error of at most 0.023.
Values may be sent and summed in bfloat16 or wider, within the bound.
A program may use at most 256 MiB of HBM per device.

```python
import math
import jax
import jax.numpy as jnp
from jax import lax

D = 2048
HEADS = 32
HEAD_DIM = 64
FF = 8192
SLOT = 512
SEQS = 16
TOKENS = 8192


def draw_lengths(key, part):
    key_one, key_two = jax.random.split(key)
    drawn = jax.random.randint(key_one, (SEQS,), SLOT // 8, SLOT + 1)
    longest = jax.random.randint(key_two, (), 0, SEQS)
    return jnp.where(jnp.arange(SEQS) == longest, SLOT, drawn).astype(jnp.int32)


def level_of(rng, extent, pieces, least, largest):
    gain = 1.0
    for position, parts in pieces:
        draws = jax.random.uniform(jax.random.fold_in(jax.random.fold_in(rng, 6), position), (parts,), jnp.float32, least / len(pieces), largest / len(pieces))
        gain = gain * jnp.repeat(jnp.exp(draws), extent[position] // parts).reshape((-1,) + (1,) * (len(extent) - 1 - position))
    return gain


def normal_values(stream_key, extent, scale, reach, cuts=(), kind=jnp.bfloat16):
    values = scale * jax.random.normal(stream_key, extent, jnp.float32)
    if cuts:
        values = values * level_of(stream_key, extent, cuts, -0.22, 0.18)
    return jnp.clip(values, -reach, reach).astype(kind)


def setup_inputs(seed: int = 0) -> dict:
    seeds = jax.random.split(jax.random.key(seed), 16)
    return {
        "hidden": normal_values(seeds[0], (TOKENS, D), 1.0, 6.0, ((0, 8),)),
        "cotangent": normal_values(seeds[1], (TOKENS, D), 1.0, 6.0, ((0, 8),)),
        "lengths": draw_lengths(jax.random.fold_in(seeds[15], 71), 0),
        "input_gain": jnp.clip(1.0 + 0.1 * jax.random.normal(seeds[3], (D,), jnp.float32), 0.5, 1.5).astype(jnp.bfloat16),
        "input_shift": normal_values(seeds[4], (D,), 0.2, 1.25, ((0, 8),)),
        "triple_weight": normal_values(seeds[5], (D, 3, D), D ** -0.5, 0.125, ((0, 8), (2, 4))),
        "triple_bias": normal_values(seeds[6], (2, D), 0.2, 1.25, ((1, 4),)),
        "merge_weight": normal_values(seeds[7], (D, D), (D // 16) ** -0.5, 0.5, ((0, 4), (1, 8))),
        "merge_bias": normal_values(seeds[8], (D,), 0.2, 1.25, ((0, 8),)),
        "middle_gain": jnp.clip(1.0 + 0.1 * jax.random.normal(seeds[9], (D,), jnp.float32), 0.5, 1.5).astype(jnp.bfloat16),
        "middle_shift": normal_values(seeds[10], (D,), 0.2, 1.25, ((0, 8),)),
        "expand_weight": normal_values(seeds[11], (D, FF), D ** -0.5, 0.125, ((0, 8), (1, 4))),
        "expand_bias": normal_values(seeds[12], (FF,), 0.2, 1.25, ((0, 4),)),
        "reduce_weight": normal_values(seeds[13], (FF, D), FF ** -0.5, 0.0625, ((0, 4), (1, 8))),
        "reduce_bias": normal_values(seeds[14], (D,), 0.2, 1.25, ((0, 8),)),
    }


@jax.custom_vjp
def low(v):
    return lax.optimization_barrier(v.astype(jnp.bfloat16)).astype(jnp.float32)

@jax.custom_vjp
def low_back(v):
    return v

def low_keep(v):
    return (low(v), None)

def low_pass(kept, grad):
    return (grad,)

def back_keep(v):
    return (v, None)

def back_low(kept, grad):
    return (low(grad),)
low.defvjp(low_keep, low_pass)
low_back.defvjp(back_keep, back_low)

def layer_norm(values, gain_vec, shift_vec):
    center = values - lax.optimization_barrier(jnp.mean(values, axis=-1, keepdims=True))
    spread = lax.optimization_barrier(jnp.mean(center * center, axis=-1, keepdims=True))
    return center * lax.rsqrt(spread + 1e-05) * gain_vec + shift_vec

def block_forward(params, seq_block, seq_lengths):
    input_gain, input_shift, triple_weight, triple_bias, merge_weight, merge_bias, middle_gain, middle_shift, expand_weight, expand_bias, reduce_weight, reduce_bias = params
    highest = lax.Precision.HIGHEST
    group = seq_block.shape[0]
    places = jnp.arange(SLOT, dtype=jnp.int32)
    valid_rows = places[None, :] < seq_lengths[:, None]
    norm_in = low(layer_norm(seq_block, input_gain, input_shift))
    triple = jnp.einsum('gtd,dcf->gtcf', norm_in, triple_weight, precision=highest)
    query_vals = low(low_back(triple[:, :, 0] + triple_bias[0]))
    key_vals = low(low_back(triple[:, :, 1]))
    value_vals = low(low_back(triple[:, :, 2] + triple_bias[1]))
    query_vals = query_vals.reshape(group, SLOT, HEADS, HEAD_DIM)
    key_vals = key_vals.reshape(group, SLOT, HEADS, HEAD_DIM)
    value_vals = value_vals.reshape(group, SLOT, HEADS, HEAD_DIM)
    raw_scores = jnp.einsum('gqhe,gkhe->ghqk', query_vals, key_vals, precision=highest)
    slopes = 2.0 ** (-8.0 * (jnp.arange(HEADS, dtype=jnp.int32) + 1).astype(jnp.float32) / HEADS)
    key_place = places.astype(jnp.float32)
    scores = low_back((raw_scores + slopes[None, :, None, None] * key_place[None, None, None, :]) * 0.125)
    allowed = (places[None, :] <= places[:, None])[None, None] & valid_rows[:, None, None, :]
    scores = jnp.where(allowed, scores, -1000000000.0)
    attention_weights = low(jax.nn.softmax(scores, axis=-1))
    mixed_heads = jnp.einsum('ghqk,gkhe->gqhe', attention_weights, value_vals, precision=highest)
    mixed_heads = low(low_back(mixed_heads.reshape(group, SLOT, D)))
    attention_branch = low_back(jnp.einsum('gtd,de->gte', mixed_heads, merge_weight, precision=highest) + merge_bias)
    residual = seq_block + attention_branch
    norm_mid = low(layer_norm(residual, middle_gain, middle_shift))
    expand_pre = low_back(jnp.einsum('gtd,df->gtf', norm_mid, expand_weight, precision=highest) + expand_bias)
    activation = low(jax.nn.gelu(expand_pre, approximate=False))
    feed_branch = low_back(jnp.einsum('gtf,fd->gtd', activation, reduce_weight, precision=highest) + reduce_bias)
    result = residual + feed_branch
    mask_rows = valid_rows[:, :, None]
    layer_rows = jnp.where(mask_rows, result, 0.0)
    square_sums = jnp.stack([jnp.sum(jnp.where(mask_rows, result * result, 0.0)), jnp.sum(jnp.where(mask_rows, attention_branch * attention_branch, 0.0)), jnp.sum(jnp.where(mask_rows, feed_branch * feed_branch, 0.0))])
    return (layer_rows, square_sums)

def reference(hidden, cotangent, lengths, input_gain, input_shift, triple_weight, triple_bias, merge_weight, merge_bias, middle_gain, middle_shift, expand_weight, expand_bias, reduce_weight, reduce_bias):
    params = tuple((weight.astype(jnp.float32) for weight in (input_gain, input_shift, triple_weight, triple_bias, merge_weight, merge_bias, middle_gain, middle_shift, expand_weight, expand_bias, reduce_weight, reduce_bias)))
    hidden_full = hidden.astype(jnp.float32)
    group = math.gcd(SEQS, max(1, 2048 // SLOT))

    def forward(param_set, hidden_rows):
        grouped_rows = hidden_rows.reshape(SEQS // group, group, SLOT, D)
        grouped_lengths = lengths.reshape(SEQS // group, group)

        def step(running, inputs):
            seq_block, seq_lengths = inputs
            layer_rows, square_sums = block_forward(param_set, seq_block, seq_lengths)
            return (running + square_sums, layer_rows)
        square_sums, layer_rows = lax.scan(jax.checkpoint(step), jnp.zeros((3,), jnp.float32), (grouped_rows, grouped_lengths))
        return (layer_rows.reshape(TOKENS, D), square_sums)
    layer_rows, pullback, square_sums = jax.vjp(forward, params, hidden_full, has_aux=True)
    param_grads, hidden_grad = pullback(cotangent.astype(jnp.float32))
    token_count = jnp.sum(lengths).astype(jnp.float32) * D
    root_means = jnp.sqrt(square_sums / token_count)
    return (layer_rows.astype(jnp.bfloat16), hidden_grad.astype(jnp.bfloat16), param_grads[0], param_grads[1], param_grads[2], param_grads[3], param_grads[4], param_grads[5], param_grads[6], param_grads[7], param_grads[8], param_grads[9], param_grads[10], param_grads[11], root_means)
```

```python
import functools

import jax
import jax.numpy as jnp
from jax import lax
from jax.experimental import pallas as pl
from jax.experimental.pallas import tpu as pltpu
from jax.sharding import PartitionSpec as P

HEADS = 32
HEAD_DIM = 64
SLOT = 512
PIECE = 64
TILE = 256
BLOCK = 512
F32 = jnp.float32
BF16 = jnp.bfloat16
MESH = pl.DeviceIdType.MESH
VMEM = pl.BlockSpec(memory_space=pltpu.VMEM)
ANY = pl.BlockSpec(memory_space=pl.ANY)


def dot32(a, b):
    return jnp.dot(a, b, preferred_element_type=F32)


def dot_nt(a, b):
    return lax.dot_general(a, b, (((1,), (1,)), ((), ())), preferred_element_type=F32)


def dot_tn(a, b):
    return lax.dot_general(a, b, (((0,), (0,)), ((), ())), preferred_element_type=F32)


def norm_parts(values):
    center = values - jnp.mean(values, axis=-1, keepdims=True)
    spread = jnp.mean(center * center, axis=-1, keepdims=True)
    rate = lax.rsqrt(spread + 1e-05)
    return center * rate, rate


def norm_back(grad, gain, normed, rate):
    scaled = grad * gain
    first = jnp.mean(scaled, axis=-1, keepdims=True)
    second = jnp.mean(scaled * normed, axis=-1, keepdims=True)
    return rate * (scaled - first - normed * second)


def block(index, size):
    return pl.ds(pl.multiple_of(index * size, size), size)


def greet(count):
    me, group = lax.axis_index("mp"), lax.axis_index("dp")
    barrier = pltpu.get_barrier_semaphore()

    @pl.when(me < count - 1)
    def _():
        pl.semaphore_signal(barrier, inc=1, device_id=(group, me + 1), device_id_type=MESH)

    @pl.when(me > 0)
    def _():
        pl.semaphore_signal(barrier, inc=1, device_id=(group, me - 1), device_id_type=MESH)

    peers = jnp.where(me > 0, 1, 0) + jnp.where(me < count - 1, 1, 0)
    pl.semaphore_wait(barrier, peers)


LAG = 1


class Line:
    def __init__(self, count, part, inbox, extra, sems):
        self.count, self.part, self.inbox, self.extra = count, part, inbox, extra
        self.pieces = part.shape[0] // PIECE
        self.sum_out, self.sum_in, self.extra_in, self.own_out, self.all_out, self.all_in = sems
        self.rows = PIECE // count
        self.me, self.group = lax.axis_index("mp"), lax.axis_index("dp")

    @staticmethod
    def scratch(count, pieces, width):
        rows = PIECE // count
        return [
            pltpu.VMEM((pieces * rows, width), BF16),
            pltpu.SemaphoreType.DMA((pieces, count)),
            pltpu.SemaphoreType.DMA((pieces, count)),
            pltpu.SemaphoreType.DMA((pieces,)),
            pltpu.SemaphoreType.DMA((pieces,)),
            pltpu.SemaphoreType.DMA((pieces, count)),
            pltpu.SemaphoreType.DMA((pieces, count)),
        ]

    def at(self, piece, owner):
        return pl.ds(pl.multiple_of(piece * PIECE + owner * self.rows, self.rows), self.rows)

    def own(self, piece):
        return block(piece, self.rows)

    def copy(self, src, dst, out, into, to):
        return pltpu.make_async_remote_copy(
            src_ref=src,
            dst_ref=dst,
            send_sem=out,
            recv_sem=into,
            device_id=(self.group, to),
            device_id_type=MESH,
        )

    def sum_copy(self, piece, owner, to):
        rows = self.at(piece, owner)
        return self.copy(
            self.part.at[rows],
            self.inbox.at[rows],
            self.sum_out.at[piece, owner],
            self.sum_in.at[piece, owner],
            to,
        )

    def extra_copy(self, piece, owner, to):
        return self.copy(
            self.part.at[self.at(piece, owner)],
            self.extra.at[self.own(piece)],
            self.sum_out.at[piece, owner],
            self.extra_in.at[piece],
            to,
        )

    def all_copy(self, piece, owner, to, own_left=False):
        rows = self.at(piece, owner)
        return self.copy(
            self.inbox.at[rows],
            self.inbox.at[rows],
            self.own_out.at[piece] if own_left else self.all_out.at[piece, owner],
            self.all_in.at[piece, owner],
            to,
        )

    def add(self, piece, owner):
        rows = self.at(piece, owner)
        self.sum_copy(piece, owner, self.me).wait_recv()
        self.part[rows, :] = (
            self.part[rows, :].astype(F32) + self.inbox[rows, :].astype(F32)
        ).astype(BF16)

    def send_right(self, piece):
        me, last = self.me, self.count - 1
        for owner in range(last, 0, -1):

            @pl.when(me < owner)
            def _(owner=owner):
                @pl.when(me > 0)
                def _():
                    self.add(piece, owner)

                self.sum_copy(piece, owner, me + 1).start()

    def send_left(self, piece):
        me, last = self.me, self.count - 1
        for owner in range(last):

            @pl.when(me > owner)
            def _(owner=owner):
                @pl.when(me < last)
                def _():
                    self.add(piece, owner)

                @pl.when(me == owner + 1)
                def _():
                    self.extra_copy(piece, owner, me - 1).start()

                @pl.when(me > owner + 1)
                def _():
                    self.sum_copy(piece, owner, me - 1).start()

    def total(self, piece, acc):
        me, rows = self.me, self.at(piece, self.me)
        acc[...] = self.part[rows, :].astype(F32)

        @pl.when(me > 0)
        def _():
            self.sum_copy(piece, me, me).wait_recv()
            acc[...] = acc[...] + self.inbox[rows, :].astype(F32)

        @pl.when(me < self.count - 1)
        def _():
            self.extra_copy(piece, me, me).wait_recv()
            acc[...] = acc[...] + self.extra[self.own(piece), :].astype(F32)

    def share(self, piece, values):
        me = self.me
        self.inbox[self.at(piece, me), :] = values

        @pl.when(me < self.count - 1)
        def _():
            self.all_copy(piece, me, me + 1).start()

        @pl.when(me > 0)
        def _():
            self.all_copy(piece, me, me - 1, own_left=True).start()

    def forward(self, piece, away):
        me, last = self.me, self.count - 1

        @pl.when(me >= away)
        def _(owner=me - away):
            self.all_copy(piece, owner, me).wait_recv()

            @pl.when(me < last)
            def _():
                self.all_copy(piece, owner, me + 1).start()

        @pl.when(me + away <= last)
        def _(owner=me + away):
            self.all_copy(piece, owner, me).wait_recv()

            @pl.when(me > 0)
            def _():
                self.all_copy(piece, owner, me - 1).start()

    def settle(self, piece):
        me, last = self.me, self.count - 1
        for owner in range(self.count):

            @pl.when(me != owner)
            def _():
                self.sum_copy(piece, owner, me).wait_send()

            @pl.when(jnp.logical_or(jnp.logical_and(me >= owner, me < last), jnp.logical_and(me < owner, me > 0)))
            def _():
                self.all_copy(piece, owner, me).wait_send()

        @pl.when(me > 0)
        def _():
            self.all_copy(piece, me, me, own_left=True).wait_send()


def tick(line, step, finish):
    def when(piece, work, *more):
        @pl.when(jnp.logical_and(piece >= 0, piece < line.pieces))
        def _():
            work(piece, *more)

    last = line.count - 1
    when(step - LAG * line.me, line.send_right)
    when(step - LAG * (last - line.me), line.send_left)
    when(step - LAG * last, finish)
    for away in range(1, line.count):
        when(step - LAG * (last + away), line.forward, away)


def ticks(count, pieces):
    return pieces + 2 * LAG * (count - 1)


def params(index):
    return pltpu.CompilerParams(
        collective_id=index, has_side_effects=True, vmem_limit_bytes=63 << 20
    )


def merge_kernel(count, pieces, mixed, merge, own, valid, vectors, middle, residual, sums, part, acc, *rest):
    line = Line(count, part, middle, rest[0], rest[1:])
    greet(count)
    sums[...] = jnp.zeros_like(sums)

    def finish(piece):
        line.total(piece, acc)
        rows = line.own(piece)
        branch = acc[...] + vectors[2:3, :]
        result = own[rows, :].astype(F32) + branch
        residual[rows, :] = result
        normed, _ = norm_parts(result)
        line.share(piece, (normed * vectors[3:4, :] + vectors[4:5, :]).astype(BF16))
        sums[0:1, :] += jnp.sum(branch * branch * valid[rows, :], axis=0, keepdims=True)

    ratio = TILE // PIECE

    @pl.loop(0, ticks(count, pieces))
    def _(step):
        @pl.when(jnp.logical_and(step < pieces, lax.rem(step, ratio) == 0))
        def _():
            rows = block(step // ratio, TILE)

            @pl.loop(0, part.shape[1] // BLOCK)
            def _(k):
                cols = block(k, BLOCK)
                part[rows, cols] = dot32(mixed[rows, :], merge[:, cols]).astype(BF16)

        tick(line, step, finish)

    @pl.loop(0, pieces)
    def _(piece):
        line.settle(piece)


def merge_call(count, mixed, merge, own, valid, vectors):
    rows, width = mixed.shape[0], merge.shape[1]
    pieces = rows // PIECE
    return pl.pallas_call(
        functools.partial(merge_kernel, count, pieces),
        name="merge_line",
        out_shape=(
            jax.ShapeDtypeStruct((rows, width), BF16),
            jax.ShapeDtypeStruct((rows // count, width), F32),
            jax.ShapeDtypeStruct((8, width), F32),
        ),
        in_specs=[VMEM] * 5,
        out_specs=(VMEM,) * 3,
        scratch_shapes=[
            pltpu.VMEM((rows, width), BF16),
            pltpu.VMEM((PIECE // count, width), F32),
            *Line.scratch(count, pieces, width),
        ],
        compiler_params=params(1),
    )(mixed, merge, own, valid, vectors)


def feed_kernel(
    count, pieces, middle_hbm, expand_hbm, reduce_hbm, grad_hbm, residual, own_grad, unit_shift, vectors,
    branch_grad, residual_grad, sums, unit_grad, feed_hbm, expand_grad, reduce_grad,
    middle, expand, reduce, grad, active, pre_grad, part, acc, stage, load_sem, stage_sem, *rest,
):
    line = Line(count, part, branch_grad, rest[0], rest[1:])
    units = expand.shape[1]
    width = expand.shape[0]
    blocks = units // BLOCK

    def load(k):
        cols = block(k, BLOCK)
        return (
            pltpu.make_async_copy(expand_hbm.at[:, cols], expand.at[:, cols], load_sem.at[0, k]),
            pltpu.make_async_copy(reduce_hbm.at[cols], reduce.at[cols], load_sem.at[1, k]),
        )

    def load_rows(k):
        rows = block(k, TILE)
        return (
            pltpu.make_async_copy(middle_hbm.at[rows], middle.at[rows], load_sem.at[2, k]),
            pltpu.make_async_copy(grad_hbm.at[rows], grad.at[rows], load_sem.at[3, k]),
        )

    tiles = middle.shape[0] // TILE
    for copy in (*load_rows(0), *load(0)):
        copy.start()
    for k in range(1, blocks):
        for copy in load(k):
            copy.start()
    for k in range(1, tiles):
        for copy in load_rows(k):
            copy.start()
    greet(count)
    sums[...] = jnp.zeros_like(sums)
    unit_grad[...] = jnp.zeros_like(unit_grad)

    def finish(piece):
        line.total(piece, acc)
        rows = line.own(piece)
        grad_mid = acc[...]
        normed, rate = norm_parts(residual[rows, :])
        grad_out = own_grad[rows, :].astype(F32)
        result = grad_out + norm_back(grad_mid, vectors[3:4, :], normed, rate)
        residual_grad[rows, :] = result
        low = result.astype(BF16)
        line.share(piece, low)
        for k, values in enumerate((low.astype(F32), grad_mid * normed, grad_mid, grad_out)):
            sums[k : k + 1, :] += jnp.sum(values, axis=0, keepdims=True)

    def load_tile(tile):
        for copy in load_rows(tile):
            copy.wait()

    def forward_tile(tile, k):
        rows, cols = block(tile, TILE), block(k, BLOCK)

        @pl.when(tile == 0)
        def _():
            for copy in load(k):
                copy.wait()

        pre = dot32(middle[rows, :], expand[:, cols]) + unit_shift[:, cols]
        half = 0.5 + 0.5 * lax.erf(pre * 0.7071067811865476)
        slope = half + pre * (0.3989422804014327 * jnp.exp(-0.5 * pre * pre))
        active[rows, cols] = (pre * half).astype(BF16)
        low = (dot_nt(grad[rows, :], reduce[cols, :]) * slope).astype(BF16)
        pre_grad[rows, cols] = low
        unit_grad[:, cols] += jnp.sum(low.astype(F32), axis=0, keepdims=True)

    def back_tile(tile, k):
        rows, cols = block(tile, TILE), block(k, BLOCK)
        part[rows, cols] = dot_nt(pre_grad[rows, :], expand[cols, :]).astype(BF16)

    def put(slot, target):
        return pltpu.make_async_copy(stage.at[slot], target, stage_sem.at[slot])

    rows_all = middle.shape[0] // BLOCK
    per_feed = rows_all * (width // BLOCK)
    per_grad = (units // BLOCK) * (width // BLOCK)
    jobs = per_feed + 2 * per_grad

    def job(index):
        slot = lax.rem(index, 2)
        across = width // BLOCK

        @pl.when(index >= 2)
        def _():
            put(slot, expand_grad.at[pl.ds(0, BLOCK), pl.ds(0, BLOCK)]).wait()

        @pl.when(index < per_grad)
        def _():
            r, c = block(index // across, BLOCK), block(lax.rem(index, across), BLOCK)
            stage[slot] = dot_tn(active[:, r], grad[:, c]).astype(BF16)
            put(slot, reduce_grad.at[r, c]).start()

        @pl.when(jnp.logical_and(index >= per_grad, index < 2 * per_grad))
        def _():
            local = index - per_grad
            r, c = block(local // across, BLOCK), block(lax.rem(local, across), BLOCK)
            stage[slot] = dot_tn(middle[:, r], pre_grad[:, c]).astype(BF16)
            put(slot, expand_grad.at[r, c]).start()

        @pl.when(index >= 2 * per_grad)
        def _():
            local = index - 2 * per_grad
            r, c = block(local // across, BLOCK), block(lax.rem(local, across), BLOCK)
            stage[slot] = dot32(active[r, :], reduce[:, c]).astype(BF16)
            put(slot, feed_hbm.at[r, c]).start()

    ratio = TILE // PIECE
    backs = width // BLOCK
    load_tile(0)
    pl.loop(0, blocks)(functools.partial(forward_tile, 0))
    pl.loop(0, backs)(functools.partial(back_tile, 0))
    steps = ticks(count, pieces)
    late = (tiles - 1) * ratio
    per_step = -(-jobs // (steps - late))

    @pl.loop(0, steps)
    def _(step):
        tick(line, step, finish)
        tile, phase = step // ratio + 1, lax.rem(step, ratio)

        @pl.when(tile < tiles)
        def _():
            @pl.when(phase == 0)
            def _():
                load_tile(tile)

            @pl.loop(phase * (blocks + backs) // ratio, (phase + 1) * (blocks + backs) // ratio)
            def _(k):
                @pl.when(k < blocks)
                def _():
                    forward_tile(tile, k)

                @pl.when(k >= blocks)
                def _():
                    back_tile(tile, k - blocks)

        @pl.when(tile >= tiles)
        def _():
            first = (step - late) * per_step

            @pl.loop(first, jnp.minimum(first + per_step, jobs))
            def _(index):
                job(index)

    for slot in range(2):
        put(slot, expand_grad.at[pl.ds(0, BLOCK), pl.ds(0, BLOCK)]).wait()

    @pl.loop(0, pieces)
    def _(piece):
        line.settle(piece)


def feed_call(count, middle, expand, reduce, grad, residual, own_grad, unit_shift, vectors):
    rows, width = middle.shape
    units = expand.shape[1]
    pieces = rows // PIECE
    most = max(units // BLOCK, rows // TILE)
    return pl.pallas_call(
        functools.partial(feed_kernel, count, pieces),
        name="feed_line",
        out_shape=(
            jax.ShapeDtypeStruct((rows, width), BF16),
            jax.ShapeDtypeStruct((rows // count, width), F32),
            jax.ShapeDtypeStruct((8, width), F32),
            jax.ShapeDtypeStruct((1, units), F32),
            jax.ShapeDtypeStruct((rows, width), BF16),
            jax.ShapeDtypeStruct((width, units), BF16),
            jax.ShapeDtypeStruct((units, width), BF16),
        ),
        in_specs=[ANY] * 4 + [VMEM] * 4,
        out_specs=(VMEM,) * 4 + (ANY,) * 3,
        scratch_shapes=[
            pltpu.VMEM((rows, width), BF16),
            pltpu.VMEM((width, units), BF16),
            pltpu.VMEM((units, width), BF16),
            pltpu.VMEM((rows, width), BF16),
            pltpu.VMEM((rows, units), BF16),
            pltpu.VMEM((rows, units), BF16),
            pltpu.VMEM((rows, width), BF16),
            pltpu.VMEM((PIECE // count, width), F32),
            pltpu.VMEM((2, BLOCK, BLOCK), BF16),
            pltpu.SemaphoreType.DMA((4, most)),
            pltpu.SemaphoreType.DMA((2,)),
            *Line.scratch(count, pieces, width),
        ],
        compiler_params=params(2),
    )(middle, expand, reduce, grad, residual, own_grad, unit_shift, vectors)


def last_kernel(
    count, pieces, triple_grad, triple, feed, own, residual, residual_grad, valid, vectors,
    hidden_grad, output, sums, part, acc, *rest,
):
    half = len(rest) // 2
    line = Line(count, part, hidden_grad, rest[0], rest[1:half])
    feed_line = Line(count, feed, output, rest[half], rest[half + 1 :])
    greet(count)
    sums[...] = jnp.zeros_like(sums)

    def finish(piece):
        line.total(piece, acc)
        rows = line.own(piece)
        grad_in = acc[...]
        normed, rate = norm_parts(own[rows, :].astype(F32))
        result = residual_grad[rows, :] + norm_back(grad_in, vectors[0:1, :], normed, rate)
        line.share(piece, result.astype(BF16))
        sums[0:1, :] += jnp.sum(grad_in * normed, axis=0, keepdims=True)
        sums[1:2, :] += jnp.sum(grad_in, axis=0, keepdims=True)

    def finish_feed(piece):
        feed_line.total(piece, acc)
        rows = feed_line.own(piece)
        branch = acc[...] + vectors[5:6, :]
        keep = valid[rows, :] > 0.5
        result = jnp.where(keep, residual[rows, :] + branch, 0.0)
        feed_line.share(piece, result.astype(BF16))
        branch = jnp.where(keep, branch, 0.0)
        sums[2:3, :] += jnp.sum(result * result, axis=0, keepdims=True)
        sums[3:4, :] += jnp.sum(branch * branch, axis=0, keepdims=True)

    ratio = TILE // PIECE

    @pl.loop(0, ticks(count, pieces))
    def _(step):
        tick(feed_line, step, finish_feed)

        @pl.when(jnp.logical_and(step < pieces, lax.rem(step, ratio) == 0))
        def _():
            rows = block(step // ratio, TILE)

            @pl.loop(0, part.shape[1] // BLOCK)
            def _(k):
                cols = block(k, BLOCK)
                part[rows, cols] = dot_nt(triple_grad[rows, :], triple[cols, :]).astype(BF16)

        tick(line, step, finish)

    @pl.loop(0, pieces)
    def _(piece):
        line.settle(piece)
        feed_line.settle(piece)


def last_call(count, triple_grad, triple, feed, own, residual, residual_grad, valid, vectors):
    rows, width = feed.shape
    pieces = rows // PIECE
    return pl.pallas_call(
        functools.partial(last_kernel, count, pieces),
        name="last_line",
        out_shape=(
            jax.ShapeDtypeStruct((rows, width), BF16),
            jax.ShapeDtypeStruct((rows, width), BF16),
            jax.ShapeDtypeStruct((8, width), F32),
        ),
        in_specs=[VMEM] * 8,
        out_specs=(VMEM,) * 3,
        scratch_shapes=[
            pltpu.VMEM((rows, width), BF16),
            pltpu.VMEM((PIECE // count, width), F32),
            *Line.scratch(count, pieces, width),
            *Line.scratch(count, pieces, width),
        ],
        compiler_params=params(3),
    )(triple_grad, triple, feed, own, residual, residual_grad, valid, vectors)


def small_kernel(groups, count, over_all, over_dp, all_out, dp_out, all_in, dp_in, own_sum, mp_in, sems, mp_sems):
    me, group = lax.axis_index("mp"), lax.axis_index("dp")
    barrier = pltpu.get_barrier_semaphore()

    @pl.loop(1, groups)
    def _(away):
        to = lax.rem(group + away, groups)
        pl.semaphore_signal(barrier, inc=1, device_id=(to, me), device_id_type=MESH)

    @pl.loop(1, count)
    def _(away):
        to = lax.rem(me + away, count)
        pl.semaphore_signal(barrier, inc=1, device_id=(group, to), device_id_type=MESH)

    pl.semaphore_wait(barrier, groups + count - 2)

    def pair(away):
        to = lax.rem(group + away, groups)
        return [
            pltpu.make_async_remote_copy(
                src_ref=src,
                dst_ref=dst,
                send_sem=sems.at[k, away],
                recv_sem=sems.at[k + 2, away],
                device_id=(to, me),
                device_id_type=MESH,
            )
            for k, (src, dst) in enumerate(
                ((over_all.at[to], all_in.at[away]), (over_dp, dp_in.at[away]))
            )
        ]

    def across(away):
        return pltpu.make_async_remote_copy(
            src_ref=own_sum,
            dst_ref=mp_in.at[away],
            send_sem=mp_sems.at[0, away],
            recv_sem=mp_sems.at[1, away],
            device_id=(group, lax.rem(me + away, count)),
            device_id_type=MESH,
        )

    @pl.loop(1, groups)
    def _(away):
        for copy in pair(away):
            copy.start()

    own_sum[...] = over_all[group]
    dp_out[...] = over_dp[...]

    @pl.loop(1, groups)
    def _(away):
        for copy in pair(away):
            copy.wait_recv()
        own_sum[...] = own_sum[...] + all_in[away]
        dp_out[...] = dp_out[...] + dp_in[away]

    @pl.loop(1, count)
    def _(away):
        across(away).start()

    all_out[...] = own_sum[...]

    @pl.loop(1, count)
    def _(away):
        across(away).wait_recv()
        all_out[...] = all_out[...] + mp_in[away]

    @pl.loop(1, groups)
    def _(away):
        for copy in pair(away):
            copy.wait_send()

    @pl.loop(1, count)
    def _(away):
        across(away).wait_send()


def small_call(groups, count, over_all, over_dp):
    return pl.pallas_call(
        functools.partial(small_kernel, groups, count),
        name="small_sums",
        out_shape=(
            jax.ShapeDtypeStruct(over_all.shape[1:], F32),
            jax.ShapeDtypeStruct(over_dp.shape, F32),
        ),
        in_specs=[VMEM] * 2,
        out_specs=(VMEM,) * 2,
        scratch_shapes=[
            pltpu.VMEM(over_all.shape, F32),
            pltpu.VMEM((groups, *over_dp.shape), F32),
            pltpu.VMEM(over_all.shape[1:], F32),
            pltpu.VMEM((count, *over_all.shape[1:]), F32),
            pltpu.SemaphoreType.DMA((4, groups)),
            pltpu.SemaphoreType.DMA((2, count)),
        ],
        compiler_params=params(4),
    )(over_all, over_dp)


def attention_scores(query_low, key_low, slopes, length):
    raw_scores = jnp.einsum("qhe,khe->hqk", query_low, key_low, preferred_element_type=F32)
    places = jnp.arange(query_low.shape[0], dtype=jnp.int32)
    key_place = places.astype(F32)
    scores = (raw_scores + slopes[:, None, None] * key_place[None, None, :]) * 0.125
    allowed = (places[None, :] <= places[:, None]) & (places[None, :] < length)
    return jnp.where(allowed[None], scores, -1000000000.0)


def make_local(groups, count):
    def local(
        hidden,
        cotangent,
        lengths,
        input_gain,
        input_shift,
        triple_weight,
        triple_bias,
        merge_weight,
        merge_bias,
        middle_gain,
        middle_shift,
        expand_weight,
        expand_bias,
        reduce_weight,
        reduce_bias,
    ):
        slot = SLOT
        rows, width = hidden.shape
        head_cols = triple_weight.shape[2]
        units = expand_weight.shape[1]
        local_heads = head_cols // HEAD_DIM
        micro = rows // slot
        me = lax.axis_index("mp")
        slopes = 2.0 ** (
            -8.0
            * (me * local_heads + jnp.arange(local_heads, dtype=jnp.int32) + 1).astype(F32)
            / HEADS
        )
        bias_pair = triple_bias.astype(F32)
        triple_full = lax.all_gather(
            triple_weight.reshape(-1, 3 * head_cols), "dp", axis=0, tiled=True
        )
        merge_full = lax.all_gather(merge_weight, "dp", axis=1, tiled=True)
        expand_full = lax.all_gather(expand_weight, "dp", axis=0, tiled=True)
        reduce_full = lax.all_gather(reduce_weight, "dp", axis=1, tiled=True)
        vectors = jnp.stack(
            [input_gain, input_shift, merge_bias, middle_gain, middle_shift, reduce_bias]
        )
        vectors = lax.all_gather(vectors, "dp", axis=1, tiled=True).astype(F32)
        vectors = jnp.pad(vectors, ((0, 2), (0, 0)))

        def own_rows(array):
            pieces = array.reshape(rows // PIECE, count, PIECE // count, -1)
            mine = lax.dynamic_index_in_dim(pieces, me, axis=1, keepdims=False)
            return mine.reshape(rows // count, -1)

        valid = (jnp.arange(slot, dtype=jnp.int32)[None, :] < lengths[:, None]).reshape(rows, 1)
        own = own_rows(hidden)
        own_valid = own_rows(valid.astype(F32))
        grad_feed = jnp.where(valid, cotangent, jnp.zeros((), BF16))
        own_grad = own_rows(grad_feed)

        normed, _ = norm_parts(hidden.astype(F32))
        norm_in = (normed * vectors[0] + vectors[1]).astype(BF16)
        saved, mixed = [], []
        shape = (slot, local_heads, HEAD_DIM)
        for b in range(micro):
            triple = dot32(norm_in[b * slot : (b + 1) * slot], triple_full)
            query = (triple[:, :head_cols] + bias_pair[0]).astype(BF16).reshape(shape)
            key = triple[:, head_cols : 2 * head_cols].astype(BF16).reshape(shape)
            value = (triple[:, 2 * head_cols :] + bias_pair[1]).astype(BF16).reshape(shape)
            scores = attention_scores(query, key, slopes, lengths[b])
            log_total = jax.nn.logsumexp(scores, axis=-1)
            probs = jnp.exp(scores - log_total[..., None]).astype(BF16)
            heads = jnp.einsum("hqk,khe->qhe", probs, value, preferred_element_type=F32)
            mixed.append(heads.reshape(slot, head_cols).astype(BF16))
            saved.append((query, key, value, log_total))
        mixed = jnp.concatenate(mixed, axis=0)
        norm_mid, residual, sums_one = merge_call(
            count, mixed, merge_full, own, own_valid, vectors
        )
        branch_grad, residual_grad, sums_two, unit_grad, feed_part, expand_grad, reduce_grad = (
            feed_call(
                count,
                norm_mid,
                expand_full,
                reduce_full,
                grad_feed,
                residual,
                own_grad,
                expand_bias.astype(F32)[None],
                vectors,
            )
        )

        def scatter(array, dim):
            return lax.psum_scatter(array, "dp", scatter_dimension=dim, tiled=True).astype(F32)

        reduce_grad = scatter(reduce_grad, 1)
        expand_grad = scatter(expand_grad, 0)
        triples = []
        for b in range(micro):
            query, key, value, log_total = saved[b]
            grad_mixed = dot_nt(branch_grad[b * slot : (b + 1) * slot], merge_full)
            grad_mixed = grad_mixed.astype(BF16).reshape(shape)
            scores = attention_scores(query, key, slopes, lengths[b])
            soft = jnp.exp(scores - log_total[..., None])
            grad_probs = jnp.einsum("qhe,khe->hqk", grad_mixed, value, preferred_element_type=F32)
            grad_value = jnp.einsum(
                "hqk,qhe->khe", soft.astype(BF16), grad_mixed, preferred_element_type=F32
            ).astype(BF16)
            row_terms = jnp.sum(soft * grad_probs, axis=-1, keepdims=True)
            grad_scores = (soft * (grad_probs - row_terms)).astype(BF16)
            grad_query = (
                0.125
                * jnp.einsum("hqk,khe->qhe", grad_scores, key, preferred_element_type=F32)
            ).astype(BF16)
            grad_key = (
                0.125
                * jnp.einsum("hqk,qhe->khe", grad_scores, query, preferred_element_type=F32)
            ).astype(BF16)
            triples.append(
                jnp.concatenate(
                    [
                        grad_query.reshape(slot, head_cols),
                        grad_key.reshape(slot, head_cols),
                        grad_value.reshape(slot, head_cols),
                    ],
                    axis=1,
                )
            )
        grad_triple = jnp.concatenate(triples, axis=0)
        merge_grad = scatter(dot_tn(mixed, branch_grad).astype(BF16), 1)
        triple_grad = scatter(dot_tn(norm_in, grad_triple).astype(BF16), 0)
        column_sums = jnp.sum(grad_triple, axis=0, dtype=F32)

        hidden_grad, output, sums_three = last_call(
            count,
            grad_triple,
            triple_full,
            feed_part,
            own,
            residual,
            residual_grad,
            own_valid,
            vectors,
        )
        squares = jnp.stack(
            [
                jnp.sum(sums_three[2]),
                jnp.sum(sums_one[0]),
                jnp.sum(sums_three[3]),
                jnp.sum(own_valid),
            ]
        )
        over_all = jnp.concatenate([sums_three[0:2], sums_two[0:4]], axis=0)
        over_all = over_all.reshape(6, groups, width // groups).transpose(1, 0, 2)
        over_all = jnp.pad(over_all, ((0, 0), (0, 2), (0, 0)))
        over_all = over_all.at[:, 6, :4].set(squares[None])
        over_dp = jnp.concatenate([column_sums, unit_grad[0]]).reshape(-1, 128)
        tail = (-over_dp.shape[0]) % 8
        over_dp = jnp.pad(over_dp, ((0, tail), (0, 0)))
        return_small, dp_small = small_call(groups, count, over_all, over_dp)
        flat = dp_small.reshape(-1)
        triple_sums = flat[: 3 * head_cols]
        unit_sums = flat[3 * head_cols : 3 * head_cols + units]
        totals = return_small[6, :4]
        root_means = jnp.sqrt(totals[:3] / (totals[3] * width))
        pair_grad = jnp.stack([triple_sums[:head_cols], triple_sums[2 * head_cols :]])
        return (
            output,
            hidden_grad,
            return_small[0],
            return_small[1],
            triple_grad.reshape(-1, 3, head_cols),
            pair_grad,
            merge_grad,
            return_small[2],
            return_small[3],
            return_small[4],
            expand_grad,
            unit_sums,
            reduce_grad,
            return_small[5],
            root_means,
        )

    return local


def solution(mesh):
    return jax.shard_map(
        make_local(mesh.shape["dp"], mesh.shape["mp"]),
        mesh=mesh,
        in_specs=(
            P("dp", None),
            P("dp", None),
            P("dp"),
            P("dp"),
            P("dp"),
            P("dp", None, "mp"),
            P(None, "mp"),
            P("mp", "dp"),
            P("dp"),
            P("dp"),
            P("dp"),
            P("dp", "mp"),
            P("mp"),
            P("mp", "dp"),
            P("dp"),
        ),
        out_specs=(
            P("dp", None),
            P("dp", None),
            P("dp"),
            P("dp"),
            P("dp", None, "mp"),
            P(None, "mp"),
            P("mp", "dp"),
            P("dp"),
            P("dp"),
            P("dp"),
            P("dp", "mp"),
            P("mp"),
            P("mp", "dp"),
            P("dp"),
            P(),
        ),
        check_vma=False,
    )
```

```python
import functools

import jax
import jax.numpy as jnp
from jax import lax
from jax.experimental import pallas as pl
from jax.experimental.pallas import tpu as pltpu
from jax.sharding import PartitionSpec as P

HEADS = 32
HEAD_DIM = 64
SLOT = 512
PIECE = 64
TILE = 256
BLOCK = 512
F32 = jnp.float32
BF16 = jnp.bfloat16
MESH = pl.DeviceIdType.MESH
VMEM = pl.BlockSpec(memory_space=pltpu.VMEM)
ANY = pl.BlockSpec(memory_space=pl.ANY)


def dot32(a, b):
    return jnp.dot(a, b, preferred_element_type=F32)


def dot_nt(a, b):
    return lax.dot_general(a, b, (((1,), (1,)), ((), ())), preferred_element_type=F32)


def dot_tn(a, b):
    return lax.dot_general(a, b, (((0,), (0,)), ((), ())), preferred_element_type=F32)


def norm_parts(values):
    center = values - jnp.mean(values, axis=-1, keepdims=True)
    spread = jnp.mean(center * center, axis=-1, keepdims=True)
    rate = lax.rsqrt(spread + 1e-05)
    return center * rate, rate


def norm_back(grad, gain, normed, rate):
    scaled = grad * gain
    first = jnp.mean(scaled, axis=-1, keepdims=True)
    second = jnp.mean(scaled * normed, axis=-1, keepdims=True)
    return rate * (scaled - first - normed * second)


def block(index, size):
    return pl.ds(pl.multiple_of(index * size, size), size)


def greet(count):
    me, group = lax.axis_index("mp"), lax.axis_index("dp")
    barrier = pltpu.get_barrier_semaphore()

    @pl.when(me < count - 1)
    def _():
        pl.semaphore_signal(barrier, inc=1, device_id=(group, me + 1), device_id_type=MESH)

    @pl.when(me > 0)
    def _():
        pl.semaphore_signal(barrier, inc=1, device_id=(group, me - 1), device_id_type=MESH)

    peers = jnp.where(me > 0, 1, 0) + jnp.where(me < count - 1, 1, 0)
    pl.semaphore_wait(barrier, peers)


LAG = 1


class Line:
    def __init__(self, count, part, inbox, extra, sems):
        self.count, self.part, self.inbox, self.extra = count, part, inbox, extra
        self.pieces = part.shape[0] // PIECE
        self.sum_out, self.sum_in, self.extra_in, self.own_out, self.all_out, self.all_in = sems
        self.rows = PIECE // count
        self.me, self.group = lax.axis_index("mp"), lax.axis_index("dp")

    @staticmethod
    def scratch(count, pieces, width):
        rows = PIECE // count
        return [
            pltpu.VMEM((pieces * rows, width), BF16),
            pltpu.SemaphoreType.DMA((pieces, count)),
            pltpu.SemaphoreType.DMA((pieces, count)),
            pltpu.SemaphoreType.DMA((pieces,)),
            pltpu.SemaphoreType.DMA((pieces,)),
            pltpu.SemaphoreType.DMA((pieces, count)),
            pltpu.SemaphoreType.DMA((pieces, count)),
        ]

    def at(self, piece, owner):
        return pl.ds(pl.multiple_of(piece * PIECE + owner * self.rows, self.rows), self.rows)

    def own(self, piece):
        return block(piece, self.rows)

    def copy(self, src, dst, out, into, to):
        return pltpu.make_async_remote_copy(
            src_ref=src,
            dst_ref=dst,
            send_sem=out,
            recv_sem=into,
            device_id=(self.group, to),
            device_id_type=MESH,
        )

    def sum_copy(self, piece, owner, to):
        rows = self.at(piece, owner)
        return self.copy(
            self.part.at[rows],
            self.inbox.at[rows],
            self.sum_out.at[piece, owner],
            self.sum_in.at[piece, owner],
            to,
        )

    def extra_copy(self, piece, owner, to):
        return self.copy(
            self.part.at[self.at(piece, owner)],
            self.extra.at[self.own(piece)],
            self.sum_out.at[piece, owner],
            self.extra_in.at[piece],
            to,
        )

    def all_copy(self, piece, owner, to, own_left=False):
        rows = self.at(piece, owner)
        return self.copy(
            self.inbox.at[rows],
            self.inbox.at[rows],
            self.own_out.at[piece] if own_left else self.all_out.at[piece, owner],
            self.all_in.at[piece, owner],
            to,
        )

    def add(self, piece, owner):
        rows = self.at(piece, owner)
        self.sum_copy(piece, owner, self.me).wait_recv()
        self.part[rows, :] = (
            self.part[rows, :].astype(F32) + self.inbox[rows, :].astype(F32)
        ).astype(BF16)

    def send_right(self, piece):
        me, last = self.me, self.count - 1
        for owner in range(last, 0, -1):

            @pl.when(me < owner)
            def _(owner=owner):
                @pl.when(me > 0)
                def _():
                    self.add(piece, owner)

                self.sum_copy(piece, owner, me + 1).start()

    def send_left(self, piece):
        me, last = self.me, self.count - 1
        for owner in range(last):

            @pl.when(me > owner)
            def _(owner=owner):
                @pl.when(me < last)
                def _():
                    self.add(piece, owner)

                @pl.when(me == owner + 1)
                def _():
                    self.extra_copy(piece, owner, me - 1).start()

                @pl.when(me > owner + 1)
                def _():
                    self.sum_copy(piece, owner, me - 1).start()

    def total(self, piece, acc):
        me, rows = self.me, self.at(piece, self.me)
        acc[...] = self.part[rows, :].astype(F32)

        @pl.when(me > 0)
        def _():
            self.sum_copy(piece, me, me).wait_recv()
            acc[...] = acc[...] + self.inbox[rows, :].astype(F32)

        @pl.when(me < self.count - 1)
        def _():
            self.extra_copy(piece, me, me).wait_recv()
            acc[...] = acc[...] + self.extra[self.own(piece), :].astype(F32)

    def share(self, piece, values):
        me = self.me
        self.inbox[self.at(piece, me), :] = values

        @pl.when(me < self.count - 1)
        def _():
            self.all_copy(piece, me, me + 1).start()

        @pl.when(me > 0)
        def _():
            self.all_copy(piece, me, me - 1, own_left=True).start()

    def forward(self, piece, away):
        me, last = self.me, self.count - 1

        @pl.when(me >= away)
        def _(owner=me - away):
            self.all_copy(piece, owner, me).wait_recv()

            @pl.when(me < last)
            def _():
                self.all_copy(piece, owner, me + 1).start()

        @pl.when(me + away <= last)
        def _(owner=me + away):
            self.all_copy(piece, owner, me).wait_recv()

            @pl.when(me > 0)
            def _():
                self.all_copy(piece, owner, me - 1).start()

    def settle(self, piece):
        me, last = self.me, self.count - 1
        for owner in range(self.count):

            @pl.when(me != owner)
            def _():
                self.sum_copy(piece, owner, me).wait_send()

            @pl.when(jnp.logical_or(jnp.logical_and(me >= owner, me < last), jnp.logical_and(me < owner, me > 0)))
            def _():
                self.all_copy(piece, owner, me).wait_send()

        @pl.when(me > 0)
        def _():
            self.all_copy(piece, me, me, own_left=True).wait_send()


def tick(line, step, finish):
    def when(piece, work, *more):
        @pl.when(jnp.logical_and(piece >= 0, piece < line.pieces))
        def _():
            work(piece, *more)

    last = line.count - 1
    when(step - LAG * line.me, line.send_right)
    when(step - LAG * (last - line.me), line.send_left)
    when(step - LAG * last, finish)
    for away in range(1, line.count):
        when(step - LAG * (last + away), line.forward, away)


def ticks(count, pieces):
    return pieces + 2 * LAG * (count - 1)


def cost(micros):
    return pl.CostEstimate(flops=int(micros * 1e9), bytes_accessed=1 << 20, transcendentals=0)


def params(index):
    return pltpu.CompilerParams(
        collective_id=index, has_side_effects=True, vmem_limit_bytes=63 << 20
    )


def tiles_of(rows):
    return [(start, min(TILE, rows - start)) for start in range(0, rows, TILE)]


def spread(work, parts):
    return [work[len(work) * k // parts : len(work) * (k + 1) // parts] for k in range(parts)]


def paced(line_tick, tiles, steps, later, drain):
    step = 0
    plans = [spread(work, size // PIECE) for (_, size), work in zip(tiles, later)]
    assert len(later) == len(tiles) and len(drain) == steps - sum(map(len, plans))
    for shares in (*plans, drain):
        span = len(shares)

        @pl.loop(0, span)
        def _(k, step=step, shares=shares):
            line_tick(step + k)
            for phase, share in enumerate(shares):
                if share:

                    @pl.when(k == phase)
                    def _(share=share):
                        for closure in share:
                            closure()

        step += span


def halves(values):
    low = lax.broadcasted_iota(jnp.int32, values.shape, 1) < HEAD_DIM
    zero = jnp.zeros((), values.dtype)
    return jnp.where(low, values, zero), jnp.where(low, zero, values)


PAIR = 2 * HEAD_DIM


def front_kernel(
    count, head_cols, slopes, norm_in, weights, shift, own, valid, segment_col, segment_row, place_row, vectors,
    middle, residual, sums, qkv, mixed, totals, part, acc, mask, *rest,
):
    line = Line(count, part, middle, rest[0], rest[1:])
    rows_all, width = middle.shape
    greet(count)
    sums[...] = jnp.zeros_like(sums)

    def finish(piece):
        line.total(piece, acc)
        rows = line.own(piece)
        branch = acc[...] + vectors[2:3, :]
        result = own[rows, :].astype(F32) + branch
        residual[rows, :] = result
        normed, _ = norm_parts(result)
        line.share(piece, (normed * vectors[3:4, :] + vectors[4:5, :]).astype(BF16))
        sums[0:1, :] += jnp.sum(branch * branch * valid[rows, :], axis=0, keepdims=True)

    def project(start, size):
        rows = pl.ds(start, size)

        @pl.loop(0, 3 * head_cols // BLOCK)
        def _(k):
            cols = block(k, BLOCK)
            qkv[rows, cols] = (dot32(norm_in[rows, :], weights[:, cols]) + shift[:, cols]).astype(BF16)

    def masks(start, size):
        keys = start + size
        row = lax.broadcasted_iota(jnp.int32, (size, keys), 0) + start
        col = lax.broadcasted_iota(jnp.int32, (size, keys), 1)
        same = segment_col[start : start + size, :] == segment_row[:, :keys]
        mask[:size, :keys] = jnp.where(jnp.logical_and(same, col <= row), 1.0, 0.0)

    def attend(start, size, pair):
        keys = start + size
        query = halves(qkv[pl.ds(start, size), block(pair, PAIR)])
        key = qkv[:keys, pl.ds(pl.multiple_of(head_cols + pair * PAIR, PAIR), PAIR)]
        value = halves(qkv[:keys, pl.ds(pl.multiple_of(2 * head_cols + pair * PAIR, PAIR), PAIR)])
        out = jnp.zeros((size, PAIR), F32)
        for k in range(2):
            scores = dot_nt(query[k], key) + slopes[2 * pair + k] * place_row[:, :keys]
            scores = jnp.where(mask[:size, :keys] > 0.5, scores * 0.125, -1000000000.0)
            most = jnp.max(scores, axis=1, keepdims=True)
            raised = jnp.exp(scores - most)
            total = jnp.sum(raised, axis=1, keepdims=True)
            out = out + dot32((raised * (1.0 / total)).astype(BF16), value[k])
            totals[pair, pl.ds(start, size), k : k + 1] = most + jnp.log(total)
        mixed[pl.ds(start, size), block(pair, PAIR)] = out.astype(BF16)

    def project_back(start, size):
        rows = pl.ds(start, size)

        @pl.loop(0, width // BLOCK)
        def _(k):
            cols = block(k, BLOCK)
            part[rows, cols] = dot_nt(mixed[rows, :], weights[cols, 3 * head_cols :]).astype(BF16)

    pairs = head_cols // PAIR

    def work(start, size):
        return [
            functools.partial(project, start, size),
            functools.partial(masks, start, size),
            *[functools.partial(attend, start, size, pair) for pair in range(pairs)],
            functools.partial(project_back, start, size),
        ]

    tiles = tiles_of(rows_all)
    for closure in work(*tiles[0]):
        closure()
    later = [work(*tile) for tile in tiles[1:]] + [[]]
    steps = ticks(count, line.pieces)
    drain = [[]] * (steps - line.pieces)
    paced(lambda step: tick(line, step, finish), tiles, steps, later, drain)

    @pl.loop(0, line.pieces)
    def _(piece):
        line.settle(piece)


SMEM = pl.BlockSpec(memory_space=pltpu.SMEM)


def front_call(count, slopes, norm_in, weights, shift, own, valid, segments, vectors):
    rows, width = norm_in.shape
    head_cols = weights.shape[1] // 4
    pieces = rows // PIECE
    return pl.pallas_call(
        functools.partial(front_kernel, count, head_cols),
        name="front_line",
        out_shape=(
            jax.ShapeDtypeStruct((rows, width), BF16),
            jax.ShapeDtypeStruct((rows // count, width), F32),
            jax.ShapeDtypeStruct((8, width), F32),
            jax.ShapeDtypeStruct((rows, 3 * head_cols), BF16),
            jax.ShapeDtypeStruct((rows, head_cols), BF16),
            jax.ShapeDtypeStruct((head_cols // PAIR, rows, 128), F32),
        ),
        in_specs=[SMEM] + [VMEM] * 9,
        out_specs=(VMEM,) * 6,
        scratch_shapes=[
            pltpu.VMEM((rows, width), BF16),
            pltpu.VMEM((PIECE // count, width), F32),
            pltpu.VMEM((TILE, rows), F32),
            *Line.scratch(count, pieces, width),
        ],
        compiler_params=params(1),
        cost_estimate=cost(120),
    )(slopes, norm_in, weights, shift, own, valid, *segments[:3], vectors)


def feed_kernel(
    count, pieces, middle_hbm, expand_hbm, reduce_hbm, grad_hbm, residual, own_grad, unit_shift, vectors,
    branch_grad, residual_grad, sums, unit_grad, feed_hbm, expand_grad, reduce_grad,
    middle, expand, reduce, grad, active, pre_grad, part, acc, stage, load_sem, stage_sem, *rest,
):
    line = Line(count, part, branch_grad, rest[0], rest[1:])
    units = expand.shape[1]
    width = expand.shape[0]
    blocks = units // BLOCK

    def load(k):
        cols = block(k, BLOCK)
        return (
            pltpu.make_async_copy(expand_hbm.at[:, cols], expand.at[:, cols], load_sem.at[0, k]),
            pltpu.make_async_copy(reduce_hbm.at[cols], reduce.at[cols], load_sem.at[1, k]),
        )

    def load_rows(k):
        rows = block(k, TILE)
        return (
            pltpu.make_async_copy(middle_hbm.at[rows], middle.at[rows], load_sem.at[2, k]),
            pltpu.make_async_copy(grad_hbm.at[rows], grad.at[rows], load_sem.at[3, k]),
        )

    tiles = middle.shape[0] // TILE
    for copy in (*load_rows(0), *load(0)):
        copy.start()
    for k in range(1, blocks):
        for copy in load(k):
            copy.start()
    for k in range(1, tiles):
        for copy in load_rows(k):
            copy.start()
    greet(count)
    sums[...] = jnp.zeros_like(sums)
    unit_grad[...] = jnp.zeros_like(unit_grad)

    def finish(piece):
        line.total(piece, acc)
        rows = line.own(piece)
        grad_mid = acc[...]
        normed, rate = norm_parts(residual[rows, :])
        grad_out = own_grad[rows, :].astype(F32)
        result = grad_out + norm_back(grad_mid, vectors[3:4, :], normed, rate)
        residual_grad[rows, :] = result
        low = result.astype(BF16)
        line.share(piece, low)
        for k, values in enumerate((low.astype(F32), grad_mid * normed, grad_mid, grad_out)):
            sums[k : k + 1, :] += jnp.sum(values, axis=0, keepdims=True)

    def load_tile(tile):
        for copy in load_rows(tile):
            copy.wait()

    def forward_tile(tile, k):
        rows, cols = block(tile, TILE), block(k, BLOCK)

        @pl.when(tile == 0)
        def _():
            for copy in load(k):
                copy.wait()

        pre = dot32(middle[rows, :], expand[:, cols]) + unit_shift[:, cols]
        half = 0.5 + 0.5 * lax.erf(pre * 0.7071067811865476)
        slope = half + pre * (0.3989422804014327 * jnp.exp(-0.5 * pre * pre))
        active[rows, cols] = (pre * half).astype(BF16)
        low = (dot_nt(grad[rows, :], reduce[cols, :]) * slope).astype(BF16)
        pre_grad[rows, cols] = low
        unit_grad[:, cols] += jnp.sum(low.astype(F32), axis=0, keepdims=True)

    def back_tile(tile, k):
        rows, cols = block(tile, TILE), block(k, BLOCK)
        part[rows, cols] = dot_nt(pre_grad[rows, :], expand[cols, :]).astype(BF16)

    def put(slot, target):
        return pltpu.make_async_copy(stage.at[slot], target, stage_sem.at[slot])

    rows_all = middle.shape[0] // BLOCK
    per_feed = rows_all * (width // BLOCK)
    per_grad = (units // BLOCK) * (width // BLOCK)
    jobs = per_feed + 2 * per_grad

    def job(index):
        slot = lax.rem(index, 2)
        across = width // BLOCK

        @pl.when(index >= 2)
        def _():
            put(slot, expand_grad.at[pl.ds(0, BLOCK), pl.ds(0, BLOCK)]).wait()

        @pl.when(index < per_grad)
        def _():
            r, c = block(index // across, BLOCK), block(lax.rem(index, across), BLOCK)
            stage[slot] = dot_tn(active[:, r], grad[:, c]).astype(BF16)
            put(slot, reduce_grad.at[r, c]).start()

        @pl.when(jnp.logical_and(index >= per_grad, index < 2 * per_grad))
        def _():
            local = index - per_grad
            r, c = block(local // across, BLOCK), block(lax.rem(local, across), BLOCK)
            stage[slot] = dot_tn(middle[:, r], pre_grad[:, c]).astype(BF16)
            put(slot, expand_grad.at[r, c]).start()

        @pl.when(index >= 2 * per_grad)
        def _():
            local = index - 2 * per_grad
            r, c = block(local // across, BLOCK), block(lax.rem(local, across), BLOCK)
            stage[slot] = dot32(active[r, :], reduce[:, c]).astype(BF16)
            put(slot, feed_hbm.at[r, c]).start()

    ratio = TILE // PIECE
    backs = width // BLOCK
    load_tile(0)
    pl.loop(0, blocks)(functools.partial(forward_tile, 0))
    pl.loop(0, backs)(functools.partial(back_tile, 0))
    steps = ticks(count, pieces)
    late = (tiles - 1) * ratio
    per_step = -(-jobs // (steps - late))

    @pl.loop(0, steps)
    def _(step):
        tick(line, step, finish)
        tile, phase = step // ratio + 1, lax.rem(step, ratio)

        @pl.when(tile < tiles)
        def _():
            @pl.when(phase == 0)
            def _():
                load_tile(tile)

            @pl.loop(phase * (blocks + backs) // ratio, (phase + 1) * (blocks + backs) // ratio)
            def _(k):
                @pl.when(k < blocks)
                def _():
                    forward_tile(tile, k)

                @pl.when(k >= blocks)
                def _():
                    back_tile(tile, k - blocks)

        @pl.when(tile >= tiles)
        def _():
            first = (step - late) * per_step

            @pl.loop(first, jnp.minimum(first + per_step, jobs))
            def _(index):
                job(index)

    for slot in range(2):
        put(slot, expand_grad.at[pl.ds(0, BLOCK), pl.ds(0, BLOCK)]).wait()

    @pl.loop(0, pieces)
    def _(piece):
        line.settle(piece)


def feed_call(count, middle, expand, reduce, grad, residual, own_grad, unit_shift, vectors):
    rows, width = middle.shape
    units = expand.shape[1]
    pieces = rows // PIECE
    most = max(units // BLOCK, rows // TILE)
    return pl.pallas_call(
        functools.partial(feed_kernel, count, pieces),
        name="feed_line",
        out_shape=(
            jax.ShapeDtypeStruct((rows, width), BF16),
            jax.ShapeDtypeStruct((rows // count, width), F32),
            jax.ShapeDtypeStruct((8, width), F32),
            jax.ShapeDtypeStruct((1, units), F32),
            jax.ShapeDtypeStruct((rows, width), BF16),
            jax.ShapeDtypeStruct((width, units), BF16),
            jax.ShapeDtypeStruct((units, width), BF16),
        ),
        in_specs=[ANY] * 4 + [VMEM] * 4,
        out_specs=(VMEM,) * 4 + (ANY,) * 3,
        scratch_shapes=[
            pltpu.VMEM((rows, width), BF16),
            pltpu.VMEM((width, units), BF16),
            pltpu.VMEM((units, width), BF16),
            pltpu.VMEM((rows, width), BF16),
            pltpu.VMEM((rows, units), BF16),
            pltpu.VMEM((rows, units), BF16),
            pltpu.VMEM((rows, width), BF16),
            pltpu.VMEM((PIECE // count, width), F32),
            pltpu.VMEM((2, BLOCK, BLOCK), BF16),
            pltpu.SemaphoreType.DMA((4, most)),
            pltpu.SemaphoreType.DMA((2,)),
            *Line.scratch(count, pieces, width),
        ],
        compiler_params=params(2),
        cost_estimate=cost(130),
    )(middle, expand, reduce, grad, residual, own_grad, unit_shift, vectors)


def back_kernel(
    count, head_cols, slopes, branch_grad, merge, qkv, mixed, norm_in, totals, segment_col, segment_row, place_col,
    feed, residual, valid, vectors,
    triple_grad, column_sums, output, sums, weight_out,
    mixed_grad, key_grad, value_grad, acc, mask, stage, stage_sem, *rest,
):
    line = Line(count, feed, output, rest[0], rest[1:])
    rows_all, width = output.shape
    greet(count)
    sums[...] = jnp.zeros_like(sums)
    column_sums[...] = jnp.zeros_like(column_sums)

    def finish(piece):
        line.total(piece, acc)
        rows = line.own(piece)
        branch = acc[...] + vectors[5:6, :]
        keep = valid[rows, :] > 0.5
        result = jnp.where(keep, residual[rows, :] + branch, 0.0)
        line.share(piece, result.astype(BF16))
        branch = jnp.where(keep, branch, 0.0)
        sums[0:1, :] += jnp.sum(result * result, axis=0, keepdims=True)
        sums[1:2, :] += jnp.sum(branch * branch, axis=0, keepdims=True)

    def open_tile(start, size):
        rows = pl.ds(start, size)
        mixed_grad[rows, :] = dot32(branch_grad[rows, :], merge[...]).astype(BF16)
        keys = start + size
        row = lax.broadcasted_iota(jnp.int32, (keys, size), 1) + start
        col = lax.broadcasted_iota(jnp.int32, (keys, size), 0)
        same = segment_row[:keys, :] == segment_col[:, start : start + size]
        mask[:keys, :size] = jnp.where(jnp.logical_and(same, col <= row), 1.0, 0.0)

    def back(start, size, first, pair):
        keys = start + size
        rows, cols = pl.ds(start, size), block(pair, PAIR)
        query = halves(qkv[rows, cols])
        key = qkv[:keys, pl.ds(pl.multiple_of(head_cols + pair * PAIR, PAIR), PAIR)]
        value = qkv[:keys, pl.ds(pl.multiple_of(2 * head_cols + pair * PAIR, PAIR), PAIR)]
        grad = halves(mixed_grad[rows, cols])
        keys_apart = halves(key)
        query_grad = jnp.zeros((size, PAIR), F32)
        key_sum = jnp.zeros((keys, PAIR), F32)
        value_sum = jnp.zeros((keys, PAIR), F32)
        for k in range(2):
            scores = dot_nt(key, query[k]) + slopes[2 * pair + k] * place_col[:keys, :]
            scores = jnp.where(mask[:keys, :size] > 0.5, scores * 0.125, -1000000000.0)
            soft = jnp.exp(scores - totals[2 * pair + k : 2 * pair + k + 1, rows])
            grad_probs = dot_nt(value, grad[k])
            row_terms = jnp.sum(soft * grad_probs, axis=0, keepdims=True)
            grad_scores = (soft * (grad_probs - row_terms)).astype(BF16)
            value_sum = value_sum + dot32(soft.astype(BF16), grad[k])
            key_sum = key_sum + dot32(grad_scores, query[k])
            query_grad = query_grad + dot_tn(grad_scores, keys_apart[k])
        triple_grad[rows, cols] = (0.125 * query_grad).astype(BF16)
        if first:
            key_grad[:keys, cols] = key_sum
            value_grad[:keys, cols] = value_sum
        else:
            key_grad[:keys, cols] += key_sum
            value_grad[:keys, cols] += value_sum

    def close_tile(start, size):
        rows = pl.ds(start, size)
        triple_grad[rows, head_cols : 2 * head_cols] = (0.125 * key_grad[rows, :]).astype(BF16)
        triple_grad[rows, 2 * head_cols :] = value_grad[rows, :].astype(BF16)
        column_sums[...] += jnp.sum(triple_grad[rows, :].astype(F32), axis=0, keepdims=True)

    def put(slot, target):
        return pltpu.make_async_copy(stage.at[slot], target, stage_sem.at[slot])

    def job(index, left, right, r, c, shift):
        slot = index % 2
        r, c, to = pl.ds(r, BLOCK), pl.ds(c, BLOCK), pl.ds(c + shift, BLOCK)
        if index >= 2:
            put(slot, weight_out.at[r, to]).wait()
        stage[slot] = dot_tn(left[:, r], right[:, c]).astype(BF16)
        put(slot, weight_out.at[r, to]).start()

    pairs = head_cols // PAIR

    def work(start, size, first):
        return [
            functools.partial(open_tile, start, size),
            *[functools.partial(back, start, size, first, pair) for pair in range(pairs)],
            functools.partial(close_tile, start, size),
        ]

    tiles = tiles_of(rows_all)
    products = [
        (branch_grad, mixed, r, c, 3 * head_cols)
        for r in range(0, width, BLOCK)
        for c in range(0, head_cols, BLOCK)
    ] + [
        (norm_in, triple_grad, r, c, 0)
        for r in range(0, width, BLOCK)
        for c in range(0, 3 * head_cols, BLOCK)
    ]
    jobs = [functools.partial(job, k, *product) for k, product in enumerate(products)]
    later = [work(*tile, k == 0) for k, tile in enumerate(reversed(tiles))]
    steps = ticks(count, line.pieces)
    drain = spread(jobs, steps - line.pieces)
    paced(lambda step: tick(line, step, finish), tiles, steps, later, drain)
    for slot in range(2):
        put(slot, weight_out.at[pl.ds(0, BLOCK), pl.ds(0, BLOCK)]).wait()

    @pl.loop(0, line.pieces)
    def _(piece):
        line.settle(piece)


def back_call(count, slopes, branch_grad, weights, qkv, mixed, norm_in, totals, segments, feed, residual, valid, vectors):
    rows, width = branch_grad.shape
    head_cols = weights.shape[1] // 4
    merge_spec = pl.BlockSpec((width, head_cols), lambda i: (0, 3), memory_space=pltpu.VMEM)
    pieces = rows // PIECE
    return pl.pallas_call(
        functools.partial(back_kernel, count, head_cols),
        name="back_line",
        out_shape=(
            jax.ShapeDtypeStruct((rows, 3 * head_cols), BF16),
            jax.ShapeDtypeStruct((1, 3 * head_cols), F32),
            jax.ShapeDtypeStruct((rows, width), BF16),
            jax.ShapeDtypeStruct((8, width), F32),
            jax.ShapeDtypeStruct((width, 4 * head_cols), BF16),
        ),
        grid=(1,),
        in_specs=[SMEM, VMEM, merge_spec] + [VMEM] * 11,
        out_specs=(VMEM,) * 4 + (ANY,),
        scratch_shapes=[
            pltpu.VMEM((rows, head_cols), BF16),
            pltpu.VMEM((rows, head_cols), F32),
            pltpu.VMEM((rows, head_cols), F32),
            pltpu.VMEM((PIECE // count, width), F32),
            pltpu.VMEM((rows, TILE), F32),
            pltpu.VMEM((2, BLOCK, BLOCK), BF16),
            pltpu.SemaphoreType.DMA((2,)),
            *Line.scratch(count, pieces, width),
        ],
        compiler_params=params(3),
        cost_estimate=cost(120),
    )(slopes, branch_grad, weights, qkv, mixed, norm_in, totals, *segments[3:], feed, residual, valid, vectors)


def greet_all(groups, count):
    me, group = lax.axis_index("mp"), lax.axis_index("dp")
    barrier = pltpu.get_barrier_semaphore()

    @pl.loop(1, groups)
    def _(away):
        to = lax.rem(group + away, groups)
        pl.semaphore_signal(barrier, inc=1, device_id=(to, me), device_id_type=MESH)

    @pl.loop(1, count)
    def _(away):
        to = lax.rem(me + away, count)
        pl.semaphore_signal(barrier, inc=1, device_id=(group, to), device_id_type=MESH)

    pl.semaphore_wait(barrier, groups + count - 2)


def last_kernel(
    groups, count, triple_grad, triple, own, residual_grad, known, over_dp, vectors,
    hidden_grad, all_out, dp_out, sums, cut, all_in, dp_in, own_sum, mp_in, sems, mp_sems, part, acc, *rest,
):
    line = Line(count, part, hidden_grad, rest[0], rest[1:])
    me, group = line.me, line.group
    span = own_sum.shape[0]
    blocks = cut.shape[0]
    greet_all(groups, count)
    sums[...] = known[...]

    def copy_to(src, dst, out, into, to):
        return pltpu.make_async_remote_copy(
            src_ref=src, dst_ref=dst, send_sem=out, recv_sem=into, device_id=to, device_id_type=MESH
        )

    def dp_copy(away):
        to = lax.rem(group + away, groups)
        return copy_to(over_dp, dp_in.at[away], sems.at[0, away], sems.at[1, away], (to, me))

    def block_copy(away):
        to = lax.rem(group + away, groups)
        src = cut.at[pl.ds(to * blocks // groups, span)]
        return copy_to(src, all_in.at[away], sems.at[2, away], sems.at[3, away], (to, me))

    def mp_copy(away):
        to = lax.rem(me + away, count)
        return copy_to(own_sum, mp_in.at[away], mp_sems.at[0, away], mp_sems.at[1, away], (group, to))

    @pl.loop(1, groups)
    def _(away):
        dp_copy(away).start()

    def send_blocks():
        for k in range(blocks):
            cut[k] = sums[:, 128 * k : 128 * (k + 1)]

        @pl.loop(1, groups)
        def _(away):
            block_copy(away).start()

    def add_blocks():
        own_sum[...] = cut[pl.ds(group * blocks // groups, span)]

        @pl.loop(1, groups)
        def _(away):
            block_copy(away).wait_recv()
            own_sum[...] = own_sum[...] + all_in[away]

        @pl.loop(1, count)
        def _(away):
            mp_copy(away).start()

    def add_rest():
        dp_out[...] = over_dp[...]

        @pl.loop(1, groups)
        def _(away):
            dp_copy(away).wait_recv()
            dp_out[...] = dp_out[...] + dp_in[away]

        all_out[...] = own_sum[...]

        @pl.loop(1, count)
        def _(away):
            mp_copy(away).wait_recv()
            all_out[...] = all_out[...] + mp_in[away]

    def finish(piece):
        line.total(piece, acc)
        rows = line.own(piece)
        grad_in = acc[...]
        normed, rate = norm_parts(own[rows, :].astype(F32))
        result = residual_grad[rows, :] + norm_back(grad_in, vectors[0:1, :], normed, rate)
        line.share(piece, result.astype(BF16))
        sums[0:1, :] += jnp.sum(grad_in * normed, axis=0, keepdims=True)
        sums[1:2, :] += jnp.sum(grad_in, axis=0, keepdims=True)

    tiles = tiles_of(part.shape[0])

    def product(start, size, c):
        part[pl.ds(start, size), c : c + BLOCK] = dot_nt(
            triple_grad[pl.ds(start, size), :], triple[c : c + BLOCK, :]
        ).astype(BF16)

    def work(start, size):
        return [functools.partial(product, start, size, c) for c in range(0, part.shape[1], BLOCK)]

    for closure in work(*tiles[0]):
        closure()
    later = [work(*tile) for tile in tiles[1:]] + [[]]
    steps = ticks(count, line.pieces)
    done = LAG * (count - 1) - 1
    drain = [[] for _ in range(steps - line.pieces)]
    drain[done].append(send_blocks)
    drain[done + 2 * LAG].append(add_blocks)
    paced(lambda step: tick(line, step, finish), tiles, steps, later, drain)
    add_rest()

    @pl.loop(0, line.pieces)
    def _(piece):
        line.settle(piece)

    @pl.loop(1, groups)
    def _(away):
        dp_copy(away).wait_send()
        block_copy(away).wait_send()

    @pl.loop(1, count)
    def _(away):
        mp_copy(away).wait_send()


def last_call(groups, count, triple_grad, weights, own, residual_grad, known, over_dp, vectors):
    rows, columns = triple_grad.shape
    width = weights.shape[0]
    triple_spec = pl.BlockSpec((width, columns), lambda i: (0, 0), memory_space=pltpu.VMEM)
    pieces = rows // PIECE
    blocks = width // 128
    span = max(1, blocks // groups)
    return pl.pallas_call(
        functools.partial(last_kernel, groups, count),
        name="last_line",
        out_shape=(
            jax.ShapeDtypeStruct((rows, width), BF16),
            jax.ShapeDtypeStruct((span, 8, 128), F32),
            jax.ShapeDtypeStruct(over_dp.shape, F32),
        ),
        grid=(1,),
        in_specs=[VMEM, triple_spec] + [VMEM] * 5,
        out_specs=(VMEM,) * 3,
        scratch_shapes=[
            pltpu.VMEM((8, width), F32),
            pltpu.VMEM((blocks, 8, 128), F32),
            pltpu.VMEM((groups, span, 8, 128), F32),
            pltpu.VMEM((groups, *over_dp.shape), F32),
            pltpu.VMEM((span, 8, 128), F32),
            pltpu.VMEM((count, span, 8, 128), F32),
            pltpu.SemaphoreType.DMA((4, groups)),
            pltpu.SemaphoreType.DMA((2, count)),
            pltpu.VMEM((rows, width), BF16),
            pltpu.VMEM((PIECE // count, width), F32),
            *Line.scratch(count, pieces, width),
        ],
        compiler_params=params(5),
        cost_estimate=cost(115),
    )(triple_grad, weights, own, residual_grad, known, over_dp, vectors)


def make_local(groups, count):
    def local(
        hidden,
        cotangent,
        lengths,
        input_gain,
        input_shift,
        triple_weight,
        triple_bias,
        merge_weight,
        merge_bias,
        middle_gain,
        middle_shift,
        expand_weight,
        expand_bias,
        reduce_weight,
        reduce_bias,
    ):
        slot = SLOT
        rows, width = hidden.shape
        head_cols = triple_weight.shape[2]
        units = expand_weight.shape[1]
        local_heads = head_cols // HEAD_DIM
        me = lax.axis_index("mp")
        slopes = 2.0 ** (
            -8.0
            * (me * local_heads + jnp.arange(local_heads, dtype=jnp.int32) + 1).astype(F32)
            / HEADS
        )
        bias_pair = triple_bias.astype(F32)
        first = jnp.concatenate([triple_weight.reshape(-1, 3 * head_cols), merge_weight.T], axis=1)
        first_full = lax.all_gather(first, "dp", axis=0, tiled=True)
        expand_full = lax.all_gather(expand_weight, "dp", axis=0, tiled=True)
        reduce_full = lax.all_gather(reduce_weight, "dp", axis=1, tiled=True)
        vectors = jnp.stack(
            [input_gain, input_shift, merge_bias, middle_gain, middle_shift, reduce_bias]
        )
        vectors = lax.all_gather(vectors, "dp", axis=1, tiled=True).astype(F32)
        vectors = jnp.pad(vectors, ((0, 2), (0, 0)))

        def own_rows(array):
            pieces = array.reshape(rows // PIECE, count, PIECE // count, -1)
            mine = lax.dynamic_index_in_dim(pieces, me, axis=1, keepdims=False)
            return mine.reshape(rows // count, -1)

        valid = (jnp.arange(slot, dtype=jnp.int32)[None, :] < lengths[:, None]).reshape(rows, 1)
        own = own_rows(hidden)
        own_valid = own_rows(valid.astype(F32))
        grad_feed = jnp.where(valid, cotangent, jnp.zeros((), BF16))
        own_grad = own_rows(grad_feed)

        normed, _ = norm_parts(hidden.astype(F32))
        norm_in = (normed * vectors[0] + vectors[1]).astype(BF16)
        seats = jnp.arange(rows, dtype=jnp.int32)
        segment = seats // slot
        places = lax.rem(seats, slot).astype(F32)
        as_key = jnp.where(valid[:, 0], segment, -1)
        as_query = jnp.where(valid[:, 0], segment, -2)
        segments = (
            as_query[:, None],
            as_key[None, :],
            places[None, :],
            as_query[None, :],
            as_key[:, None],
            places[:, None],
        )
        shift = jnp.concatenate([bias_pair[0], jnp.zeros_like(bias_pair[0]), bias_pair[1]])[None]
        norm_mid, residual, sums_one, qkv, mixed, totals = front_call(
            count, slopes, norm_in, first_full, shift, own, own_valid, segments, vectors
        )
        totals = totals[:, :, :2].transpose(0, 2, 1).reshape(local_heads, rows)
        branch_grad, residual_grad, sums_two, unit_grad, feed_part, expand_grad, reduce_grad = (
            feed_call(
                count,
                norm_mid,
                expand_full,
                reduce_full,
                grad_feed,
                residual,
                own_grad,
                expand_bias.astype(F32)[None],
                vectors,
            )
        )

        def scatter(array, dim):
            own_block = lax.psum_scatter(array, "dp", scatter_dimension=dim, tiled=True)
            return own_block.astype(F32)

        reduce_grad = scatter(reduce_grad, 1)
        expand_grad = scatter(expand_grad, 0)
        grad_triple, column_sums, output, sums_three, first_grad = back_call(
            count,
            slopes,
            branch_grad,
            first_full,
            qkv,
            mixed,
            norm_in,
            totals,
            segments,
            feed_part,
            residual,
            own_valid,
            vectors,
        )
        first_grad = scatter(first_grad, 0)
        triple_grad = first_grad[:, : 3 * head_cols]
        merge_grad = first_grad[:, 3 * head_cols :].T
        squares = jnp.stack(
            [
                jnp.sum(sums_three[0]),
                jnp.sum(sums_one[0]),
                jnp.sum(sums_three[1]),
                jnp.sum(own_valid),
            ]
        )
        lanes = jnp.tile(jnp.pad(squares, (0, 124)), width // 128)
        known = jnp.concatenate(
            [jnp.zeros((2, width), F32), sums_two[:4], lanes[None], jnp.zeros((1, width), F32)]
        )
        over_dp = jnp.concatenate([column_sums[0], unit_grad[0]]).reshape(-1, 128)
        tail = (-over_dp.shape[0]) % 8
        over_dp = jnp.pad(over_dp, ((0, tail), (0, 0)))
        hidden_grad, small, dp_small = last_call(
            groups, count, grad_triple, first_full, own, residual_grad, known, over_dp, vectors
        )
        share = width // groups
        small = small.transpose(1, 0, 2).reshape(8, -1)
        totals = small[6, :4]
        if share < 128:
            place = lax.rem(lax.axis_index("dp") * share, 128)
            small = lax.dynamic_slice_in_dim(small, place, share, axis=1)
        flat = dp_small.reshape(-1)
        triple_sums = flat[: 3 * head_cols]
        unit_sums = flat[3 * head_cols : 3 * head_cols + units]
        root_means = jnp.sqrt(totals[:3] / (totals[3] * width))
        pair_grad = jnp.stack([triple_sums[:head_cols], triple_sums[2 * head_cols :]])
        return (
            output,
            hidden_grad,
            small[0],
            small[1],
            triple_grad.reshape(-1, 3, head_cols),
            pair_grad,
            merge_grad,
            small[2],
            small[3],
            small[4],
            expand_grad,
            unit_sums,
            reduce_grad,
            small[5],
            root_means,
        )

    return local


def solution(mesh):
    local = make_local(mesh.shape["dp"], mesh.shape["mp"])

    return jax.shard_map(
        local,
        mesh=mesh,
        in_specs=(
            P("dp", None),
            P("dp", None),
            P("dp"),
            P("dp"),
            P("dp"),
            P("dp", None, "mp"),
            P(None, "mp"),
            P("mp", "dp"),
            P("dp"),
            P("dp"),
            P("dp"),
            P("dp", "mp"),
            P("mp"),
            P("mp", "dp"),
            P("dp"),
        ),
        out_specs=(
            P("dp", None),
            P("dp", None),
            P("dp"),
            P("dp"),
            P("dp", None, "mp"),
            P(None, "mp"),
            P("mp", "dp"),
            P("dp"),
            P("dp"),
            P("dp"),
            P("dp", "mp"),
            P("mp"),
            P("mp", "dp"),
            P("dp"),
            P(),
        ),
        check_vma=False,
    )
```

```python
import functools

import jax
import jax.numpy as jnp
from jax import lax
from jax.experimental import pallas as pl
from jax.experimental.pallas import tpu as pltpu
from jax.sharding import PartitionSpec as P

HEADS = 32
HEAD_DIM = 64
SLOT = 512
PIECE = 64
TILE = 256
BLOCK = 512
F32 = jnp.float32
BF16 = jnp.bfloat16
MESH = pl.DeviceIdType.MESH
VMEM = pl.BlockSpec(memory_space=pltpu.VMEM)
ANY = pl.BlockSpec(memory_space=pl.ANY)


def dot32(a, b):
    return jnp.dot(a, b, preferred_element_type=F32)


def dot_nt(a, b):
    return lax.dot_general(a, b, (((1,), (1,)), ((), ())), preferred_element_type=F32)


def dot_tn(a, b):
    return lax.dot_general(a, b, (((0,), (0,)), ((), ())), preferred_element_type=F32)


def norm_parts(values):
    center = values - jnp.mean(values, axis=-1, keepdims=True)
    spread = jnp.mean(center * center, axis=-1, keepdims=True)
    rate = lax.rsqrt(spread + 1e-05)
    return center * rate, rate


def norm_back(grad, gain, normed, rate):
    scaled = grad * gain
    first = jnp.mean(scaled, axis=-1, keepdims=True)
    second = jnp.mean(scaled * normed, axis=-1, keepdims=True)
    return rate * (scaled - first - normed * second)


def block(index, size):
    return pl.ds(pl.multiple_of(index * size, size), size)


def greet(count):
    me, group = lax.axis_index("mp"), lax.axis_index("dp")
    barrier = pltpu.get_barrier_semaphore()

    @pl.when(me < count - 1)
    def _():
        pl.semaphore_signal(barrier, inc=1, device_id=(group, me + 1), device_id_type=MESH)

    @pl.when(me > 0)
    def _():
        pl.semaphore_signal(barrier, inc=1, device_id=(group, me - 1), device_id_type=MESH)

    peers = jnp.where(me > 0, 1, 0) + jnp.where(me < count - 1, 1, 0)
    pl.semaphore_wait(barrier, peers)


LAG = 1


class Line:
    def __init__(self, count, part, result, inbox, extra, *sems):
        self.count, self.part, self.inbox, self.extra, self.result = count, part, inbox, extra, result
        self.pieces = part.shape[0] // PIECE
        self.sum_out, self.sum_in, self.extra_in, self.own_out, self.all_out, self.all_in, self.flushed = sems
        self.rows = PIECE // count
        self.me, self.group = lax.axis_index("mp"), lax.axis_index("dp")

    @staticmethod
    def scratch(count, pieces, width):
        rows = PIECE // count
        return [
            pltpu.VMEM((pieces * PIECE, width), BF16),
            pltpu.VMEM((pieces * rows, width), BF16),
            pltpu.SemaphoreType.DMA((pieces, count)),
            pltpu.SemaphoreType.DMA((pieces, count)),
            pltpu.SemaphoreType.DMA((pieces,)),
            pltpu.SemaphoreType.DMA((pieces,)),
            pltpu.SemaphoreType.DMA((pieces, count)),
            pltpu.SemaphoreType.DMA((pieces, count)),
            pltpu.SemaphoreType.DMA((pieces,)),
        ]

    def at(self, piece, owner):
        return pl.ds(pl.multiple_of(piece * PIECE + owner * self.rows, self.rows), self.rows)

    def own(self, piece):
        return block(piece, self.rows)

    def copy(self, src, dst, out, into, to):
        return pltpu.make_async_remote_copy(
            src_ref=src,
            dst_ref=dst,
            send_sem=out,
            recv_sem=into,
            device_id=(self.group, to),
            device_id_type=MESH,
        )

    def sum_copy(self, piece, owner, to):
        rows = self.at(piece, owner)
        return self.copy(
            self.part.at[rows],
            self.inbox.at[rows],
            self.sum_out.at[piece, owner],
            self.sum_in.at[piece, owner],
            to,
        )

    def extra_copy(self, piece, owner, to):
        return self.copy(
            self.part.at[self.at(piece, owner)],
            self.extra.at[self.own(piece)],
            self.sum_out.at[piece, owner],
            self.extra_in.at[piece],
            to,
        )

    def all_copy(self, piece, owner, to, own_left=False):
        rows = self.at(piece, owner)
        return self.copy(
            self.inbox.at[rows],
            self.inbox.at[rows],
            self.own_out.at[piece] if own_left else self.all_out.at[piece, owner],
            self.all_in.at[piece, owner],
            to,
        )

    def add(self, piece, owner):
        rows = self.at(piece, owner)
        self.sum_copy(piece, owner, self.me).wait_recv()
        self.part[rows, :] = (
            self.part[rows, :].astype(F32) + self.inbox[rows, :].astype(F32)
        ).astype(BF16)

    def send_right(self, piece):
        me, last = self.me, self.count - 1
        for owner in range(last, 0, -1):

            @pl.when(me < owner)
            def _(owner=owner):
                @pl.when(me > 0)
                def _():
                    self.add(piece, owner)

                self.sum_copy(piece, owner, me + 1).start()

    def send_left(self, piece):
        me, last = self.me, self.count - 1
        for owner in range(last):

            @pl.when(me > owner)
            def _(owner=owner):
                @pl.when(me < last)
                def _():
                    self.add(piece, owner)

                @pl.when(me == owner + 1)
                def _():
                    self.extra_copy(piece, owner, me - 1).start()

                @pl.when(me > owner + 1)
                def _():
                    self.sum_copy(piece, owner, me - 1).start()

    def total(self, piece, acc):
        me, rows = self.me, self.at(piece, self.me)
        acc[...] = self.part[rows, :].astype(F32)

        @pl.when(me > 0)
        def _():
            self.sum_copy(piece, me, me).wait_recv()
            acc[...] = acc[...] + self.inbox[rows, :].astype(F32)

        @pl.when(me < self.count - 1)
        def _():
            self.extra_copy(piece, me, me).wait_recv()
            acc[...] = acc[...] + self.extra[self.own(piece), :].astype(F32)

    def share(self, piece, values):
        me = self.me
        self.inbox[self.at(piece, me), :] = values

        @pl.when(me < self.count - 1)
        def _():
            self.all_copy(piece, me, me + 1).start()

        @pl.when(me > 0)
        def _():
            self.all_copy(piece, me, me - 1, own_left=True).start()

    def forward(self, piece, away):
        me, last = self.me, self.count - 1

        @pl.when(me >= away)
        def _(owner=me - away):
            self.all_copy(piece, owner, me).wait_recv()

            @pl.when(me < last)
            def _():
                self.all_copy(piece, owner, me + 1).start()

        @pl.when(me + away <= last)
        def _(owner=me + away):
            self.all_copy(piece, owner, me).wait_recv()

            @pl.when(me > 0)
            def _():
                self.all_copy(piece, owner, me - 1).start()

    def flush_copy(self, piece):
        rows = block(piece, PIECE)
        return pltpu.make_async_copy(self.inbox.at[rows], self.result.at[rows], self.flushed.at[piece])

    def flush(self, piece):
        self.flush_copy(piece).start()

    def settle(self, piece):
        me, last = self.me, self.count - 1
        self.flush_copy(piece).wait()
        for owner in range(self.count):

            @pl.when(me != owner)
            def _():
                self.sum_copy(piece, owner, me).wait_send()

            @pl.when(jnp.logical_or(jnp.logical_and(me >= owner, me < last), jnp.logical_and(me < owner, me > 0)))
            def _():
                self.all_copy(piece, owner, me).wait_send()

        @pl.when(me > 0)
        def _():
            self.all_copy(piece, me, me, own_left=True).wait_send()


def tick(line, step, finish):
    def when(piece, work, *more):
        @pl.when(jnp.logical_and(piece >= 0, piece < line.pieces))
        def _():
            work(piece, *more)

    last = line.count - 1
    when(step - LAG * line.me, line.send_right)
    when(step - LAG * (last - line.me), line.send_left)
    when(step - LAG * last, finish)
    for away in range(1, line.count):
        when(step - LAG * (last + away), line.forward, away)
    when(step - LAG * 2 * last, line.flush)


def ticks(count, pieces):
    return pieces + 2 * LAG * (count - 1)


def cost(micros):
    return pl.CostEstimate(flops=int(micros * 1e9), bytes_accessed=1 << 20, transcendentals=0)


def params(index):
    return pltpu.CompilerParams(
        collective_id=index, has_side_effects=True, vmem_limit_bytes=63 << 20
    )


def tiles_of(rows):
    return [(start, min(TILE, rows - start)) for start in range(0, rows, TILE)]


def spread(work, parts):
    return [work[len(work) * k // parts : len(work) * (k + 1) // parts] for k in range(parts)]


def paced(line_tick, tiles, steps, later, drain):
    step = 0
    plans = [spread(work, size // PIECE) for (_, size), work in zip(tiles, later)]
    assert len(later) == len(tiles) and len(drain) == steps - sum(map(len, plans))
    for shares in (*plans, drain):
        span = len(shares)

        @pl.loop(0, span)
        def _(k, step=step, shares=shares):
            line_tick(step + k)
            for phase, share in enumerate(shares):
                if share:

                    @pl.when(k == phase)
                    def _(share=share):
                        for closure in share:
                            closure()

        step += span


def halves(values):
    low = lax.broadcasted_iota(jnp.int32, values.shape, 1) < HEAD_DIM
    zero = jnp.zeros((), values.dtype)
    return jnp.where(low, values, zero), jnp.where(low, zero, values)


PAIR = 2 * HEAD_DIM


def front_kernel(
    count, head_cols, slopes, norm_hbm, weights_hbm, shift, own, valid, segment_col, segment_row, place_row, vectors,
    middle, residual, sums, qkv_hbm, mixed_hbm, totals,
    norm_in, weights, qkv, mixed, load_sem, save_sem, part, acc, mask, *rest,
):
    line = Line(count, part, middle, *rest)
    rows_all, width = middle.shape
    tiles = tiles_of(rows_all)
    blocks = weights.shape[1] // BLOCK

    def load_rows(k):
        rows = pl.ds(tiles[k][0], tiles[k][1])
        return pltpu.make_async_copy(norm_hbm.at[rows], norm_in.at[rows], load_sem.at[0, k])

    def load_columns(k):
        cols = block(k, BLOCK)
        return pltpu.make_async_copy(weights_hbm.at[:, cols], weights.at[:, cols], load_sem.at[1, k])

    load_rows(0).start()
    for k in range(blocks):
        load_columns(k).start()
    for k in range(1, len(tiles)):
        load_rows(k).start()
    greet(count)
    sums[...] = jnp.zeros_like(sums)

    def finish(piece):
        line.total(piece, acc)
        rows = line.own(piece)
        branch = acc[...] + vectors[2:3, :]
        result = own[rows, :].astype(F32) + branch
        residual[rows, :] = result
        normed, _ = norm_parts(result)
        line.share(piece, (normed * vectors[3:4, :] + vectors[4:5, :]).astype(BF16))
        sums[0:1, :] += jnp.sum(branch * branch * valid[rows, :], axis=0, keepdims=True)

    def project(start, size):
        rows = pl.ds(start, size)
        load_rows(start // TILE).wait()

        @pl.loop(0, 3 * head_cols // BLOCK)
        def _(k):
            cols = block(k, BLOCK)
            if start == 0:
                load_columns(k).wait()
            qkv[rows, cols] = (dot32(norm_in[rows, :], weights[:, cols]) + shift[:, cols]).astype(BF16)

    def masks(start, size):
        keys = start + size
        row = lax.broadcasted_iota(jnp.int32, (size, keys), 0) + start
        col = lax.broadcasted_iota(jnp.int32, (size, keys), 1)
        same = segment_col[start : start + size, :] == segment_row[:, :keys]
        mask[:size, :keys] = jnp.where(jnp.logical_and(same, col <= row), 1.0, 0.0)

    def attend(start, size, pair):
        keys = start + size
        query = halves(qkv[pl.ds(start, size), block(pair, PAIR)])
        key = qkv[:keys, pl.ds(pl.multiple_of(head_cols + pair * PAIR, PAIR), PAIR)]
        value = halves(qkv[:keys, pl.ds(pl.multiple_of(2 * head_cols + pair * PAIR, PAIR), PAIR)])
        out = jnp.zeros((size, PAIR), F32)
        sums_log = jnp.zeros((size, 128), F32)
        lane = lax.broadcasted_iota(jnp.int32, (size, 128), 1)
        for k in range(2):
            scores = dot_nt(query[k], key) + slopes[2 * pair + k] * place_row[:, :keys]
            scores = jnp.where(mask[:size, :keys] > 0.5, scores * 0.125, -1000000000.0)
            most = jnp.max(scores, axis=1, keepdims=True)
            raised = jnp.exp(scores - most)
            total = jnp.sum(raised, axis=1, keepdims=True)
            out = out + dot32((raised * (1.0 / total)).astype(BF16), value[k])
            sums_log = jnp.where(lane == k, most + jnp.log(total), sums_log)
        totals[2 * pair : 2 * pair + 2, start : start + size] = sums_log.T[:2, :]
        mixed[pl.ds(start, size), block(pair, PAIR)] = out.astype(BF16)

    def project_back(start, size):
        rows = pl.ds(start, size)
        if start == 0:
            for k in range(3 * head_cols // BLOCK, blocks):
                load_columns(k).wait()

        @pl.loop(0, width // BLOCK)
        def _(k):
            cols = block(k, BLOCK)
            part[rows, cols] = dot_nt(mixed[rows, :], weights[cols, 3 * head_cols :]).astype(BF16)

    pairs = head_cols // PAIR

    def work(start, size):
        return [
            functools.partial(project, start, size),
            functools.partial(masks, start, size),
            *[functools.partial(attend, start, size, pair) for pair in range(pairs)],
            functools.partial(project_back, start, size),
        ]

    saves = (
        pltpu.make_async_copy(qkv, qkv_hbm, save_sem.at[0]),
        pltpu.make_async_copy(mixed, mixed_hbm, save_sem.at[1]),
    )

    def save():
        for copy in saves:
            copy.start()

    for closure in work(*tiles[0]):
        closure()
    later = [work(*tile) for tile in tiles[1:]] + [[save]]
    steps = ticks(count, line.pieces)
    drain = [[]] * (steps - line.pieces)
    paced(lambda step: tick(line, step, finish), tiles, steps, later, drain)
    for copy in saves:
        copy.wait()

    @pl.loop(0, line.pieces)
    def _(piece):
        line.settle(piece)


SMEM = pl.BlockSpec(memory_space=pltpu.SMEM)


def front_call(count, slopes, norm_in, weights, shift, own, valid, segments, vectors):
    rows, width = norm_in.shape
    head_cols = weights.shape[1] // 4
    pieces = rows // PIECE
    return pl.pallas_call(
        functools.partial(front_kernel, count, head_cols),
        name="front_line",
        out_shape=(
            jax.ShapeDtypeStruct((rows, width), BF16),
            jax.ShapeDtypeStruct((rows // count, width), F32),
            jax.ShapeDtypeStruct((8, width), F32),
            jax.ShapeDtypeStruct((rows, 3 * head_cols), BF16),
            jax.ShapeDtypeStruct((rows, head_cols), BF16),
            jax.ShapeDtypeStruct((head_cols // HEAD_DIM, rows), F32),
        ),
        in_specs=[SMEM] + [ANY] * 2 + [VMEM] * 7,
        out_specs=(ANY, VMEM, VMEM, ANY, ANY, VMEM),
        scratch_shapes=[
            pltpu.VMEM((rows, width), BF16),
            pltpu.VMEM(weights.shape, BF16),
            pltpu.VMEM((rows, 3 * head_cols), BF16),
            pltpu.VMEM((rows, head_cols), BF16),
            pltpu.SemaphoreType.DMA((2, max(len(tiles_of(rows)), weights.shape[1] // BLOCK))),
            pltpu.SemaphoreType.DMA((2,)),
            pltpu.VMEM((rows, width), BF16),
            pltpu.VMEM((PIECE // count, width), F32),
            pltpu.VMEM((TILE, rows), F32),
            *Line.scratch(count, pieces, width),
        ],
        compiler_params=params(1),
        cost_estimate=cost(120),
    )(slopes, norm_in, weights, shift, own, valid, *segments[:3], vectors)


def feed_kernel(
    count, pieces, middle_hbm, expand_hbm, reduce_hbm, grad_hbm, residual, own_grad, unit_shift, vectors,
    branch_grad, residual_grad, sums, unit_grad, feed_hbm, expand_grad, reduce_grad,
    middle, expand, reduce, grad, active, pre_grad, part, acc, stage, load_sem, stage_sem, *rest,
):
    line = Line(count, part, branch_grad, *rest)
    units = expand.shape[1]
    width = expand.shape[0]
    blocks = units // BLOCK

    def load(k):
        cols = block(k, BLOCK)
        return (
            pltpu.make_async_copy(expand_hbm.at[:, cols], expand.at[:, cols], load_sem.at[0, k]),
            pltpu.make_async_copy(reduce_hbm.at[cols], reduce.at[cols], load_sem.at[1, k]),
        )

    def load_rows(k):
        rows = block(k, TILE)
        return (
            pltpu.make_async_copy(middle_hbm.at[rows], middle.at[rows], load_sem.at[2, k]),
            pltpu.make_async_copy(grad_hbm.at[rows], grad.at[rows], load_sem.at[3, k]),
        )

    tiles = middle.shape[0] // TILE
    for copy in (*load_rows(0), *load(0)):
        copy.start()
    for k in range(1, blocks):
        for copy in load(k):
            copy.start()
    for k in range(1, tiles):
        for copy in load_rows(k):
            copy.start()
    greet(count)
    sums[...] = jnp.zeros_like(sums)
    unit_grad[...] = jnp.zeros_like(unit_grad)

    def finish(piece):
        line.total(piece, acc)
        rows = line.own(piece)
        grad_mid = acc[...]
        normed, rate = norm_parts(residual[rows, :])
        grad_out = own_grad[rows, :].astype(F32)
        result = grad_out + norm_back(grad_mid, vectors[3:4, :], normed, rate)
        residual_grad[rows, :] = result
        low = result.astype(BF16)
        line.share(piece, low)
        for k, values in enumerate((low.astype(F32), grad_mid * normed, grad_mid, grad_out)):
            sums[k : k + 1, :] += jnp.sum(values, axis=0, keepdims=True)

    def load_tile(tile):
        for copy in load_rows(tile):
            copy.wait()

    def forward_tile(tile, k):
        rows, cols = block(tile, TILE), block(k, BLOCK)

        @pl.when(tile == 0)
        def _():
            for copy in load(k):
                copy.wait()

        pre = dot32(middle[rows, :], expand[:, cols]) + unit_shift[:, cols]
        half = 0.5 + 0.5 * lax.erf(pre * 0.7071067811865476)
        slope = half + pre * (0.3989422804014327 * jnp.exp(-0.5 * pre * pre))
        active[rows, cols] = (pre * half).astype(BF16)
        low = (dot_nt(grad[rows, :], reduce[cols, :]) * slope).astype(BF16)
        pre_grad[rows, cols] = low
        unit_grad[:, cols] += jnp.sum(low.astype(F32), axis=0, keepdims=True)

    def back_tile(tile, k):
        rows, cols = block(tile, TILE), block(k, BLOCK)
        part[rows, cols] = dot_nt(pre_grad[rows, :], expand[cols, :]).astype(BF16)

    def put(slot, target):
        return pltpu.make_async_copy(stage.at[slot], target, stage_sem.at[slot])

    rows_all = middle.shape[0] // BLOCK
    per_feed = rows_all * (width // BLOCK)
    per_grad = (units // BLOCK) * (width // BLOCK)
    jobs = per_feed + 2 * per_grad

    def job(index):
        slot = lax.rem(index, 2)
        across = width // BLOCK

        @pl.when(index >= 2)
        def _():
            put(slot, expand_grad.at[pl.ds(0, BLOCK), pl.ds(0, BLOCK)]).wait()

        @pl.when(index < per_grad)
        def _():
            r, c = block(index // across, BLOCK), block(lax.rem(index, across), BLOCK)
            stage[slot] = dot_tn(active[:, r], grad[:, c]).astype(BF16)
            put(slot, reduce_grad.at[r, c]).start()

        @pl.when(jnp.logical_and(index >= per_grad, index < 2 * per_grad))
        def _():
            local = index - per_grad
            r, c = block(local // across, BLOCK), block(lax.rem(local, across), BLOCK)
            stage[slot] = dot_tn(middle[:, r], pre_grad[:, c]).astype(BF16)
            put(slot, expand_grad.at[r, c]).start()

        @pl.when(index >= 2 * per_grad)
        def _():
            local = index - 2 * per_grad
            r, c = block(local // across, BLOCK), block(lax.rem(local, across), BLOCK)
            stage[slot] = dot32(active[r, :], reduce[:, c]).astype(BF16)
            put(slot, feed_hbm.at[r, c]).start()

    ratio = TILE // PIECE
    backs = width // BLOCK
    load_tile(0)
    pl.loop(0, blocks)(functools.partial(forward_tile, 0))
    pl.loop(0, backs)(functools.partial(back_tile, 0))
    steps = ticks(count, pieces)
    late = (tiles - 1) * ratio
    per_step = -(-jobs // (steps - late))

    @pl.loop(0, steps)
    def _(step):
        tick(line, step, finish)
        tile, phase = step // ratio + 1, lax.rem(step, ratio)

        @pl.when(tile < tiles)
        def _():
            @pl.when(phase == 0)
            def _():
                load_tile(tile)

            @pl.loop(phase * (blocks + backs) // ratio, (phase + 1) * (blocks + backs) // ratio)
            def _(k):
                @pl.when(k < blocks)
                def _():
                    forward_tile(tile, k)

                @pl.when(k >= blocks)
                def _():
                    back_tile(tile, k - blocks)

        @pl.when(tile >= tiles)
        def _():
            first = (step - late) * per_step

            @pl.loop(first, jnp.minimum(first + per_step, jobs))
            def _(index):
                job(index)

    for slot in range(2):
        put(slot, expand_grad.at[pl.ds(0, BLOCK), pl.ds(0, BLOCK)]).wait()

    @pl.loop(0, pieces)
    def _(piece):
        line.settle(piece)


def feed_call(count, middle, expand, reduce, grad, residual, own_grad, unit_shift, vectors):
    rows, width = middle.shape
    units = expand.shape[1]
    pieces = rows // PIECE
    most = max(units // BLOCK, rows // TILE)
    return pl.pallas_call(
        functools.partial(feed_kernel, count, pieces),
        name="feed_line",
        out_shape=(
            jax.ShapeDtypeStruct((rows, width), BF16),
            jax.ShapeDtypeStruct((rows // count, width), F32),
            jax.ShapeDtypeStruct((8, width), F32),
            jax.ShapeDtypeStruct((1, units), F32),
            jax.ShapeDtypeStruct((rows, width), BF16),
            jax.ShapeDtypeStruct((width, units), BF16),
            jax.ShapeDtypeStruct((units, width), BF16),
        ),
        in_specs=[ANY] * 4 + [VMEM] * 4,
        out_specs=(ANY,) + (VMEM,) * 3 + (ANY,) * 3,
        scratch_shapes=[
            pltpu.VMEM((rows, width), BF16),
            pltpu.VMEM((width, units), BF16),
            pltpu.VMEM((units, width), BF16),
            pltpu.VMEM((rows, width), BF16),
            pltpu.VMEM((rows, units), BF16),
            pltpu.VMEM((rows, units), BF16),
            pltpu.VMEM((rows, width), BF16),
            pltpu.VMEM((PIECE // count, width), F32),
            pltpu.VMEM((2, BLOCK, BLOCK), BF16),
            pltpu.SemaphoreType.DMA((4, most)),
            pltpu.SemaphoreType.DMA((2,)),
            *Line.scratch(count, pieces, width),
        ],
        compiler_params=params(2),
        cost_estimate=cost(130),
    )(middle, expand, reduce, grad, residual, own_grad, unit_shift, vectors)


def back_kernel(
    count, head_cols, slopes, branch_hbm, merge, qkv, mixed, norm_hbm, totals, segment_col, segment_row, place_col,
    feed_hbm, residual_hbm, valid, vectors,
    triple_grad, column_sums, output, sums, weight_out,
    branch_grad, norm_in, feed, residual, load_sem, save_sem,
    mixed_grad, key_grad, value_grad, acc, mask, stage, stage_sem, *rest,
):
    line = Line(count, feed, output, *rest)
    rows_all, width = output.shape
    tiles = tiles_of(rows_all)

    def load_feed(k):
        rows = pl.ds(tiles[k][0], tiles[k][1])
        return pltpu.make_async_copy(feed_hbm.at[rows], feed.at[rows], load_sem.at[0, k])

    def load_grad(k):
        rows = pl.ds(tiles[k][0], tiles[k][1])
        return pltpu.make_async_copy(branch_hbm.at[rows], branch_grad.at[rows], load_sem.at[1, k])

    load_residual = pltpu.make_async_copy(residual_hbm, residual, load_sem.at[2, 0])
    load_norm = pltpu.make_async_copy(norm_hbm, norm_in, load_sem.at[2, 1])
    load_feed(0).start()
    load_grad(len(tiles) - 1).start()
    load_residual.start()
    for k in range(1, len(tiles)):
        load_feed(k).start()
        load_grad(len(tiles) - 1 - k).start()
    load_norm.start()
    greet(count)
    load_feed(0).wait()
    load_residual.wait()
    sums[...] = jnp.zeros_like(sums)
    column_sums[...] = jnp.zeros_like(column_sums)

    def finish(piece):
        line.total(piece, acc)
        rows = line.own(piece)
        branch = acc[...] + vectors[5:6, :]
        keep = valid[rows, :] > 0.5
        result = jnp.where(keep, residual[rows, :] + branch, 0.0)
        line.share(piece, result.astype(BF16))
        branch = jnp.where(keep, branch, 0.0)
        sums[0:1, :] += jnp.sum(result * result, axis=0, keepdims=True)
        sums[1:2, :] += jnp.sum(branch * branch, axis=0, keepdims=True)

    def open_tile(start, size):
        rows = pl.ds(start, size)
        load_grad(start // TILE).wait()
        mixed_grad[rows, :] = dot32(branch_grad[rows, :], merge[...]).astype(BF16)
        keys = start + size
        row = lax.broadcasted_iota(jnp.int32, (keys, size), 1) + start
        col = lax.broadcasted_iota(jnp.int32, (keys, size), 0)
        same = segment_row[:keys, :] == segment_col[:, start : start + size]
        mask[:keys, :size] = jnp.where(jnp.logical_and(same, col <= row), 1.0, 0.0)

    def back(start, size, first, pair):
        keys = start + size
        rows, cols = pl.ds(start, size), block(pair, PAIR)
        query = halves(qkv[rows, cols])
        key = qkv[:keys, pl.ds(pl.multiple_of(head_cols + pair * PAIR, PAIR), PAIR)]
        value = qkv[:keys, pl.ds(pl.multiple_of(2 * head_cols + pair * PAIR, PAIR), PAIR)]
        grad = halves(mixed_grad[rows, cols])
        keys_apart = halves(key)
        query_grad = jnp.zeros((size, PAIR), F32)
        key_sum = jnp.zeros((keys, PAIR), F32)
        value_sum = jnp.zeros((keys, PAIR), F32)
        for k in range(2):
            scores = dot_nt(key, query[k]) + slopes[2 * pair + k] * place_col[:keys, :]
            scores = jnp.where(mask[:keys, :size] > 0.5, scores * 0.125, -1000000000.0)
            soft = jnp.exp(scores - totals[2 * pair + k : 2 * pair + k + 1, rows])
            grad_probs = dot_nt(value, grad[k])
            row_terms = jnp.sum(soft * grad_probs, axis=0, keepdims=True)
            grad_scores = (soft * (grad_probs - row_terms)).astype(BF16)
            value_sum = value_sum + dot32(soft.astype(BF16), grad[k])
            key_sum = key_sum + dot32(grad_scores, query[k])
            query_grad = query_grad + dot_tn(grad_scores, keys_apart[k])
        triple_grad[rows, cols] = (0.125 * query_grad).astype(BF16)
        if first:
            key_grad[:keys, cols] = key_sum
            value_grad[:keys, cols] = value_sum
        else:
            key_grad[:keys, cols] += key_sum
            value_grad[:keys, cols] += value_sum

    def close_tile(start, size):
        rows = pl.ds(start, size)
        triple_grad[rows, head_cols : 2 * head_cols] = (0.125 * key_grad[rows, :]).astype(BF16)
        triple_grad[rows, 2 * head_cols :] = value_grad[rows, :].astype(BF16)
        column_sums[...] += jnp.sum(triple_grad[rows, :].astype(F32), axis=0, keepdims=True)

    def put(slot, target):
        return pltpu.make_async_copy(stage.at[slot], target, stage_sem.at[slot])

    def job(index, left, right, r, c, shift):
        slot = index % 2
        r, c, to = pl.ds(r, BLOCK), pl.ds(c, BLOCK), pl.ds(c + shift, BLOCK)
        if index >= 2:
            put(slot, weight_out.at[r, to]).wait()
        stage[slot] = dot_tn(left[:, r], right[:, c]).astype(BF16)
        put(slot, weight_out.at[r, to]).start()

    pairs = head_cols // PAIR

    def work(start, size, first):
        return [
            functools.partial(open_tile, start, size),
            *[functools.partial(back, start, size, first, pair) for pair in range(pairs)],
            functools.partial(close_tile, start, size),
        ]

    products = [
        (branch_grad, mixed, r, c, 3 * head_cols)
        for r in range(0, width, BLOCK)
        for c in range(0, head_cols, BLOCK)
    ] + [
        (norm_in, triple_grad, r, c, 0)
        for r in range(0, width, BLOCK)
        for c in range(0, 3 * head_cols, BLOCK)
    ]
    jobs = [functools.partial(job, k, *product) for k, product in enumerate(products)]
    later = [work(*tile, k == 0) for k, tile in enumerate(reversed(tiles))]
    for k in range(1, len(tiles)):
        later[k - 1].append(lambda k=k: load_feed(k).wait())
    later[-1].append(load_norm.wait)
    steps = ticks(count, line.pieces)
    drain = spread(jobs, steps - line.pieces)
    paced(lambda step: tick(line, step, finish), tiles, steps, later, drain)
    for slot in range(2):
        put(slot, weight_out.at[pl.ds(0, BLOCK), pl.ds(0, BLOCK)]).wait()

    @pl.loop(0, line.pieces)
    def _(piece):
        line.settle(piece)


def back_call(count, slopes, branch_grad, weights, qkv, mixed, norm_in, totals, segments, feed, residual, valid, vectors):
    rows, width = branch_grad.shape
    head_cols = weights.shape[1] // 4
    merge_spec = pl.BlockSpec((width, head_cols), lambda i: (0, 3), memory_space=pltpu.VMEM)
    pieces = rows // PIECE
    return pl.pallas_call(
        functools.partial(back_kernel, count, head_cols),
        name="back_line",
        out_shape=(
            jax.ShapeDtypeStruct((rows, 3 * head_cols), BF16),
            jax.ShapeDtypeStruct((1, 3 * head_cols), F32),
            jax.ShapeDtypeStruct((rows, width), BF16),
            jax.ShapeDtypeStruct((8, width), F32),
            jax.ShapeDtypeStruct((width, 4 * head_cols), BF16),
        ),
        grid=(1,),
        in_specs=[SMEM, ANY, merge_spec, VMEM, VMEM, ANY] + [VMEM] * 4 + [ANY] * 2 + [VMEM] * 2,
        out_specs=(VMEM, VMEM, ANY, VMEM, ANY),
        scratch_shapes=[
            pltpu.VMEM((rows, width), BF16),
            pltpu.VMEM((rows, width), BF16),
            pltpu.VMEM((rows, width), BF16),
            pltpu.VMEM((rows // count, width), F32),
            pltpu.SemaphoreType.DMA((3, max(2, len(tiles_of(rows))))),
            pltpu.SemaphoreType.DMA((2,)),
            pltpu.VMEM((rows, head_cols), BF16),
            pltpu.VMEM((rows, head_cols), F32),
            pltpu.VMEM((rows, head_cols), F32),
            pltpu.VMEM((PIECE // count, width), F32),
            pltpu.VMEM((rows, TILE), F32),
            pltpu.VMEM((2, BLOCK, BLOCK), BF16),
            pltpu.SemaphoreType.DMA((2,)),
            *Line.scratch(count, pieces, width),
        ],
        compiler_params=params(3),
        cost_estimate=cost(120),
    )(slopes, branch_grad, weights, qkv, mixed, norm_in, totals, *segments[3:], feed, residual, valid, vectors)


def greet_all(groups, count):
    me, group = lax.axis_index("mp"), lax.axis_index("dp")
    barrier = pltpu.get_barrier_semaphore()

    @pl.loop(1, groups)
    def _(away):
        to = lax.rem(group + away, groups)
        pl.semaphore_signal(barrier, inc=1, device_id=(to, me), device_id_type=MESH)

    @pl.loop(1, count)
    def _(away):
        to = lax.rem(me + away, count)
        pl.semaphore_signal(barrier, inc=1, device_id=(group, to), device_id_type=MESH)

    pl.semaphore_wait(barrier, groups + count - 2)


def last_kernel(
    groups, count, triple_grad, triple_hbm, own, residual_grad, front_sums, feed_sums, back_sums, valid,
    column_sums, unit_grad, vectors,
    hidden_grad, all_out, dp_out,
    triple, load_sem, sums, over_dp, cut, all_in, dp_in, own_sum, mp_in, sems, mp_sems, part, acc, *rest,
):
    line = Line(count, part, hidden_grad, *rest)
    me, group = line.me, line.group
    span = own_sum.shape[0]
    blocks = cut.shape[0]
    columns = triple.shape[1]

    def load(k):
        rows = block(k, BLOCK)
        return pltpu.make_async_copy(
            triple_hbm.at[rows, pl.ds(0, columns)], triple.at[rows], load_sem.at[k]
        )

    for k in range(triple.shape[0] // BLOCK):
        load(k).start()
    greet_all(groups, count)
    sums[0:2, :] = jnp.zeros_like(sums[0:2, :])
    sums[2:6, :] = feed_sums[0:4, :]
    sums[6:8, :] = jnp.zeros_like(sums[6:8, :])
    lane = lax.broadcasted_iota(jnp.int32, (1, 128), 1)
    squares = jnp.zeros((1, 128), F32)
    for k, row in enumerate((back_sums[0:1, :], front_sums[0:1, :], back_sums[1:2, :])):
        squares = jnp.where(lane == k, jnp.sum(row, axis=1, keepdims=True), squares)
    tokens = jnp.sum(valid[...], axis=0, keepdims=True)
    squares = jnp.where(lane == 3, tokens, squares)
    over_dp[...] = jnp.zeros_like(over_dp)
    wide = column_sums.shape[1] // 128
    for k in range(wide):
        over_dp[k : k + 1, :] = column_sums[:, 128 * k : 128 * (k + 1)]
    for k in range(unit_grad.shape[1] // 128):
        over_dp[wide + k : wide + k + 1, :] = unit_grad[:, 128 * k : 128 * (k + 1)]

    def copy_to(src, dst, out, into, to):
        return pltpu.make_async_remote_copy(
            src_ref=src, dst_ref=dst, send_sem=out, recv_sem=into, device_id=to, device_id_type=MESH
        )

    def dp_copy(away):
        to = lax.rem(group + away, groups)
        return copy_to(over_dp, dp_in.at[away], sems.at[0, away], sems.at[1, away], (to, me))

    def block_copy(away):
        to = lax.rem(group + away, groups)
        src = cut.at[pl.ds(to * blocks // groups, span)]
        return copy_to(src, all_in.at[away], sems.at[2, away], sems.at[3, away], (to, me))

    def mp_copy(away):
        to = lax.rem(me + away, count)
        return copy_to(own_sum, mp_in.at[away], mp_sems.at[0, away], mp_sems.at[1, away], (group, to))

    @pl.loop(1, groups)
    def _(away):
        dp_copy(away).start()

    def send_blocks():
        for k in range(blocks):
            cut[k] = sums[:, 128 * k : 128 * (k + 1)]
            cut[k, 6:7, :] = squares

        @pl.loop(1, groups)
        def _(away):
            block_copy(away).start()

    def add_blocks():
        own_sum[...] = cut[pl.ds(group * blocks // groups, span)]

        @pl.loop(1, groups)
        def _(away):
            block_copy(away).wait_recv()
            own_sum[...] = own_sum[...] + all_in[away]

        @pl.loop(1, count)
        def _(away):
            mp_copy(away).start()

    def add_rest():
        dp_out[...] = over_dp[...]

        @pl.loop(1, groups)
        def _(away):
            dp_copy(away).wait_recv()
            dp_out[...] = dp_out[...] + dp_in[away]

        all_out[...] = own_sum[...]

        @pl.loop(1, count)
        def _(away):
            mp_copy(away).wait_recv()
            all_out[...] = all_out[...] + mp_in[away]

    def finish(piece):
        line.total(piece, acc)
        rows = line.own(piece)
        grad_in = acc[...]
        normed, rate = norm_parts(own[rows, :].astype(F32))
        result = residual_grad[rows, :] + norm_back(grad_in, vectors[0:1, :], normed, rate)
        line.share(piece, result.astype(BF16))
        sums[0:1, :] += jnp.sum(grad_in * normed, axis=0, keepdims=True)
        sums[1:2, :] += jnp.sum(grad_in, axis=0, keepdims=True)

    tiles = tiles_of(part.shape[0])

    def product(start, size, c):
        if start == 0:
            load(c // BLOCK).wait()
        part[pl.ds(start, size), c : c + BLOCK] = dot_nt(
            triple_grad[pl.ds(start, size), :], triple[c : c + BLOCK, :]
        ).astype(BF16)

    def work(start, size):
        return [functools.partial(product, start, size, c) for c in range(0, part.shape[1], BLOCK)]

    for closure in work(*tiles[0]):
        closure()
    later = [work(*tile) for tile in tiles[1:]] + [[]]
    steps = ticks(count, line.pieces)
    done = LAG * (count - 1) - 1
    drain = [[] for _ in range(steps - line.pieces)]
    drain[done].append(send_blocks)
    drain[done + 2 * LAG].append(add_blocks)
    paced(lambda step: tick(line, step, finish), tiles, steps, later, drain)
    add_rest()

    @pl.loop(0, line.pieces)
    def _(piece):
        line.settle(piece)

    @pl.loop(1, groups)
    def _(away):
        dp_copy(away).wait_send()
        block_copy(away).wait_send()

    @pl.loop(1, count)
    def _(away):
        mp_copy(away).wait_send()


def last_call(groups, count, triple_grad, weights, own, residual_grad, sums, valid, column_sums, unit_grad, vectors):
    rows, columns = triple_grad.shape
    width = weights.shape[0]
    apart = (-(-(columns + unit_grad.shape[1]) // 1024) * 8, 128)
    pieces = rows // PIECE
    blocks = width // 128
    span = max(1, blocks // groups)
    return pl.pallas_call(
        functools.partial(last_kernel, groups, count),
        name="last_line",
        out_shape=(
            jax.ShapeDtypeStruct((rows, width), BF16),
            jax.ShapeDtypeStruct((span, 8, 128), F32),
            jax.ShapeDtypeStruct(apart, F32),
        ),
        in_specs=[VMEM, ANY] + [VMEM] * 9,
        out_specs=(ANY, VMEM, VMEM),
        scratch_shapes=[
            pltpu.VMEM((width, columns), BF16),
            pltpu.SemaphoreType.DMA((width // BLOCK,)),
            pltpu.VMEM((8, width), F32),
            pltpu.VMEM(apart, F32),
            pltpu.VMEM((blocks, 8, 128), F32),
            pltpu.VMEM((groups, span, 8, 128), F32),
            pltpu.VMEM((groups, *apart), F32),
            pltpu.VMEM((span, 8, 128), F32),
            pltpu.VMEM((count, span, 8, 128), F32),
            pltpu.SemaphoreType.DMA((4, groups)),
            pltpu.SemaphoreType.DMA((2, count)),
            pltpu.VMEM((rows, width), BF16),
            pltpu.VMEM((PIECE // count, width), F32),
            *Line.scratch(count, pieces, width),
        ],
        compiler_params=params(5),
        cost_estimate=cost(115),
    )(triple_grad, weights, own, residual_grad, *sums, valid, column_sums, unit_grad, vectors)


def close_kernel(reduce_hbm, expand_hbm, first_hbm, output_hbm, hidden_hbm, *rest):
    reduce_out, expand_out, triple_out, merge_out, output_out, hidden_out = rest[:6]
    reduce, expand, first, output, hidden, reduce_wide, expand_wide, triple, merge, into, out = rest[6:]
    chunk = 256
    rows = output.shape[0]

    def copy(src, dst, sem):
        return pltpu.make_async_copy(src, dst, sem)

    ins = [
        copy(reduce_hbm, reduce, into.at[0]),
        copy(expand_hbm, expand, into.at[1]),
        copy(first_hbm, first, into.at[2]),
    ]
    outs = [
        copy(reduce_wide, reduce_out, out.at[0]),
        copy(expand_wide, expand_out, out.at[1]),
        copy(triple, triple_out, out.at[2]),
        copy(merge, merge_out, out.at[3]),
    ]
    large = []
    for k, (src, held, dst) in enumerate(((output_hbm, output, output_out), (hidden_hbm, hidden, hidden_out))):
        for start in range(0, rows, chunk):
            part = pl.ds(start, chunk)
            sem = 4 + k * (rows // chunk) + start // chunk
            large.append(
                (copy(src.at[part], held.at[part], into.at[sem]), copy(held.at[part], dst.at[part], out.at[sem]))
            )
    for one in ins:
        one.start()
    for one, _ in large:
        one.start()

    def widen(src, dst):
        step = 64

        @pl.loop(0, src.shape[0] // step)
        def _(k):
            part = block(k, step)
            dst[part, :] = src[part, :].astype(F32)

    ins[0].wait()
    widen(reduce, reduce_wide)
    outs[0].start()
    ins[1].wait()
    widen(expand, expand_wide)
    outs[1].start()
    ins[2].wait()
    wide = triple.shape[2]
    for k in range(3):
        triple[k] = first[:, k * wide : (k + 1) * wide].astype(F32)
    outs[2].start()
    merge[...] = first[:, 3 * wide :].astype(F32).T
    outs[3].start()
    for one, two in large:
        one.wait()
        two.start()
    for one in outs:
        one.wait()
    for _, two in large:
        two.wait()


def close_call(reduce_grad, expand_grad, first_grad, output, hidden_grad):
    block_rows, columns = first_grad.shape
    wide = columns // 4
    shapes = [
        (reduce_grad.shape, F32),
        (expand_grad.shape, F32),
        ((3, block_rows, wide), F32),
        ((wide, block_rows), F32),
        (output.shape, BF16),
        (hidden_grad.shape, BF16),
    ]
    ins = (reduce_grad, expand_grad, first_grad, output, hidden_grad)
    sems = 4 + 2 * (output.shape[0] // 256)
    return pl.pallas_call(
        close_kernel,
        name="close",
        out_shape=tuple(jax.ShapeDtypeStruct(*shape) for shape in shapes),
        in_specs=[ANY] * 5,
        out_specs=(ANY,) * 6,
        scratch_shapes=[
            *[pltpu.VMEM(array.shape, BF16) for array in ins],
            *[pltpu.VMEM(shape, F32) for shape, _ in shapes[:4]],
            pltpu.SemaphoreType.DMA((sems,)),
            pltpu.SemaphoreType.DMA((sems,)),
        ],
        compiler_params=pltpu.CompilerParams(vmem_limit_bytes=63 << 20),
    )(*ins)


def make_local(groups, count):
    def local(
        hidden,
        cotangent,
        lengths,
        input_gain,
        input_shift,
        triple_weight,
        triple_bias,
        merge_weight,
        merge_bias,
        middle_gain,
        middle_shift,
        expand_weight,
        expand_bias,
        reduce_weight,
        reduce_bias,
    ):
        slot = SLOT
        rows, width = hidden.shape
        head_cols = triple_weight.shape[2]
        units = expand_weight.shape[1]
        local_heads = head_cols // HEAD_DIM
        me = lax.axis_index("mp")
        slopes = 2.0 ** (
            -8.0
            * (me * local_heads + jnp.arange(local_heads, dtype=jnp.int32) + 1).astype(F32)
            / HEADS
        )
        bias_pair = triple_bias.astype(F32)
        first = jnp.concatenate([triple_weight.reshape(-1, 3 * head_cols), merge_weight.T], axis=1)
        first_full = lax.all_gather(first, "dp", axis=0, tiled=True)
        expand_full = lax.all_gather(expand_weight, "dp", axis=0, tiled=True)
        reduce_full = lax.all_gather(reduce_weight, "dp", axis=1, tiled=True)
        vectors = jnp.stack(
            [input_gain, input_shift, merge_bias, middle_gain, middle_shift, reduce_bias]
        )
        vectors = lax.all_gather(vectors, "dp", axis=1, tiled=True).astype(F32)
        vectors = jnp.pad(vectors, ((0, 2), (0, 0)))

        def own_rows(array):
            pieces = array.reshape(rows // PIECE, count, PIECE // count, -1)
            mine = lax.dynamic_index_in_dim(pieces, me, axis=1, keepdims=False)
            return mine.reshape(rows // count, -1)

        valid = (jnp.arange(slot, dtype=jnp.int32)[None, :] < lengths[:, None]).reshape(rows, 1)
        own = own_rows(hidden)
        own_valid = own_rows(valid.astype(F32))
        grad_feed = jnp.where(valid, cotangent, jnp.zeros((), BF16))
        own_grad = own_rows(grad_feed)

        normed, _ = norm_parts(hidden.astype(F32))
        norm_in = (normed * vectors[0] + vectors[1]).astype(BF16)
        seats = jnp.arange(rows, dtype=jnp.int32)
        segment = seats // slot
        places = lax.rem(seats, slot).astype(F32)
        as_key = jnp.where(valid[:, 0], segment, -1)
        as_query = jnp.where(valid[:, 0], segment, -2)
        segments = (
            as_query[:, None],
            as_key[None, :],
            places[None, :],
            as_query[None, :],
            as_key[:, None],
            places[:, None],
        )
        shift = jnp.concatenate([bias_pair[0], jnp.zeros_like(bias_pair[0]), bias_pair[1]])[None]
        norm_mid, residual, sums_one, qkv, mixed, totals = front_call(
            count, slopes, norm_in, first_full, shift, own, own_valid, segments, vectors
        )
        branch_grad, residual_grad, sums_two, unit_grad, feed_part, expand_grad, reduce_grad = (
            feed_call(
                count,
                norm_mid,
                expand_full,
                reduce_full,
                grad_feed,
                residual,
                own_grad,
                expand_bias.astype(F32)[None],
                vectors,
            )
        )

        def scatter(array, dim):
            return lax.psum_scatter(array, "dp", scatter_dimension=dim, tiled=True)

        reduce_grad = scatter(reduce_grad, 1)
        expand_grad = scatter(expand_grad, 0)
        grad_triple, column_sums, output, sums_three, first_grad = back_call(
            count,
            slopes,
            branch_grad,
            first_full,
            qkv,
            mixed,
            norm_in,
            totals,
            segments,
            feed_part,
            residual,
            own_valid,
            vectors,
        )
        first_grad = scatter(first_grad, 0)
        hidden_grad, small, dp_small = last_call(
            groups,
            count,
            grad_triple,
            first_full,
            own,
            residual_grad,
            (sums_one, sums_two, sums_three),
            own_valid,
            column_sums,
            unit_grad,
            vectors,
        )
        reduce_grad, expand_grad, triple_grad, merge_grad, output, hidden_grad = close_call(
            reduce_grad, expand_grad, first_grad, output, hidden_grad
        )
        share = width // groups
        small = small.transpose(1, 0, 2).reshape(8, -1)
        totals = small[6, :4]
        if share < 128:
            place = lax.rem(lax.axis_index("dp") * share, 128)
            small = lax.dynamic_slice_in_dim(small, place, share, axis=1)
        flat = dp_small.reshape(-1)
        triple_sums = flat[: 3 * head_cols]
        unit_sums = flat[3 * head_cols : 3 * head_cols + units]
        root_means = jnp.sqrt(totals[:3] / (totals[3] * width))
        pair_grad = jnp.stack([triple_sums[:head_cols], triple_sums[2 * head_cols :]])
        return (
            output,
            hidden_grad,
            small[0],
            small[1],
            triple_grad.transpose(1, 0, 2),
            pair_grad,
            merge_grad,
            small[2],
            small[3],
            small[4],
            expand_grad,
            unit_sums,
            reduce_grad,
            small[5],
            root_means,
        )

    return local


def solution(mesh):
    local = make_local(mesh.shape["dp"], mesh.shape["mp"])

    return jax.shard_map(
        local,
        mesh=mesh,
        in_specs=(
            P("dp", None),
            P("dp", None),
            P("dp"),
            P("dp"),
            P("dp"),
            P("dp", None, "mp"),
            P(None, "mp"),
            P("mp", "dp"),
            P("dp"),
            P("dp"),
            P("dp"),
            P("dp", "mp"),
            P("mp"),
            P("mp", "dp"),
            P("dp"),
        ),
        out_specs=(
            P("dp", None),
            P("dp", None),
            P("dp"),
            P("dp"),
            P("dp", None, "mp"),
            P(None, "mp"),
            P("mp", "dp"),
            P("dp"),
            P("dp"),
            P("dp"),
            P("dp", "mp"),
            P("mp"),
            P("mp", "dp"),
            P("dp"),
            P(),
        ),
        check_vma=False,
    )
```

```python
import functools

import jax
import jax.numpy as jnp
from jax import lax
from jax.experimental import pallas as pl
from jax.experimental.layout import Layout, with_layout_constraint
from jax.experimental.pallas import tpu as pltpu
from jax.sharding import PartitionSpec as P

HEADS = 32
HEAD_DIM = 64
SLOT = 512
PIECE = 64
TILE = 256
BLOCK = 512
F32 = jnp.float32
BF16 = jnp.bfloat16
MESH = pl.DeviceIdType.MESH
VMEM = pl.BlockSpec(memory_space=pltpu.VMEM)
ANY = pl.BlockSpec(memory_space=pl.ANY)


def dot32(a, b):
    return jnp.dot(a, b, preferred_element_type=F32)


def dot_nt(a, b):
    return lax.dot_general(a, b, (((1,), (1,)), ((), ())), preferred_element_type=F32)


def dot_tn(a, b):
    return lax.dot_general(a, b, (((0,), (0,)), ((), ())), preferred_element_type=F32)


def norm_parts(values):
    center = values - jnp.mean(values, axis=-1, keepdims=True)
    spread = jnp.mean(center * center, axis=-1, keepdims=True)
    rate = lax.rsqrt(spread + 1e-05)
    return center * rate, rate


def norm_back(grad, gain, normed, rate):
    scaled = grad * gain
    first = jnp.mean(scaled, axis=-1, keepdims=True)
    second = jnp.mean(scaled * normed, axis=-1, keepdims=True)
    return rate * (scaled - first - normed * second)


def block(index, size):
    return pl.ds(pl.multiple_of(index * size, size), size)


def greet(count):
    me, group = lax.axis_index("mp"), lax.axis_index("dp")
    barrier = pltpu.get_barrier_semaphore()

    @pl.when(me < count - 1)
    def _():
        pl.semaphore_signal(barrier, inc=1, device_id=(group, me + 1), device_id_type=MESH)

    @pl.when(me > 0)
    def _():
        pl.semaphore_signal(barrier, inc=1, device_id=(group, me - 1), device_id_type=MESH)

    peers = jnp.where(me > 0, 1, 0) + jnp.where(me < count - 1, 1, 0)
    pl.semaphore_wait(barrier, peers)


LAG = 1


class Line:
    def __init__(self, count, part, result, inbox, extra, *sems):
        self.count, self.part, self.inbox, self.extra, self.result = count, part, inbox, extra, result
        self.pieces = part.shape[0] // PIECE
        self.sum_out, self.sum_in, self.extra_in, self.own_out, self.all_out, self.all_in, self.flushed = sems
        self.rows = PIECE // count
        self.me, self.group = lax.axis_index("mp"), lax.axis_index("dp")

    @staticmethod
    def scratch(count, pieces, width):
        rows = PIECE // count
        return [
            pltpu.VMEM((pieces * PIECE, width), BF16),
            pltpu.VMEM((pieces * rows, width), BF16),
            pltpu.SemaphoreType.DMA((pieces, count)),
            pltpu.SemaphoreType.DMA((pieces, count)),
            pltpu.SemaphoreType.DMA((pieces,)),
            pltpu.SemaphoreType.DMA((pieces,)),
            pltpu.SemaphoreType.DMA((pieces, count)),
            pltpu.SemaphoreType.DMA((pieces, count)),
            pltpu.SemaphoreType.DMA((pieces,)),
        ]

    def at(self, piece, owner):
        return pl.ds(pl.multiple_of(piece * PIECE + owner * self.rows, self.rows), self.rows)

    def own(self, piece):
        return block(piece, self.rows)

    def copy(self, src, dst, out, into, to):
        return pltpu.make_async_remote_copy(
            src_ref=src,
            dst_ref=dst,
            send_sem=out,
            recv_sem=into,
            device_id=(self.group, to),
            device_id_type=MESH,
        )

    def sum_copy(self, piece, owner, to):
        rows = self.at(piece, owner)
        return self.copy(
            self.part.at[rows],
            self.inbox.at[rows],
            self.sum_out.at[piece, owner],
            self.sum_in.at[piece, owner],
            to,
        )

    def extra_copy(self, piece, owner, to):
        return self.copy(
            self.part.at[self.at(piece, owner)],
            self.extra.at[self.own(piece)],
            self.sum_out.at[piece, owner],
            self.extra_in.at[piece],
            to,
        )

    def all_copy(self, piece, owner, to, own_left=False):
        rows = self.at(piece, owner)
        return self.copy(
            self.inbox.at[rows],
            self.inbox.at[rows],
            self.own_out.at[piece] if own_left else self.all_out.at[piece, owner],
            self.all_in.at[piece, owner],
            to,
        )

    def add(self, piece, owner):
        rows = self.at(piece, owner)
        self.sum_copy(piece, owner, self.me).wait_recv()
        self.part[rows, :] = (
            self.part[rows, :].astype(F32) + self.inbox[rows, :].astype(F32)
        ).astype(BF16)

    def send_right(self, piece):
        me, last = self.me, self.count - 1
        for owner in range(last, 0, -1):

            @pl.when(me < owner)
            def _(owner=owner):
                @pl.when(me > 0)
                def _():
                    self.add(piece, owner)

                self.sum_copy(piece, owner, me + 1).start()

    def send_left(self, piece):
        me, last = self.me, self.count - 1
        for owner in range(last):

            @pl.when(me > owner)
            def _(owner=owner):
                @pl.when(me < last)
                def _():
                    self.add(piece, owner)

                @pl.when(me == owner + 1)
                def _():
                    self.extra_copy(piece, owner, me - 1).start()

                @pl.when(me > owner + 1)
                def _():
                    self.sum_copy(piece, owner, me - 1).start()

    def total(self, piece, acc):
        me, rows = self.me, self.at(piece, self.me)
        acc[...] = self.part[rows, :].astype(F32)

        @pl.when(me > 0)
        def _():
            self.sum_copy(piece, me, me).wait_recv()
            acc[...] = acc[...] + self.inbox[rows, :].astype(F32)

        @pl.when(me < self.count - 1)
        def _():
            self.extra_copy(piece, me, me).wait_recv()
            acc[...] = acc[...] + self.extra[self.own(piece), :].astype(F32)

    def share(self, piece, values):
        me = self.me
        self.inbox[self.at(piece, me), :] = values

        @pl.when(me < self.count - 1)
        def _():
            self.all_copy(piece, me, me + 1).start()

        @pl.when(me > 0)
        def _():
            self.all_copy(piece, me, me - 1, own_left=True).start()

    def forward(self, piece, away):
        me, last = self.me, self.count - 1

        @pl.when(me >= away)
        def _(owner=me - away):
            self.all_copy(piece, owner, me).wait_recv()

            @pl.when(me < last)
            def _():
                self.all_copy(piece, owner, me + 1).start()

        @pl.when(me + away <= last)
        def _(owner=me + away):
            self.all_copy(piece, owner, me).wait_recv()

            @pl.when(me > 0)
            def _():
                self.all_copy(piece, owner, me - 1).start()

    def flush_copy(self, piece):
        rows = block(piece, PIECE)
        return pltpu.make_async_copy(self.inbox.at[rows], self.result.at[rows], self.flushed.at[piece])

    def flush(self, piece):
        self.flush_copy(piece).start()

    def settle(self, piece):
        me, last = self.me, self.count - 1
        self.flush_copy(piece).wait()
        for owner in range(self.count):

            @pl.when(me != owner)
            def _():
                self.sum_copy(piece, owner, me).wait_send()

            @pl.when(jnp.logical_or(jnp.logical_and(me >= owner, me < last), jnp.logical_and(me < owner, me > 0)))
            def _():
                self.all_copy(piece, owner, me).wait_send()

        @pl.when(me > 0)
        def _():
            self.all_copy(piece, me, me, own_left=True).wait_send()


def tick(line, step, finish):
    def when(piece, work, *more):
        @pl.when(jnp.logical_and(piece >= 0, piece < line.pieces))
        def _():
            work(piece, *more)

    last = line.count - 1
    when(step - LAG * line.me, line.send_right)
    when(step - LAG * (last - line.me), line.send_left)
    when(step - LAG * last, finish)
    for away in range(1, line.count):
        when(step - LAG * (last + away), line.forward, away)
    when(step - LAG * 2 * last, line.flush)


def ticks(count, pieces):
    return pieces + 2 * LAG * (count - 1)


def cost(micros):
    return pl.CostEstimate(flops=int(micros * 1e9), bytes_accessed=1 << 20, transcendentals=0)


def params(index, variant):
    return pltpu.CompilerParams(
        collective_id=8 * variant + index, has_side_effects=True, vmem_limit_bytes=63 << 20
    )


def tiles_of(rows):
    return [(start, min(TILE, rows - start)) for start in range(0, rows, TILE)]


def spread(work, parts):
    return [work[len(work) * k // parts : len(work) * (k + 1) // parts] for k in range(parts)]


def paced(line_tick, tiles, steps, later, drain):
    step = 0
    plans = [spread(work, size // PIECE) for (_, size), work in zip(tiles, later)]
    assert len(later) == len(tiles) and len(drain) == steps - sum(map(len, plans))
    for shares in (*plans, drain):
        span = len(shares)

        @pl.loop(0, span)
        def _(k, step=step, shares=shares):
            line_tick(step + k)
            for phase, share in enumerate(shares):
                if share:

                    @pl.when(k == phase)
                    def _(share=share):
                        for closure in share:
                            closure()

        step += span


def halves(values):
    low = lax.broadcasted_iota(jnp.int32, values.shape, 1) < HEAD_DIM
    zero = jnp.zeros((), values.dtype)
    return jnp.where(low, values, zero), jnp.where(low, zero, values)


PAIR = 2 * HEAD_DIM


def front_kernel(
    count, head_cols, slopes, norm_hbm, weights_hbm, shift, own, valid, segment_col, segment_row, place_row, vectors,
    middle, residual, sums, qkv_hbm, mixed_hbm, totals,
    norm_in, weights, qkv, mixed, load_sem, save_sem, part, acc, mask, *rest,
):
    line = Line(count, part, middle, *rest)
    rows_all, width = norm_in.shape
    tiles = tiles_of(rows_all)
    blocks = weights.shape[1] // BLOCK

    def load_rows(k):
        rows = pl.ds(tiles[k][0], tiles[k][1])
        return pltpu.make_async_copy(norm_hbm.at[rows], norm_in.at[rows], load_sem.at[0, k])

    def load_columns(k):
        cols = block(k, BLOCK)
        return pltpu.make_async_copy(weights_hbm.at[:, cols], weights.at[:, cols], load_sem.at[1, k])

    load_rows(0).start()
    for k in range(blocks):
        load_columns(k).start()
    for k in range(1, len(tiles)):
        load_rows(k).start()
    greet(count)
    sums[...] = jnp.zeros_like(sums)

    def finish(piece):
        line.total(piece, acc)
        rows = line.own(piece)
        branch = acc[...] + vectors[2:3, :]
        result = own[rows, :].astype(F32) + branch
        residual[rows, :] = result
        normed, _ = norm_parts(result)
        line.share(piece, (normed * vectors[3:4, :] + vectors[4:5, :]).astype(BF16))
        sums[0:1, :] += jnp.sum(branch * branch * valid[rows, :], axis=0, keepdims=True)

    def project(start, size):
        rows = pl.ds(start, size)
        load_rows(start // TILE).wait()

        @pl.loop(0, 3 * head_cols // BLOCK)
        def _(k):
            cols = block(k, BLOCK)
            if start == 0:
                load_columns(k).wait()
            qkv[rows, cols] = (dot32(norm_in[rows, :], weights[:, cols]) + shift[:, cols]).astype(BF16)

    def masks(start, size):
        keys = start + size
        row = lax.broadcasted_iota(jnp.int32, (size, keys), 0) + start
        col = lax.broadcasted_iota(jnp.int32, (size, keys), 1)
        same = segment_col[start : start + size, :] == segment_row[:, :keys]
        mask[:size, :keys] = jnp.where(jnp.logical_and(same, col <= row), 1.0, 0.0)

    def attend(start, size, pair):
        keys = start + size
        query = halves(qkv[pl.ds(start, size), block(pair, PAIR)])
        key = qkv[:keys, pl.ds(pl.multiple_of(head_cols + pair * PAIR, PAIR), PAIR)]
        value = halves(qkv[:keys, pl.ds(pl.multiple_of(2 * head_cols + pair * PAIR, PAIR), PAIR)])
        out = jnp.zeros((size, PAIR), F32)
        sums_log = jnp.zeros((size, 128), F32)
        lane = lax.broadcasted_iota(jnp.int32, (size, 128), 1)
        for k in range(2):
            scores = dot_nt(query[k], key) + slopes[2 * pair + k] * place_row[:, :keys]
            scores = jnp.where(mask[:size, :keys] > 0.5, scores * 0.125, -1000000000.0)
            most = jnp.max(scores, axis=1, keepdims=True)
            raised = jnp.exp(scores - most)
            total = jnp.sum(raised, axis=1, keepdims=True)
            out = out + dot32((raised * (1.0 / total)).astype(BF16), value[k])
            sums_log = jnp.where(lane == k, most + jnp.log(total), sums_log)
        totals[2 * pair : 2 * pair + 2, start : start + size] = sums_log.T[:2, :]
        mixed[pl.ds(start, size), block(pair, PAIR)] = out.astype(BF16)

    def project_back(start, size):
        rows = pl.ds(start, size)
        if start == 0:
            for k in range(3 * head_cols // BLOCK, blocks):
                load_columns(k).wait()

        @pl.loop(0, width // BLOCK)
        def _(k):
            cols = block(k, BLOCK)
            part[rows, cols] = dot_nt(mixed[rows, :], weights[cols, 3 * head_cols :]).astype(BF16)

    pairs = head_cols // PAIR

    def work(start, size):
        return [
            functools.partial(project, start, size),
            functools.partial(masks, start, size),
            *[functools.partial(attend, start, size, pair) for pair in range(pairs)],
            functools.partial(project_back, start, size),
        ]

    saves = (
        pltpu.make_async_copy(qkv, qkv_hbm, save_sem.at[0]),
        pltpu.make_async_copy(mixed, mixed_hbm, save_sem.at[1]),
    )

    def save():
        for copy in saves:
            copy.start()

    for closure in work(*tiles[0]):
        closure()
    later = [work(*tile) for tile in tiles[1:]] + [[save]]
    steps = ticks(count, line.pieces)
    drain = [[]] * (steps - line.pieces)
    paced(lambda step: tick(line, step, finish), tiles, steps, later, drain)
    for copy in saves:
        copy.wait()

    @pl.loop(0, line.pieces)
    def _(piece):
        line.settle(piece)


SMEM = pl.BlockSpec(memory_space=pltpu.SMEM)


def front_call(count, rows, variant, slopes, norm_in, weights, shift, own, valid, segments, vectors):
    width = norm_in.shape[1]
    head_cols = weights.shape[1] // 4
    pieces = rows // PIECE
    return pl.pallas_call(
        functools.partial(front_kernel, count, head_cols),
        name="front_line",
        out_shape=(
            jax.ShapeDtypeStruct((rows, width), BF16),
            jax.ShapeDtypeStruct((rows // count, width), F32),
            jax.ShapeDtypeStruct((8, width), F32),
            jax.ShapeDtypeStruct((rows, 3 * head_cols), BF16),
            jax.ShapeDtypeStruct((rows, head_cols), BF16),
            jax.ShapeDtypeStruct((head_cols // HEAD_DIM, rows), F32),
        ),
        in_specs=[SMEM] + [ANY] * 2 + [VMEM] * 7,
        out_specs=(ANY, VMEM, VMEM, ANY, ANY, VMEM),
        scratch_shapes=[
            pltpu.VMEM((rows, width), BF16),
            pltpu.VMEM(weights.shape, BF16),
            pltpu.VMEM((rows, 3 * head_cols), BF16),
            pltpu.VMEM((rows, head_cols), BF16),
            pltpu.SemaphoreType.DMA((2, max(len(tiles_of(rows)), weights.shape[1] // BLOCK))),
            pltpu.SemaphoreType.DMA((2,)),
            pltpu.VMEM((rows, width), BF16),
            pltpu.VMEM((PIECE // count, width), F32),
            pltpu.VMEM((TILE, rows), F32),
            *Line.scratch(count, pieces, width),
        ],
        compiler_params=params(1, variant),
        cost_estimate=cost(120),
    )(slopes, norm_in, weights, shift, own, valid, *segments[:3], vectors)


def feed_kernel(
    count, pieces, middle_hbm, expand_hbm, reduce_hbm, grad_hbm, residual, own_grad, unit_shift, vectors,
    branch_grad, residual_grad, sums, unit_grad, feed_hbm, expand_grad, reduce_grad,
    middle, expand, reduce, grad, active, pre_grad, part, acc, stage, load_sem, stage_sem, *rest,
):
    line = Line(count, part, branch_grad, *rest)
    units = expand.shape[1]
    width = expand.shape[0]
    blocks = units // BLOCK

    def load(k):
        cols = block(k, BLOCK)
        return (
            pltpu.make_async_copy(expand_hbm.at[:, cols], expand.at[:, cols], load_sem.at[0, k]),
            pltpu.make_async_copy(reduce_hbm.at[cols], reduce.at[cols], load_sem.at[1, k]),
        )

    tiles = tiles_of(middle.shape[0])

    def load_rows(k):
        rows = pl.ds(tiles[k][0], tiles[k][1])
        return (
            pltpu.make_async_copy(middle_hbm.at[rows], middle.at[rows], load_sem.at[2, k]),
            pltpu.make_async_copy(grad_hbm.at[rows], grad.at[rows], load_sem.at[3, k]),
        )

    for copy in (*load_rows(0), *load(0)):
        copy.start()
    for k in range(1, blocks):
        for copy in load(k):
            copy.start()
    for k in range(1, len(tiles)):
        for copy in load_rows(k):
            copy.start()
    greet(count)
    sums[...] = jnp.zeros_like(sums)
    unit_grad[...] = jnp.zeros_like(unit_grad)

    def finish(piece):
        line.total(piece, acc)
        rows = line.own(piece)
        grad_mid = acc[...]
        normed, rate = norm_parts(residual[rows, :])
        grad_out = own_grad[rows, :].astype(F32)
        result = grad_out + norm_back(grad_mid, vectors[3:4, :], normed, rate)
        residual_grad[rows, :] = result
        low = result.astype(BF16)
        line.share(piece, low)
        for k, values in enumerate((low.astype(F32), grad_mid * normed, grad_mid, grad_out)):
            sums[k : k + 1, :] += jnp.sum(values, axis=0, keepdims=True)

    def forward(start, size, low_k, high_k):
        rows = pl.ds(start, size)
        if low_k == 0:
            for copy in load_rows(start // TILE):
                copy.wait()

        @pl.loop(low_k, high_k)
        def _(k):
            cols = block(k, BLOCK)
            if start == 0:
                for copy in load(k):
                    copy.wait()
            pre = dot32(middle[rows, :], expand[:, cols]) + unit_shift[:, cols]
            half = 0.5 + 0.5 * lax.erf(pre * 0.7071067811865476)
            slope = half + pre * (0.3989422804014327 * jnp.exp(-0.5 * pre * pre))
            active[rows, cols] = (pre * half).astype(BF16)
            low = (dot_nt(grad[rows, :], reduce[cols, :]) * slope).astype(BF16)
            pre_grad[rows, cols] = low
            unit_grad[:, cols] += jnp.sum(low.astype(F32), axis=0, keepdims=True)

    def backward(start, size, low_k, high_k):
        rows = pl.ds(start, size)

        @pl.loop(low_k, high_k)
        def _(k):
            cols = block(k, BLOCK)
            part[rows, cols] = dot_nt(pre_grad[rows, :], expand[cols, :]).astype(BF16)

    staged = {"rows": 0}

    def settle_slot(slot):
        rows = pl.ds(0, staged["rows"])
        pltpu.make_async_copy(
            stage.at[slot, rows], feed_hbm.at[rows, pl.ds(0, BLOCK)], stage_sem.at[slot]
        ).wait()

    def emit(target, start, size, product):
        before = staged["rows"]

        @pl.loop(0, target.shape[1] // BLOCK)
        def _(k):
            slot = lax.rem(k, 4)
            if before:
                settle_slot(slot)
            stage[slot, :size, :] = product(block(k, BLOCK)).astype(BF16)
            pltpu.make_async_copy(
                stage.at[slot, pl.ds(0, size)],
                target.at[pl.ds(start, size), block(k, BLOCK)],
                stage_sem.at[slot],
            ).start()

        staged["rows"] = size

    def feed_product(start, size):
        emit(feed_hbm, start, size, lambda cols: dot32(active[pl.ds(start, size), :], reduce[:, cols]))

    def reduce_product(start):
        emit(reduce_grad, start, BLOCK, lambda cols: dot_tn(active[:, pl.ds(start, BLOCK)], grad[:, cols]))

    def expand_product(start):
        emit(expand_grad, start, BLOCK, lambda cols: dot_tn(middle[:, pl.ds(start, BLOCK)], pre_grad[:, cols]))

    backs = width // BLOCK
    assert backs == 4 and blocks == 4

    def work(start, size):
        return [
            functools.partial(forward, start, size, 0, blocks // 2),
            functools.partial(forward, start, size, blocks // 2, blocks),
            functools.partial(backward, start, size, 0, backs // 2),
            functools.partial(backward, start, size, backs // 2, backs),
        ]

    for closure in work(*tiles[0]):
        closure()
    later = [
        [*work(*after), functools.partial(feed_product, *tile)] for tile, after in zip(tiles, tiles[1:])
    ]
    products = [functools.partial(reduce_product, r) for r in range(0, units, BLOCK)]
    products += [functools.partial(expand_product, r) for r in range(0, width, BLOCK)]
    steps = ticks(count, pieces)
    beside = tiles[-1][1] // PIECE
    taken = len(products) * beside // (steps - pieces + beside)
    later.append([functools.partial(feed_product, *tiles[-1]), *products[:taken]])
    drain = spread(products[taken:], steps - pieces)
    paced(lambda step: tick(line, step, finish), tiles, steps, later, drain)
    for slot in range(4):
        settle_slot(slot)

    @pl.loop(0, pieces)
    def _(piece):
        line.settle(piece)


def feed_call(count, variant, middle, expand, reduce, grad, residual, own_grad, unit_shift, vectors):
    rows, width = middle.shape
    units = expand.shape[1]
    pieces = rows // PIECE
    most = max(units // BLOCK, len(tiles_of(rows)))
    return pl.pallas_call(
        functools.partial(feed_kernel, count, pieces),
        name="feed_line",
        out_shape=(
            jax.ShapeDtypeStruct((rows, width), BF16),
            jax.ShapeDtypeStruct((rows // count, width), F32),
            jax.ShapeDtypeStruct((8, width), F32),
            jax.ShapeDtypeStruct((1, units), F32),
            jax.ShapeDtypeStruct((rows, width), BF16),
            jax.ShapeDtypeStruct((width, units), BF16),
            jax.ShapeDtypeStruct((units, width), BF16),
        ),
        in_specs=[ANY] * 4 + [VMEM] * 4,
        out_specs=(ANY,) + (VMEM,) * 3 + (ANY,) * 3,
        scratch_shapes=[
            pltpu.VMEM((rows, width), BF16),
            pltpu.VMEM((width, units), BF16),
            pltpu.VMEM((units, width), BF16),
            pltpu.VMEM((rows, width), BF16),
            pltpu.VMEM((rows, units), BF16),
            pltpu.VMEM((rows, units), BF16),
            pltpu.VMEM((rows, width), BF16),
            pltpu.VMEM((PIECE // count, width), F32),
            pltpu.VMEM((4, BLOCK, BLOCK), BF16),
            pltpu.SemaphoreType.DMA((4, most)),
            pltpu.SemaphoreType.DMA((4,)),
            *Line.scratch(count, pieces, width),
        ],
        compiler_params=params(2, variant),
        cost_estimate=cost(130),
    )(middle, expand, reduce, grad, residual, own_grad, unit_shift, vectors)


def back_kernel(
    count, head_cols, slopes, branch_hbm, merge, qkv, mixed, norm_hbm, totals, segment_col, segment_row, place_col,
    feed_hbm, residual_hbm, valid, vectors,
    triple_grad, column_sums, output, sums, weight_out,
    branch_grad, norm_in, feed, residual, load_sem, save_sem,
    mixed_grad, key_grad, value_grad, acc, mask, stage, stage_sem, *rest,
):
    line = Line(count, feed, output, *rest)
    rows_all, width = branch_grad.shape
    tiles = tiles_of(rows_all)

    def load_feed(k):
        rows = pl.ds(tiles[k][0], tiles[k][1])
        return pltpu.make_async_copy(feed_hbm.at[rows], feed.at[rows], load_sem.at[0, k])

    def load_grad(k):
        rows = pl.ds(tiles[k][0], tiles[k][1])
        return pltpu.make_async_copy(branch_hbm.at[rows], branch_grad.at[rows], load_sem.at[1, k])

    load_residual = pltpu.make_async_copy(residual_hbm, residual, load_sem.at[2, 0])
    load_norm = pltpu.make_async_copy(norm_hbm.at[pl.ds(0, rows_all)], norm_in, load_sem.at[2, 1])
    load_feed(0).start()
    load_grad(len(tiles) - 1).start()
    load_residual.start()
    for k in range(1, len(tiles)):
        load_feed(k).start()
        load_grad(len(tiles) - 1 - k).start()
    load_norm.start()
    greet(count)
    load_feed(0).wait()
    load_residual.wait()
    sums[...] = jnp.zeros_like(sums)
    column_sums[...] = jnp.zeros_like(column_sums)

    def finish(piece):
        line.total(piece, acc)
        rows = line.own(piece)
        branch = acc[...] + vectors[5:6, :]
        keep = valid[rows, :] > 0.5
        result = jnp.where(keep, residual[rows, :] + branch, 0.0)
        line.share(piece, result.astype(BF16))
        branch = jnp.where(keep, branch, 0.0)
        sums[0:1, :] += jnp.sum(result * result, axis=0, keepdims=True)
        sums[1:2, :] += jnp.sum(branch * branch, axis=0, keepdims=True)

    def open_tile(start, size):
        rows = pl.ds(start, size)
        load_grad(start // TILE).wait()
        mixed_grad[rows, :] = dot32(branch_grad[rows, :], merge[...]).astype(BF16)
        keys = start + size
        row = lax.broadcasted_iota(jnp.int32, (keys, size), 1) + start
        col = lax.broadcasted_iota(jnp.int32, (keys, size), 0)
        same = segment_row[:keys, :] == segment_col[:, start : start + size]
        mask[:keys, :size] = jnp.where(jnp.logical_and(same, col <= row), 1.0, 0.0)

    def back(start, size, first, pair):
        keys = start + size
        rows, cols = pl.ds(start, size), block(pair, PAIR)
        query = halves(qkv[rows, cols])
        key = qkv[:keys, pl.ds(pl.multiple_of(head_cols + pair * PAIR, PAIR), PAIR)]
        value = qkv[:keys, pl.ds(pl.multiple_of(2 * head_cols + pair * PAIR, PAIR), PAIR)]
        grad = halves(mixed_grad[rows, cols])
        keys_apart = halves(key)
        query_grad = jnp.zeros((size, PAIR), F32)
        key_sum = jnp.zeros((keys, PAIR), F32)
        value_sum = jnp.zeros((keys, PAIR), F32)
        for k in range(2):
            scores = dot_nt(key, query[k]) + slopes[2 * pair + k] * place_col[:keys, :]
            scores = jnp.where(mask[:keys, :size] > 0.5, scores * 0.125, -1000000000.0)
            soft = jnp.exp(scores - totals[2 * pair + k : 2 * pair + k + 1, rows])
            grad_probs = dot_nt(value, grad[k])
            row_terms = jnp.sum(soft * grad_probs, axis=0, keepdims=True)
            grad_scores = (soft * (grad_probs - row_terms)).astype(BF16)
            value_sum = value_sum + dot32(soft.astype(BF16), grad[k])
            key_sum = key_sum + dot32(grad_scores, query[k])
            query_grad = query_grad + dot_tn(grad_scores, keys_apart[k])
        triple_grad[rows, cols] = (0.125 * query_grad).astype(BF16)
        if first:
            key_grad[:keys, cols] = key_sum
            value_grad[:keys, cols] = value_sum
        else:
            key_grad[:keys, cols] += key_sum
            value_grad[:keys, cols] += value_sum

    def close_tile(start, size):
        rows = pl.ds(start, size)
        triple_grad[rows, head_cols : 2 * head_cols] = (0.125 * key_grad[rows, :]).astype(BF16)
        triple_grad[rows, 2 * head_cols :] = value_grad[rows, :].astype(BF16)
        column_sums[...] += jnp.sum(triple_grad[rows, :].astype(F32), axis=0, keepdims=True)

    def put(slot, target):
        return pltpu.make_async_copy(stage.at[slot], target, stage_sem.at[slot])

    def job(index, left, right, r, c, shift):
        slot = index % 2
        r, c, to = pl.ds(r, BLOCK), pl.ds(c, BLOCK), pl.ds(c + shift, BLOCK)
        if index >= 2:
            put(slot, weight_out.at[r, to]).wait()
        stage[slot] = dot_tn(left[:, r], right[:, c]).astype(BF16)
        put(slot, weight_out.at[r, to]).start()

    pairs = head_cols // PAIR

    def work(start, size, first):
        return [
            functools.partial(open_tile, start, size),
            *[functools.partial(back, start, size, first, pair) for pair in range(pairs)],
            functools.partial(close_tile, start, size),
        ]

    products = [
        (branch_grad, mixed, r, c, 3 * head_cols)
        for r in range(0, width, BLOCK)
        for c in range(0, head_cols, BLOCK)
    ] + [
        (norm_in, triple_grad, r, c, 0)
        for r in range(0, width, BLOCK)
        for c in range(0, 3 * head_cols, BLOCK)
    ]
    jobs = [functools.partial(job, k, *product) for k, product in enumerate(products)]
    later = [work(*tile, k == 0) for k, tile in enumerate(reversed(tiles))]
    for k in range(1, len(tiles)):
        later[k - 1].append(lambda k=k: load_feed(k).wait())
    later[-1].append(load_norm.wait)
    steps = ticks(count, line.pieces)
    drain = spread(jobs, steps - line.pieces)
    paced(lambda step: tick(line, step, finish), tiles, steps, later, drain)
    for slot in range(2):
        put(slot, weight_out.at[pl.ds(0, BLOCK), pl.ds(0, BLOCK)]).wait()

    @pl.loop(0, line.pieces)
    def _(piece):
        line.settle(piece)


def back_call(count, whole, variant, slopes, branch_grad, weights, qkv, mixed, norm_in, totals, segments, feed, residual, valid, vectors):
    rows, width = branch_grad.shape
    head_cols = weights.shape[1] // 4
    merge_spec = pl.BlockSpec((width, head_cols), lambda i: (0, 3), memory_space=pltpu.VMEM)
    pieces = rows // PIECE
    return pl.pallas_call(
        functools.partial(back_kernel, count, head_cols),
        name="back_line",
        out_shape=(
            jax.ShapeDtypeStruct((rows, 3 * head_cols), BF16),
            jax.ShapeDtypeStruct((1, 3 * head_cols), F32),
            jax.ShapeDtypeStruct((whole, width), BF16),
            jax.ShapeDtypeStruct((8, width), F32),
            jax.ShapeDtypeStruct((width, 4 * head_cols), BF16),
        ),
        grid=(1,),
        in_specs=[SMEM, ANY, merge_spec, VMEM, VMEM, ANY] + [VMEM] * 4 + [ANY] * 2 + [VMEM] * 2,
        out_specs=(VMEM, VMEM, ANY, VMEM, ANY),
        scratch_shapes=[
            pltpu.VMEM((rows, width), BF16),
            pltpu.VMEM((rows, width), BF16),
            pltpu.VMEM((rows, width), BF16),
            pltpu.VMEM((rows // count, width), F32),
            pltpu.SemaphoreType.DMA((3, max(2, len(tiles_of(rows))))),
            pltpu.SemaphoreType.DMA((2,)),
            pltpu.VMEM((rows, head_cols), BF16),
            pltpu.VMEM((rows, head_cols), F32),
            pltpu.VMEM((rows, head_cols), F32),
            pltpu.VMEM((PIECE // count, width), F32),
            pltpu.VMEM((rows, TILE), F32),
            pltpu.VMEM((2, BLOCK, BLOCK), BF16),
            pltpu.SemaphoreType.DMA((2,)),
            *Line.scratch(count, pieces, width),
        ],
        compiler_params=params(3, variant),
        cost_estimate=cost(120),
    )(slopes, branch_grad, weights, qkv, mixed, norm_in, totals, *segments[3:], feed, residual, valid, vectors)


def greet_all(groups, count):
    me, group = lax.axis_index("mp"), lax.axis_index("dp")
    barrier = pltpu.get_barrier_semaphore()

    @pl.loop(1, groups)
    def _(away):
        to = lax.rem(group + away, groups)
        pl.semaphore_signal(barrier, inc=1, device_id=(to, me), device_id_type=MESH)

    @pl.loop(1, count)
    def _(away):
        to = lax.rem(me + away, count)
        pl.semaphore_signal(barrier, inc=1, device_id=(group, to), device_id_type=MESH)

    pl.semaphore_wait(barrier, groups + count - 2)


def last_kernel(
    groups, count, triple_grad, triple_hbm, own, residual_grad, front_sums, feed_sums, back_sums, valid,
    column_sums, unit_grad, vectors, first_hbm,
    hidden_grad, all_out, dp_out, first_out,
    mine, theirs, others, pair_sems, chip_sems,
    triple, load_sem, sums, over_dp, cut, all_in, dp_in, own_sum, mp_in, sems, mp_sems, part, acc, *rest,
):
    line = Line(count, part, hidden_grad, *rest)
    me, group = line.me, line.group
    span = own_sum.shape[0]
    blocks = cut.shape[0]
    columns = triple.shape[1]

    def copy_to(src, dst, out, into, to):
        return pltpu.make_async_remote_copy(
            src_ref=src, dst_ref=dst, send_sem=out, recv_sem=into, device_id=to, device_id_type=MESH
        )

    def load(k):
        rows = block(k, BLOCK)
        return pltpu.make_async_copy(
            triple_hbm.at[rows, pl.ds(0, columns)], triple.at[rows], load_sem.at[k]
        )

    for k in range(triple.shape[0] // BLOCK):
        load(k).start()

    chips, depth = mine.shape[0], mine.shape[1]
    parity, chip = lax.rem(group, 2), group // 2
    partner = group + 1 - 2 * parity

    def rows_of(owner):
        return pl.ds(pl.multiple_of(owner * depth, depth), depth)

    def mine_copy(q):
        return pltpu.make_async_copy(first_hbm.at[rows_of(2 * q + parity)], mine.at[q], pair_sems.at[0, q])

    def half_copy(q):
        src = first_hbm.at[rows_of(2 * q + 1 - parity)]
        return copy_to(src, theirs.at[q], pair_sems.at[1, q], pair_sems.at[2, q], (partner, me))

    def chip_copy(away):
        to = lax.rem(chip + away, chips)
        return copy_to(
            mine.at[to], others.at[away], chip_sems.at[0, away], chip_sems.at[1, away], (2 * to + parity, me)
        )

    def add_half(away):
        q = lax.rem(chip + away, chips)
        mine_copy(q).wait()
        half_copy(q).wait_recv()

        @pl.loop(0, depth // 64)
        def _(k):
            rows = block(k, 64)
            mine[q, rows, :] = (mine[q, rows, :].astype(F32) + theirs[q, rows, :].astype(F32)).astype(BF16)

    def send_chip(away):
        add_half(away)
        chip_copy(away).start()

    def add_chips():
        add_half(0)

        @pl.loop(1, chips)
        def _(away):
            chip_copy(away).wait_recv()

        @pl.loop(0, depth // 64)
        def _(k):
            rows = block(k, 64)
            first_out[rows, :] = mine[chip, rows, :].astype(F32)

            @pl.loop(1, chips)
            def _(away):
                first_out[rows, :] += others[away, rows, :].astype(F32)

    greet_all(groups, count)

    @pl.loop(0, chips)
    def _(q):
        mine_copy(q).start()
        half_copy(q).start()

    sums[0:2, :] = jnp.zeros_like(sums[0:2, :])
    sums[2:6, :] = feed_sums[0:4, :]
    sums[6:8, :] = jnp.zeros_like(sums[6:8, :])
    lane = lax.broadcasted_iota(jnp.int32, (1, 128), 1)
    squares = jnp.zeros((1, 128), F32)
    for k, row in enumerate((back_sums[0:1, :], front_sums[0:1, :], back_sums[1:2, :])):
        squares = jnp.where(lane == k, jnp.sum(row, axis=1, keepdims=True), squares)
    tokens = jnp.sum(valid[...], axis=0, keepdims=True)
    squares = jnp.where(lane == 3, tokens, squares)
    over_dp[...] = jnp.zeros_like(over_dp)
    wide = column_sums.shape[1] // 128
    for k in range(wide):
        over_dp[k : k + 1, :] = column_sums[:, 128 * k : 128 * (k + 1)]
    for k in range(unit_grad.shape[1] // 128):
        over_dp[wide + k : wide + k + 1, :] = unit_grad[:, 128 * k : 128 * (k + 1)]

    def dp_copy(away):
        to = lax.rem(group + away, groups)
        return copy_to(over_dp, dp_in.at[away], sems.at[0, away], sems.at[1, away], (to, me))

    def block_copy(away):
        to = lax.rem(group + away, groups)
        src = cut.at[pl.ds(to * blocks // groups, span)]
        return copy_to(src, all_in.at[away], sems.at[2, away], sems.at[3, away], (to, me))

    def mp_copy(away):
        to = lax.rem(me + away, count)
        return copy_to(own_sum, mp_in.at[away], mp_sems.at[0, away], mp_sems.at[1, away], (group, to))

    @pl.loop(1, groups)
    def _(away):
        dp_copy(away).start()

    def send_blocks():
        for k in range(blocks):
            cut[k] = sums[:, 128 * k : 128 * (k + 1)]
            cut[k, 6:7, :] = squares

        @pl.loop(1, groups)
        def _(away):
            block_copy(away).start()

    def add_blocks():
        own_sum[...] = cut[pl.ds(group * blocks // groups, span)]

        @pl.loop(1, groups)
        def _(away):
            block_copy(away).wait_recv()
            own_sum[...] = own_sum[...] + all_in[away]

        @pl.loop(1, count)
        def _(away):
            mp_copy(away).start()

    def add_rest():
        dp_out[...] = over_dp[...]

        @pl.loop(1, groups)
        def _(away):
            dp_copy(away).wait_recv()
            dp_out[...] = dp_out[...] + dp_in[away]

        all_out[...] = own_sum[...]

        @pl.loop(1, count)
        def _(away):
            mp_copy(away).wait_recv()
            all_out[...] = all_out[...] + mp_in[away]

    def finish(piece):
        line.total(piece, acc)
        rows = line.own(piece)
        grad_in = acc[...]
        normed, rate = norm_parts(own[rows, :].astype(F32))
        result = residual_grad[rows, :] + norm_back(grad_in, vectors[0:1, :], normed, rate)
        line.share(piece, result.astype(BF16))
        sums[0:1, :] += jnp.sum(grad_in * normed, axis=0, keepdims=True)
        sums[1:2, :] += jnp.sum(grad_in, axis=0, keepdims=True)

    tiles = tiles_of(part.shape[0])

    def product(start, size, c):
        if start == 0:
            load(c // BLOCK).wait()
        part[pl.ds(start, size), c : c + BLOCK] = dot_nt(
            triple_grad[pl.ds(start, size), :], triple[c : c + BLOCK, :]
        ).astype(BF16)

    def work(start, size):
        return [functools.partial(product, start, size, c) for c in range(0, part.shape[1], BLOCK)]

    for closure in work(*tiles[0]):
        closure()
    later = [work(*tile) for tile in tiles[1:]] + [[]]
    sends = [[] for _ in tiles]
    if chips <= 8:
        for away in range(1, chips):
            sends[0].append(functools.partial(send_chip, away))
    else:

        def send_chips():
            pl.loop(1, chips)(send_chip)

        sends[0].append(send_chips)
    later = [one + two for one, two in zip(later, sends)]
    steps = ticks(count, line.pieces)
    done = LAG * (count - 1) - 1
    drain = [[] for _ in range(steps - line.pieces)]
    drain[done].append(send_blocks)
    drain[done + 2 * LAG].append(add_blocks)
    paced(lambda step: tick(line, step, finish), tiles, steps, later, drain)
    add_rest()
    add_chips()

    @pl.loop(0, line.pieces)
    def _(piece):
        line.settle(piece)

    @pl.loop(0, chips)
    def _(q):
        half_copy(q).wait_send()

    @pl.loop(1, chips)
    def _(away):
        chip_copy(away).wait_send()

    @pl.loop(1, groups)
    def _(away):
        dp_copy(away).wait_send()
        block_copy(away).wait_send()

    @pl.loop(1, count)
    def _(away):
        mp_copy(away).wait_send()


def last_call(groups, count, whole, variant, triple_grad, weights, own, residual_grad, sums, valid, column_sums, unit_grad, vectors, first_grad):
    rows, columns = triple_grad.shape
    width = weights.shape[0]
    apart = (-(-(columns + unit_grad.shape[1]) // 1024) * 8, 128)
    pieces = rows // PIECE
    blocks = width // 128
    span = max(1, blocks // groups)
    chips, depth = groups // 2, width // groups
    return pl.pallas_call(
        functools.partial(last_kernel, groups, count),
        name="last_line",
        out_shape=(
            jax.ShapeDtypeStruct((whole, width), BF16),
            jax.ShapeDtypeStruct((span, 8, 128), F32),
            jax.ShapeDtypeStruct(apart, F32),
            jax.ShapeDtypeStruct((depth, first_grad.shape[1]), F32),
        ),
        in_specs=[VMEM, ANY] + [VMEM] * 9 + [ANY],
        out_specs=(ANY, VMEM, VMEM, VMEM),
        scratch_shapes=[
            *[pltpu.VMEM((chips, depth, first_grad.shape[1]), BF16)] * 3,
            pltpu.SemaphoreType.DMA((3, chips)),
            pltpu.SemaphoreType.DMA((2, chips)),
            pltpu.VMEM((width, columns), BF16),
            pltpu.SemaphoreType.DMA((width // BLOCK,)),
            pltpu.VMEM((8, width), F32),
            pltpu.VMEM(apart, F32),
            pltpu.VMEM((blocks, 8, 128), F32),
            pltpu.VMEM((groups, span, 8, 128), F32),
            pltpu.VMEM((groups, *apart), F32),
            pltpu.VMEM((span, 8, 128), F32),
            pltpu.VMEM((count, span, 8, 128), F32),
            pltpu.SemaphoreType.DMA((4, groups)),
            pltpu.SemaphoreType.DMA((2, count)),
            pltpu.VMEM((rows, width), BF16),
            pltpu.VMEM((PIECE // count, width), F32),
            *Line.scratch(count, pieces, width),
        ],
        compiler_params=params(5, variant),
        cost_estimate=cost(115),
    )(triple_grad, weights, own, residual_grad, *sums, valid, column_sums, unit_grad, vectors, first_grad)


def close_kernel(reduce_hbm, expand_hbm, first_hbm, *rest):
    reduce_out, expand_out, triple_out, merge_out = rest[:4]
    reduce, expand, first, reduce_wide, expand_wide, triple, merge, into, out = rest[4:]

    def copy(src, dst, sem):
        return pltpu.make_async_copy(src, dst, sem)

    ins = [
        copy(reduce_hbm, reduce, into.at[0]),
        copy(expand_hbm, expand, into.at[1]),
        copy(first_hbm, first, into.at[2]),
    ]
    outs = [
        copy(reduce_wide, reduce_out, out.at[0]),
        copy(expand_wide, expand_out, out.at[1]),
        copy(triple, triple_out, out.at[2]),
        copy(merge, merge_out, out.at[3]),
    ]
    for one in ins:
        one.start()

    def widen(src, dst):
        step = 64

        @pl.loop(0, src.shape[0] // step)
        def _(k):
            part = block(k, step)
            dst[part, :] = src[part, :].astype(F32)

    ins[0].wait()
    widen(reduce, reduce_wide)
    outs[0].start()
    ins[1].wait()
    widen(expand, expand_wide)
    outs[1].start()
    ins[2].wait()
    wide = triple.shape[2]
    for k in range(3):
        triple[k] = first[:, k * wide : (k + 1) * wide]
    outs[2].start()
    merge[...] = first[:, 3 * wide :].T
    outs[3].start()
    for one in outs:
        one.wait()


def close_call(reduce_grad, expand_grad, first_grad):
    block_rows, columns = first_grad.shape
    wide = columns // 4
    shapes = [reduce_grad.shape, expand_grad.shape, (3, block_rows, wide), (wide, block_rows)]
    ins = (reduce_grad, expand_grad, first_grad)
    return pl.pallas_call(
        close_kernel,
        name="close",
        out_shape=tuple(jax.ShapeDtypeStruct(shape, F32) for shape in shapes),
        in_specs=[ANY] * 3,
        out_specs=(ANY,) * 4,
        scratch_shapes=[
            *[pltpu.VMEM(array.shape, array.dtype) for array in ins],
            *[pltpu.VMEM(shape, F32) for shape in shapes],
            pltpu.SemaphoreType.DMA((3,)),
            pltpu.SemaphoreType.DMA((4,)),
        ],
        compiler_params=pltpu.CompilerParams(vmem_limit_bytes=63 << 20),
        cost_estimate=cost(6),
    )(*ins)


def unpack_kernel(facts, *rest):
    sources, (held, into, out) = rest[:6], rest[6:]
    packed, swapped, results = sources[0:2], sources[2:4], sources[4:6]
    slots = results[0].shape[0] // SLOT

    def fetch_own(array, slot):
        source = packed[array].at[pl.ds(pl.multiple_of(facts[slot], 16), SLOT)]
        return pltpu.make_async_copy(source, held.at[array, pl.ds(slot * SLOT, SLOT)], into.at[array, slot])

    def fetch_other(array, slot):
        target = held.at[array, pl.ds(slot * SLOT, SLOT)]
        return pltpu.make_async_copy(swapped[array], target, into.at[array, slot])

    def store(array, slot):
        rows = pl.ds(slot * SLOT, SLOT)
        return pltpu.make_async_copy(held.at[array, rows], results[array].at[rows], out.at[array, slot])

    every = [(array, slot) for array in range(2) for slot in range(slots)]
    for array, slot in every:
        @pl.when(facts[slots + slot] == 0)
        def _(array=array, slot=slot):
            fetch_own(array, slot).start()

        @pl.when(facts[slots + slot] != 0)
        def _(array=array, slot=slot):
            fetch_other(array, slot).start()

    for array, slot in every:
        fetch_other(array, slot).wait()
        length = facts[2 * slots + slot]

        @pl.loop(0, SLOT // 64)
        def _(k):
            rows = pl.ds(pl.multiple_of(slot * SLOT + k * 64, 64), 64)
            place = lax.broadcasted_iota(jnp.int32, (64, held.shape[2]), 0) + k * 64
            values = held[array, rows, :].astype(F32)
            held[array, rows, :] = jnp.where(place < length, values, 0.0).astype(BF16)

        store(array, slot).start()
    for array, slot in every:
        store(array, slot).wait()


def unpack_call(facts, packed, swapped):
    rows, width = packed[0].shape
    slots = rows // SLOT
    return pl.pallas_call(
        unpack_kernel,
        name="unpack",
        out_shape=(jax.ShapeDtypeStruct((rows, width), BF16),) * 2,
        in_specs=[SMEM] + [ANY] * 4,
        out_specs=(ANY,) * 2,
        scratch_shapes=[
            pltpu.VMEM((2, rows, width), BF16),
            pltpu.SemaphoreType.DMA((2, slots)),
            pltpu.SemaphoreType.DMA((2, slots)),
        ],
        compiler_params=pltpu.CompilerParams(vmem_limit_bytes=63 << 20),
        cost_estimate=cost(6),
    )(facts, *packed, *swapped)


SIZES = (768, 832, 896, 960)


def make_local(groups, count):
    def local(
        hidden,
        cotangent,
        lengths,
        input_gain,
        input_shift,
        triple_weight,
        triple_bias,
        merge_weight,
        merge_bias,
        middle_gain,
        middle_shift,
        expand_weight,
        expand_bias,
        reduce_weight,
        reduce_bias,
    ):
        rows, width = hidden.shape
        slots = rows // SLOT
        head_cols = triple_weight.shape[2]
        units = expand_weight.shape[1]
        local_heads = head_cols // HEAD_DIM
        me, group = lax.axis_index("mp"), lax.axis_index("dp")
        share = width // groups
        slopes = 2.0 ** (
            -8.0
            * (me * local_heads + jnp.arange(local_heads, dtype=jnp.int32) + 1).astype(F32)
            / HEADS
        )
        bias_pair = triple_bias.astype(F32)
        first = jnp.concatenate([triple_weight.reshape(-1, 3 * head_cols), merge_weight.T], axis=1)
        by_rows = Layout(major_to_minor=(0, 1))
        first = with_layout_constraint(first, by_rows)
        first_full = with_layout_constraint(lax.all_gather(first, "dp", axis=0, tiled=True), by_rows)
        parts = jnp.stack([lengths // 16, lax.rem(lengths, 16)]).reshape(-1)
        parts = jnp.pad(parts, (0, share - 2 * slots)).astype(BF16)
        vectors = jnp.stack(
            [input_gain, input_shift, merge_bias, middle_gain, middle_shift, reduce_bias, parts]
        )
        vectors = lax.all_gather(vectors, "dp", axis=1, tiled=True).astype(F32)
        table = vectors[6].reshape(groups, share)[:, : 2 * slots].astype(jnp.int32)
        table = 16 * table[:, :slots] + table[:, slots:]
        vectors = jnp.pad(vectors, ((0, 1), (0, 0)))

        whole = -(-table // 16) * 16
        if slots == 2 and groups % 2 == 0:
            left, right = whole[0::2], whole[1::2]
            sums = jnp.stack(
                [
                    jnp.maximum(left[:, 0] + left[:, 1], right[:, 0] + right[:, 1]),
                    jnp.maximum(left[:, 0] + right[:, 0], left[:, 1] + right[:, 1]),
                    jnp.maximum(left[:, 0] + right[:, 1], left[:, 1] + right[:, 0]),
                ]
            )
            needed = jnp.max(jnp.min(sums, axis=0))
            choice = jnp.argmin(sums[:, group // 2]).astype(jnp.int32)
            odd = lax.rem(group, 2)
            given = jnp.where((odd == 1) & (choice == 1), 0, 1)
            taken = jnp.where((odd == 0) & (choice == 1), 0, 1)
            swaps = choice > 0
            partners = [(k, k + 1 - 2 * (k % 2)) for k in range(groups)]

            def trade(array):
                return lax.ppermute(array, "dp", partners)

            other_length = table[group + 1 - 2 * odd, taken]
            changed = [swaps & (given == k) for k in range(slots)]
            now = [jnp.where(changed[k], other_length, lengths[k]) for k in range(slots)]

            def enter(array):
                mine = lax.dynamic_slice_in_dim(array, given * SLOT, SLOT, axis=0)
                came = trade(mine)
                return [
                    jnp.where(changed[k], came, array[k * SLOT : (k + 1) * SLOT]) for k in range(slots)
                ]

        else:
            needed = jnp.max(jnp.sum(whole, axis=1))
            changed = [jnp.zeros((), bool)] * slots
            given = jnp.zeros((), jnp.int32)
            now = [lengths[k] for k in range(slots)]

            def trade(array):
                return array

            def enter(array):
                return [array[k * SLOT : (k + 1) * SLOT] for k in range(slots)]

        starts = [jnp.zeros((), jnp.int32)]
        for k in range(slots - 1):
            starts.append(starts[-1] + -(-now[k] // 16) * 16)
        seats = jnp.arange(rows, dtype=jnp.int32)
        segment = sum((seats >= starts[k]).astype(jnp.int32) for k in range(1, slots))
        first_seat = sum(jnp.where(segment == k, starts[k], 0) for k in range(slots))
        length_at = sum(jnp.where(segment == k, now[k], 0) for k in range(slots))
        places = seats - first_seat
        valid = places < length_at

        def pack(pieces):
            packed = jnp.concatenate(pieces, axis=0)
            for k in range(1, slots):
                packed = lax.dynamic_update_slice_in_dim(packed, pieces[k], starts[k], axis=0)
            return packed

        def own_rows(array):
            split = array.reshape(rows // PIECE, count, PIECE // count, -1)
            mine = lax.dynamic_index_in_dim(split, me, axis=1, keepdims=False)
            return mine.reshape(rows // count, -1)

        tokens = pack(enter(hidden))
        grad_feed = jnp.where(valid[:, None], pack(enter(cotangent)), jnp.zeros((), BF16))
        own = own_rows(tokens)
        own_valid = own_rows(valid.astype(F32)[:, None])
        own_grad = own_rows(grad_feed)
        normed, _ = norm_parts(tokens.astype(F32))
        norm_in = (normed * vectors[0] + vectors[1]).astype(BF16)
        as_key = jnp.where(valid, segment, -1)
        as_query = jnp.where(valid, segment, -2)
        spots = places.astype(F32)
        segments = (
            as_query[:, None],
            as_key[None, :],
            spots[None, :],
            as_query[None, :],
            as_key[:, None],
            spots[:, None],
        )
        shift = jnp.concatenate([bias_pair[0], jnp.zeros_like(bias_pair[0]), bias_pair[1]])[None]
        unit_shift = expand_bias.astype(F32)[None]

        def scatter(array, dim):
            return lax.psum_scatter(array, "dp", scatter_dimension=dim, tiled=True)

        def layer(variant, size):
            expand_full = lax.all_gather(expand_weight, "dp", axis=0, tiled=True)
            reduce_full = lax.all_gather(reduce_weight, "dp", axis=1, tiled=True)
            norm_mid, residual, sums_one, qkv, mixed, totals = front_call(
                count, size, variant, slopes, norm_in, first_full, shift, own, own_valid, segments, vectors
            )
            branch_grad, residual_grad, sums_two, unit_grad, feed_part, expand_grad, reduce_grad = feed_call(
                count,
                variant,
                norm_mid,
                expand_full,
                reduce_full,
                grad_feed,
                residual,
                own_grad,
                unit_shift,
                vectors,
            )
            reduce_grad = scatter(reduce_grad, 1)
            expand_grad = scatter(expand_grad, 0)
            grad_triple, column_sums, output, sums_three, first_grad = back_call(
                count,
                rows,
                variant,
                slopes,
                branch_grad,
                first_full,
                qkv,
                mixed,
                norm_in,
                totals,
                segments,
                feed_part,
                residual,
                own_valid,
                vectors,
            )
            hidden_grad, small, dp_small, first_grad = last_call(
                groups,
                count,
                rows,
                variant,
                grad_triple,
                first_full,
                own,
                residual_grad,
                (sums_one, sums_two, sums_three),
                own_valid,
                column_sums,
                unit_grad,
                vectors,
                first_grad,
            )
            return lax.optimization_barrier(
                (output, hidden_grad, small, dp_small, reduce_grad, expand_grad, first_grad)
            )

        sizes = [size for size in SIZES if size < rows] + [rows]

        def branch(variant, size):
            def run():
                return layer(variant, size)

            return run

        index = sum((needed > size).astype(jnp.int32) for size in sizes[:-1])
        output, hidden_grad, small, dp_small, reduce_grad, expand_grad, first_grad = lax.switch(
            index, [branch(k, size) for k, size in enumerate(sizes)]
        )
        at = sum(jnp.where(given == k, starts[k], 0) for k in range(slots))
        swapped = [
            trade(lax.dynamic_slice_in_dim(array, at, SLOT, axis=0)) for array in (output, hidden_grad)
        ]
        facts = jnp.stack([*starts, *[one.astype(jnp.int32) for one in changed], *lengths])
        reduce_grad, expand_grad, triple_grad, merge_grad = close_call(reduce_grad, expand_grad, first_grad)
        output, hidden_grad = unpack_call(facts, (output, hidden_grad), swapped)
        small = small.transpose(1, 0, 2).reshape(8, -1)
        totals = small[6, :4]
        if share < 128:
            place = lax.rem(group * share, 128)
            small = lax.dynamic_slice_in_dim(small, place, share, axis=1)
        flat = dp_small.reshape(-1)
        triple_sums = flat[: 3 * head_cols]
        unit_sums = flat[3 * head_cols : 3 * head_cols + units]
        root_means = jnp.sqrt(totals[:3] / (totals[3] * width))
        pair_grad = jnp.stack([triple_sums[:head_cols], triple_sums[2 * head_cols :]])
        return (
            output,
            hidden_grad,
            small[0],
            small[1],
            triple_grad.transpose(1, 0, 2),
            pair_grad,
            merge_grad,
            small[2],
            small[3],
            small[4],
            expand_grad,
            unit_sums,
            reduce_grad,
            small[5],
            root_means,
        )

    return local


def solution(mesh):
    return jax.shard_map(
        make_local(mesh.shape["dp"], mesh.shape["mp"]),
        mesh=mesh,
        in_specs=(
            P("dp", None),
            P("dp", None),
            P("dp"),
            P("dp"),
            P("dp"),
            P("dp", None, "mp"),
            P(None, "mp"),
            P("mp", "dp"),
            P("dp"),
            P("dp"),
            P("dp"),
            P("dp", "mp"),
            P("mp"),
            P("mp", "dp"),
            P("dp"),
        ),
        out_specs=(
            P("dp", None),
            P("dp", None),
            P("dp"),
            P("dp"),
            P("dp", None, "mp"),
            P(None, "mp"),
            P("mp", "dp"),
            P("dp"),
            P("dp"),
            P("dp"),
            P("dp", "mp"),
            P("mp"),
            P("mp", "dp"),
            P("dp"),
            P(),
        ),
        check_vma=False,
    )
```

```python
import functools

import jax
import jax.numpy as jnp
from jax import lax
from jax.experimental import pallas as pl
from jax.experimental.layout import Layout, with_layout_constraint
from jax.experimental.pallas import tpu as pltpu
from jax.sharding import PartitionSpec as P

HEADS = 32
HEAD_DIM = 64
SLOT = 512
PIECE = 64
TILE = 256
BLOCK = 512
F32 = jnp.float32
BF16 = jnp.bfloat16
MESH = pl.DeviceIdType.MESH
VMEM = pl.BlockSpec(memory_space=pltpu.VMEM)
ANY = pl.BlockSpec(memory_space=pl.ANY)


def dot32(a, b):
    return jnp.dot(a, b, preferred_element_type=F32)


def dot_nt(a, b):
    return lax.dot_general(a, b, (((1,), (1,)), ((), ())), preferred_element_type=F32)


def dot_tn(a, b):
    return lax.dot_general(a, b, (((0,), (0,)), ((), ())), preferred_element_type=F32)


def norm_parts(values):
    center = values - jnp.mean(values, axis=-1, keepdims=True)
    spread = jnp.mean(center * center, axis=-1, keepdims=True)
    rate = lax.rsqrt(spread + 1e-05)
    return center * rate, rate


def norm_back(grad, gain, normed, rate):
    scaled = grad * gain
    first = jnp.mean(scaled, axis=-1, keepdims=True)
    second = jnp.mean(scaled * normed, axis=-1, keepdims=True)
    return rate * (scaled - first - normed * second)


def block(index, size):
    return pl.ds(pl.multiple_of(index * size, size), size)


def greet(count):
    me, group = lax.axis_index("mp"), lax.axis_index("dp")
    barrier = pltpu.get_barrier_semaphore()

    @pl.when(me < count - 1)
    def _():
        pl.semaphore_signal(barrier, inc=1, device_id=(group, me + 1), device_id_type=MESH)

    @pl.when(me > 0)
    def _():
        pl.semaphore_signal(barrier, inc=1, device_id=(group, me - 1), device_id_type=MESH)

    peers = jnp.where(me > 0, 1, 0) + jnp.where(me < count - 1, 1, 0)
    pl.semaphore_wait(barrier, peers)


LAG = 1


class Line:
    def __init__(self, count, part, result, inbox, extra, *sems):
        self.count, self.part, self.inbox, self.extra, self.result = count, part, inbox, extra, result
        self.pieces = part.shape[0] // PIECE
        self.sum_out, self.sum_in, self.extra_in, self.own_out, self.all_out, self.all_in, self.flushed = sems
        self.rows = PIECE // count
        self.me, self.group = lax.axis_index("mp"), lax.axis_index("dp")

    @staticmethod
    def scratch(count, pieces, width):
        rows = PIECE // count
        return [
            pltpu.VMEM((pieces * PIECE, width), BF16),
            pltpu.VMEM((pieces * rows, width), BF16),
            pltpu.SemaphoreType.DMA((pieces, count)),
            pltpu.SemaphoreType.DMA((pieces, count)),
            pltpu.SemaphoreType.DMA((pieces,)),
            pltpu.SemaphoreType.DMA((pieces,)),
            pltpu.SemaphoreType.DMA((pieces, count)),
            pltpu.SemaphoreType.DMA((pieces, count)),
            pltpu.SemaphoreType.DMA((pieces,)),
        ]

    def at(self, piece, owner):
        return pl.ds(pl.multiple_of(piece * PIECE + owner * self.rows, self.rows), self.rows)

    def own(self, piece):
        return block(piece, self.rows)

    def copy(self, src, dst, out, into, to):
        return pltpu.make_async_remote_copy(
            src_ref=src,
            dst_ref=dst,
            send_sem=out,
            recv_sem=into,
            device_id=(self.group, to),
            device_id_type=MESH,
        )

    def sum_copy(self, piece, owner, to):
        rows = self.at(piece, owner)
        return self.copy(
            self.part.at[rows],
            self.inbox.at[rows],
            self.sum_out.at[piece, owner],
            self.sum_in.at[piece, owner],
            to,
        )

    def extra_copy(self, piece, owner, to):
        return self.copy(
            self.part.at[self.at(piece, owner)],
            self.extra.at[self.own(piece)],
            self.sum_out.at[piece, owner],
            self.extra_in.at[piece],
            to,
        )

    def all_copy(self, piece, owner, to, own_left=False):
        rows = self.at(piece, owner)
        return self.copy(
            self.inbox.at[rows],
            self.inbox.at[rows],
            self.own_out.at[piece] if own_left else self.all_out.at[piece, owner],
            self.all_in.at[piece, owner],
            to,
        )

    def add(self, piece, owner):
        rows = self.at(piece, owner)
        self.sum_copy(piece, owner, self.me).wait_recv()
        self.part[rows, :] = (
            self.part[rows, :].astype(F32) + self.inbox[rows, :].astype(F32)
        ).astype(BF16)

    def send_right(self, piece):
        me, last = self.me, self.count - 1
        for owner in range(last, 0, -1):

            @pl.when(me < owner)
            def _(owner=owner):
                @pl.when(me > 0)
                def _():
                    self.add(piece, owner)

                self.sum_copy(piece, owner, me + 1).start()

    def send_left(self, piece):
        me, last = self.me, self.count - 1
        for owner in range(last):

            @pl.when(me > owner)
            def _(owner=owner):
                @pl.when(me < last)
                def _():
                    self.add(piece, owner)

                @pl.when(me == owner + 1)
                def _():
                    self.extra_copy(piece, owner, me - 1).start()

                @pl.when(me > owner + 1)
                def _():
                    self.sum_copy(piece, owner, me - 1).start()

    def total(self, piece, acc):
        me, rows = self.me, self.at(piece, self.me)
        acc[...] = self.part[rows, :].astype(F32)

        @pl.when(me > 0)
        def _():
            self.sum_copy(piece, me, me).wait_recv()
            acc[...] = acc[...] + self.inbox[rows, :].astype(F32)

        @pl.when(me < self.count - 1)
        def _():
            self.extra_copy(piece, me, me).wait_recv()
            acc[...] = acc[...] + self.extra[self.own(piece), :].astype(F32)

    def share(self, piece, values):
        me = self.me
        self.inbox[self.at(piece, me), :] = values

        @pl.when(me < self.count - 1)
        def _():
            self.all_copy(piece, me, me + 1).start()

        @pl.when(me > 0)
        def _():
            self.all_copy(piece, me, me - 1, own_left=True).start()

    def forward(self, piece, away):
        me, last = self.me, self.count - 1

        @pl.when(me >= away)
        def _(owner=me - away):
            self.all_copy(piece, owner, me).wait_recv()

            @pl.when(me < last)
            def _():
                self.all_copy(piece, owner, me + 1).start()

        @pl.when(me + away <= last)
        def _(owner=me + away):
            self.all_copy(piece, owner, me).wait_recv()

            @pl.when(me > 0)
            def _():
                self.all_copy(piece, owner, me - 1).start()

    def flush_copy(self, piece):
        rows = block(piece, PIECE)
        return pltpu.make_async_copy(self.inbox.at[rows], self.result.at[rows], self.flushed.at[piece])

    def flush(self, piece):
        self.flush_copy(piece).start()

    def settle(self, piece):
        me, last = self.me, self.count - 1
        self.flush_copy(piece).wait()
        for owner in range(self.count):

            @pl.when(me != owner)
            def _():
                self.sum_copy(piece, owner, me).wait_send()

            @pl.when(jnp.logical_or(jnp.logical_and(me >= owner, me < last), jnp.logical_and(me < owner, me > 0)))
            def _():
                self.all_copy(piece, owner, me).wait_send()

        @pl.when(me > 0)
        def _():
            self.all_copy(piece, me, me, own_left=True).wait_send()


def tick(line, step, finish):
    def when(piece, work, *more):
        @pl.when(jnp.logical_and(piece >= 0, piece < line.pieces))
        def _():
            work(piece, *more)

    last = line.count - 1
    when(step - LAG * line.me, line.send_right)
    when(step - LAG * (last - line.me), line.send_left)
    when(step - LAG * last, finish)
    for away in range(1, line.count):
        when(step - LAG * (last + away), line.forward, away)
    when(step - LAG * 2 * last, line.flush)


def ticks(count, pieces):
    return pieces + 2 * LAG * (count - 1)


def cost(micros):
    return pl.CostEstimate(flops=int(micros * 1e9), bytes_accessed=1 << 20, transcendentals=0)


def params(index, variant):
    return pltpu.CompilerParams(
        collective_id=8 * variant + index, has_side_effects=True, vmem_limit_bytes=63 << 20
    )


def tiles_of(rows):
    return [(start, min(TILE, rows - start)) for start in range(0, rows, TILE)]


def spread(work, parts):
    return [work[len(work) * k // parts : len(work) * (k + 1) // parts] for k in range(parts)]


def paced(line_tick, tiles, steps, later, drain):
    step = 0
    spans = [size // PIECE for _, size in tiles]
    plans = [work if callable(work) else spread(work, span) for work, span in zip(later, spans)]
    spans.append(steps - sum(spans))
    assert len(later) == len(tiles) and (callable(drain) or len(drain) == spans[-1])
    for span, shares in zip(spans, (*plans, drain)):

        @pl.loop(0, span)
        def _(k, step=step, span=span, shares=shares):
            line_tick(step + k)
            if callable(shares):
                shares(k, span)
            else:
                for phase, share in enumerate(shares):
                    if share:

                        @pl.when(k == phase)
                        def _(share=share):
                            for closure in share:
                                closure()

        step += span


def stepped(opening, each, amount, closing):
    def work(k, span):
        per = -(-amount // span)

        @pl.when(k == 0)
        def _():
            for closure in opening:
                closure()

        pl.loop(jnp.minimum(k * per, amount), jnp.minimum((k + 1) * per, amount))(each)

        @pl.when(k == span - 1)
        def _():
            for closure in closing:
                closure()

    return work


def halves(values):
    low = lax.broadcasted_iota(jnp.int32, values.shape, 1) < HEAD_DIM
    zero = jnp.zeros((), values.dtype)
    return jnp.where(low, values, zero), jnp.where(low, zero, values)


PAIR = 2 * HEAD_DIM


def front_kernel(
    count, head_cols, slopes, norm_hbm, weights_hbm, shift, own, valid, segment_col, segment_row, place_row, vectors,
    middle, residual, sums, qkv_hbm, mixed_hbm, totals,
    norm_in, weights, qkv, mixed, load_sem, save_sem, part, acc, mask, *rest,
):
    line = Line(count, part, middle, *rest)
    rows_all, width = norm_in.shape
    tiles = tiles_of(rows_all)
    blocks = weights.shape[1] // BLOCK

    def load_rows(k):
        rows = pl.ds(tiles[k][0], tiles[k][1])
        return pltpu.make_async_copy(norm_hbm.at[rows], norm_in.at[rows], load_sem.at[0, k])

    def load_columns(k):
        cols = block(k, BLOCK)
        return pltpu.make_async_copy(weights_hbm.at[:, cols], weights.at[:, cols], load_sem.at[1, k])

    load_rows(0).start()
    for k in range(blocks):
        load_columns(k).start()
    for k in range(1, len(tiles)):
        load_rows(k).start()
    greet(count)
    sums[...] = jnp.zeros_like(sums)

    def finish(piece):
        line.total(piece, acc)
        rows = line.own(piece)
        branch = acc[...] + vectors[2:3, :]
        result = own[rows, :].astype(F32) + branch
        residual[rows, :] = result
        normed, _ = norm_parts(result)
        line.share(piece, (normed * vectors[3:4, :] + vectors[4:5, :]).astype(BF16))
        sums[0:1, :] += jnp.sum(branch * branch * valid[rows, :], axis=0, keepdims=True)

    def project(start, size):
        rows = pl.ds(start, size)
        load_rows(start // TILE).wait()

        @pl.loop(0, 3 * head_cols // BLOCK)
        def _(k):
            cols = block(k, BLOCK)
            if start == 0:
                load_columns(k).wait()
            qkv[rows, cols] = (dot32(norm_in[rows, :], weights[:, cols]) + shift[:, cols]).astype(BF16)

    def masks(start, size):
        keys = start + size
        row = lax.broadcasted_iota(jnp.int32, (size, keys), 0) + start
        col = lax.broadcasted_iota(jnp.int32, (size, keys), 1)
        same = segment_col[start : start + size, :] == segment_row[:, :keys]
        mask[:size, :keys] = jnp.where(jnp.logical_and(same, col <= row), 1.0, 0.0)

    def attend(start, size, pair):
        keys = start + size
        query = halves(qkv[pl.ds(start, size), block(pair, PAIR)])
        key = qkv[:keys, pl.ds(pl.multiple_of(head_cols + pair * PAIR, PAIR), PAIR)]
        value = halves(qkv[:keys, pl.ds(pl.multiple_of(2 * head_cols + pair * PAIR, PAIR), PAIR)])
        out = jnp.zeros((size, PAIR), F32)
        sums_log = jnp.zeros((size, 128), F32)
        lane = lax.broadcasted_iota(jnp.int32, (size, 128), 1)
        for k in range(2):
            scores = dot_nt(query[k], key) + slopes[2 * pair + k] * place_row[:, :keys]
            scores = jnp.where(mask[:size, :keys] > 0.5, scores * 0.125, -1000000000.0)
            most = jnp.max(scores, axis=1, keepdims=True)
            raised = jnp.exp(scores - most)
            total = jnp.sum(raised, axis=1, keepdims=True)
            out = out + dot32((raised * (1.0 / total)).astype(BF16), value[k])
            sums_log = jnp.where(lane == k, most + jnp.log(total), sums_log)
        totals[pair, :, start : start + size] = sums_log.T[:2, :]
        mixed[pl.ds(start, size), block(pair, PAIR)] = out.astype(BF16)

    def project_back(start, size):
        rows = pl.ds(start, size)
        if start == 0:
            for k in range(3 * head_cols // BLOCK, blocks):
                load_columns(k).wait()

        @pl.loop(0, width // BLOCK)
        def _(k):
            cols = block(k, BLOCK)
            part[rows, cols] = dot_nt(mixed[rows, :], weights[cols, 3 * head_cols :]).astype(BF16)

    pairs = head_cols // PAIR

    def work(start, size, *more):
        return stepped(
            [functools.partial(project, start, size), functools.partial(masks, start, size)],
            functools.partial(attend, start, size),
            pairs,
            [functools.partial(project_back, start, size), *more],
        )

    saves = (
        pltpu.make_async_copy(qkv, qkv_hbm, save_sem.at[0]),
        pltpu.make_async_copy(mixed, mixed_hbm, save_sem.at[1]),
    )

    def save():
        for copy in saves:
            copy.start()

    project(*tiles[0])
    masks(*tiles[0])
    pl.loop(0, pairs)(functools.partial(attend, *tiles[0]))
    project_back(*tiles[0])
    later = [work(*tile) for tile in tiles[1:]] + [[save]]
    steps = ticks(count, line.pieces)
    drain = [[]] * (steps - line.pieces)
    paced(lambda step: tick(line, step, finish), tiles, steps, later, drain)
    for copy in saves:
        copy.wait()

    @pl.loop(0, line.pieces)
    def _(piece):
        line.settle(piece)


SMEM = pl.BlockSpec(memory_space=pltpu.SMEM)


def front_call(count, rows, variant, slopes, norm_in, weights, shift, own, valid, segments, vectors):
    width = norm_in.shape[1]
    head_cols = weights.shape[1] // 4
    pieces = rows // PIECE
    return pl.pallas_call(
        functools.partial(front_kernel, count, head_cols),
        name="front_line",
        out_shape=(
            jax.ShapeDtypeStruct((rows, width), BF16),
            jax.ShapeDtypeStruct((rows // count, width), F32),
            jax.ShapeDtypeStruct((8, width), F32),
            jax.ShapeDtypeStruct((rows, 3 * head_cols), BF16),
            jax.ShapeDtypeStruct((rows, head_cols), BF16),
            jax.ShapeDtypeStruct((head_cols // PAIR, 2, rows), F32),
        ),
        in_specs=[SMEM] + [ANY] * 2 + [VMEM] * 7,
        out_specs=(ANY, VMEM, VMEM, ANY, ANY, VMEM),
        scratch_shapes=[
            pltpu.VMEM((rows, width), BF16),
            pltpu.VMEM(weights.shape, BF16),
            pltpu.VMEM((rows, 3 * head_cols), BF16),
            pltpu.VMEM((rows, head_cols), BF16),
            pltpu.SemaphoreType.DMA((2, max(len(tiles_of(rows)), weights.shape[1] // BLOCK))),
            pltpu.SemaphoreType.DMA((2,)),
            pltpu.VMEM((rows, width), BF16),
            pltpu.VMEM((PIECE // count, width), F32),
            pltpu.VMEM((TILE, rows), F32),
            *Line.scratch(count, pieces, width),
        ],
        compiler_params=params(1, variant),
        cost_estimate=cost(120),
    )(slopes, norm_in, weights, shift, own, valid, *segments[:3], vectors)


def feed_kernel(
    count, pieces, middle_hbm, expand_hbm, reduce_hbm, grad_hbm, residual, own_grad, unit_shift, vectors,
    branch_grad, residual_grad, sums, unit_grad, feed_hbm, expand_grad, reduce_grad,
    middle, expand, reduce, grad, active, pre_grad, part, acc, stage, feed_stage, load_sem, stage_sem, feed_sem, *rest,
):
    line = Line(count, part, branch_grad, *rest)
    units = expand.shape[1]
    width = expand.shape[0]
    blocks = units // BLOCK

    def load(k):
        cols = block(k, BLOCK)
        return (
            pltpu.make_async_copy(expand_hbm.at[:, cols], expand.at[:, cols], load_sem.at[0, k]),
            pltpu.make_async_copy(reduce_hbm.at[cols], reduce.at[cols], load_sem.at[1, k]),
        )

    tiles = tiles_of(middle.shape[0])

    def load_rows(k):
        rows = pl.ds(tiles[k][0], tiles[k][1])
        return (
            pltpu.make_async_copy(middle_hbm.at[rows], middle.at[rows], load_sem.at[2, k]),
            pltpu.make_async_copy(grad_hbm.at[rows], grad.at[rows], load_sem.at[3, k]),
        )

    for copy in (*load_rows(0), *load(0)):
        copy.start()
    for k in range(1, blocks):
        for copy in load(k):
            copy.start()
    for k in range(1, len(tiles)):
        for copy in load_rows(k):
            copy.start()
    greet(count)
    sums[...] = jnp.zeros_like(sums)
    unit_grad[...] = jnp.zeros_like(unit_grad)

    def finish(piece):
        line.total(piece, acc)
        rows = line.own(piece)
        grad_mid = acc[...]
        normed, rate = norm_parts(residual[rows, :])
        grad_out = own_grad[rows, :].astype(F32)
        result = grad_out + norm_back(grad_mid, vectors[3:4, :], normed, rate)
        residual_grad[rows, :] = result
        low = result.astype(BF16)
        line.share(piece, low)
        for k, values in enumerate((low.astype(F32), grad_mid * normed, grad_mid, grad_out)):
            sums[k : k + 1, :] += jnp.sum(values, axis=0, keepdims=True)

    def forward(start, size, k):
        rows, cols = pl.ds(start, size), block(k, BLOCK)
        if start == 0:
            for copy in load(k):
                copy.wait()
        pre = dot32(middle[rows, :], expand[:, cols]) + unit_shift[:, cols]
        half = 0.5 + 0.5 * lax.erf(pre * 0.7071067811865476)
        slope = half + pre * (0.3989422804014327 * jnp.exp(-0.5 * pre * pre))
        active[rows, cols] = (pre * half).astype(BF16)
        low = (dot_nt(grad[rows, :], reduce[cols, :]) * slope).astype(BF16)
        pre_grad[rows, cols] = low
        unit_grad[:, cols] += jnp.sum(low.astype(F32), axis=0, keepdims=True)

    def backward(start, size, k):
        rows, cols = pl.ds(start, size), block(k, BLOCK)
        part[rows, cols] = dot_nt(pre_grad[rows, :], expand[cols, :]).astype(BF16)

    backs = width // BLOCK

    def unit(start, size, k):
        @pl.when(k < blocks)
        def _():
            forward(start, size, k)

        @pl.when(k >= blocks)
        def _():
            backward(start, size, k - blocks)

    staged = {"rows": 0}

    def settle_slot(slot):
        rows = pl.ds(0, staged["rows"])
        pltpu.make_async_copy(
            feed_stage.at[slot, rows], feed_hbm.at[rows, pl.ds(0, BLOCK)], feed_sem.at[slot]
        ).wait()

    def feed_product(start, size):
        before = staged["rows"]
        rows = pl.ds(start, size)

        @pl.loop(0, backs)
        def _(k):
            slot, cols = lax.rem(k, 4), block(k, BLOCK)
            if before:
                settle_slot(slot)
            feed_stage[slot, :size, :] = dot32(active[rows, :], reduce[:, cols]).astype(BF16)
            pltpu.make_async_copy(
                feed_stage.at[slot, pl.ds(0, size)], feed_hbm.at[rows, cols], feed_sem.at[slot]
            ).start()

        staged["rows"] = size

    def put(slot, target):
        return pltpu.make_async_copy(stage.at[slot], target, stage_sem.at[slot])

    def product(u):
        def emit(target, start, columns, value):
            @pl.loop(0, columns // BLOCK)
            def _(k):
                slot, cols = lax.rem(k, 4), block(k, BLOCK)

                @pl.when(u > 0)
                def _():
                    put(slot, target.at[pl.ds(0, BLOCK), pl.ds(0, BLOCK)]).wait()

                stage[slot] = value(cols).astype(BF16)
                put(slot, target.at[start, cols]).start()

        @pl.when(u < blocks)
        def _():
            rows = block(u, BLOCK)
            emit(reduce_grad, rows, width, lambda cols: dot_tn(active[:, rows], grad[:, cols]))

        @pl.when(u >= blocks)
        def _():
            rows = block(u - blocks, BLOCK)
            emit(expand_grad, rows, units, lambda cols: dot_tn(middle[:, rows], pre_grad[:, cols]))

    assert backs == 4 and blocks == 4

    def arrive(start):
        for copy in load_rows(start // TILE):
            copy.wait()

    arrive(0)
    pl.loop(0, blocks + backs)(functools.partial(unit, *tiles[0]))
    later = [
        stepped(
            [functools.partial(arrive, after[0])],
            functools.partial(unit, *after),
            blocks + backs,
            [functools.partial(feed_product, *tile)],
        )
        for tile, after in zip(tiles, tiles[1:])
    ]
    steps = ticks(count, pieces)
    beside = tiles[-1][1] // PIECE
    amount = blocks + backs
    taken = amount * beside // (steps - pieces + beside)
    later.append(stepped([functools.partial(feed_product, *tiles[-1])], product, taken, []))
    drain = stepped([], lambda u: product(u + taken), amount - taken, [])
    paced(lambda step: tick(line, step, finish), tiles, steps, later, drain)
    for slot in range(4):
        put(slot, expand_grad.at[pl.ds(0, BLOCK), pl.ds(0, BLOCK)]).wait()
    for slot in range(4):
        settle_slot(slot)

    @pl.loop(0, pieces)
    def _(piece):
        line.settle(piece)


def feed_call(count, variant, middle, expand, reduce, grad, residual, own_grad, unit_shift, vectors):
    rows, width = middle.shape
    units = expand.shape[1]
    pieces = rows // PIECE
    most = max(units // BLOCK, len(tiles_of(rows)))
    return pl.pallas_call(
        functools.partial(feed_kernel, count, pieces),
        name="feed_line",
        out_shape=(
            jax.ShapeDtypeStruct((rows, width), BF16),
            jax.ShapeDtypeStruct((rows // count, width), F32),
            jax.ShapeDtypeStruct((8, width), F32),
            jax.ShapeDtypeStruct((1, units), F32),
            jax.ShapeDtypeStruct((rows, width), BF16),
            jax.ShapeDtypeStruct((width, units), BF16),
            jax.ShapeDtypeStruct((units, width), BF16),
        ),
        in_specs=[ANY] * 4 + [VMEM] * 4,
        out_specs=(ANY,) + (VMEM,) * 3 + (ANY,) * 3,
        scratch_shapes=[
            pltpu.VMEM((rows, width), BF16),
            pltpu.VMEM((width, units), BF16),
            pltpu.VMEM((units, width), BF16),
            pltpu.VMEM((rows, width), BF16),
            pltpu.VMEM((rows, units), BF16),
            pltpu.VMEM((rows, units), BF16),
            pltpu.VMEM((rows, width), BF16),
            pltpu.VMEM((PIECE // count, width), F32),
            pltpu.VMEM((4, BLOCK, BLOCK), BF16),
            pltpu.VMEM((4, TILE, BLOCK), BF16),
            pltpu.SemaphoreType.DMA((4, most)),
            pltpu.SemaphoreType.DMA((4,)),
            pltpu.SemaphoreType.DMA((4,)),
            *Line.scratch(count, pieces, width),
        ],
        compiler_params=params(2, variant),
        cost_estimate=cost(130),
    )(middle, expand, reduce, grad, residual, own_grad, unit_shift, vectors)


def back_kernel(
    count, head_cols, slopes, branch_hbm, merge, qkv, mixed, norm_hbm, totals, segment_col, segment_row, place_col,
    feed_hbm, residual_hbm, valid, vectors,
    triple_grad, column_sums, output, sums, weight_out,
    branch_grad, norm_in, feed, residual, load_sem, save_sem,
    mixed_grad, key_grad, value_grad, acc, mask, stage, stage_sem, *rest,
):
    line = Line(count, feed, output, *rest)
    rows_all, width = branch_grad.shape
    tiles = tiles_of(rows_all)

    def load_feed(k):
        rows = pl.ds(tiles[k][0], tiles[k][1])
        return pltpu.make_async_copy(feed_hbm.at[rows], feed.at[rows], load_sem.at[0, k])

    def load_grad(k):
        rows = pl.ds(tiles[k][0], tiles[k][1])
        return pltpu.make_async_copy(branch_hbm.at[rows], branch_grad.at[rows], load_sem.at[1, k])

    load_residual = pltpu.make_async_copy(residual_hbm, residual, load_sem.at[2, 0])
    load_norm = pltpu.make_async_copy(norm_hbm.at[pl.ds(0, rows_all)], norm_in, load_sem.at[2, 1])
    load_feed(0).start()
    load_grad(len(tiles) - 1).start()
    load_residual.start()
    for k in range(1, len(tiles)):
        load_feed(k).start()
        load_grad(len(tiles) - 1 - k).start()
    load_norm.start()
    greet(count)
    load_feed(0).wait()
    load_residual.wait()
    sums[...] = jnp.zeros_like(sums)
    column_sums[...] = jnp.zeros_like(column_sums)

    def finish(piece):
        line.total(piece, acc)
        rows = line.own(piece)
        branch = acc[...] + vectors[5:6, :]
        keep = valid[rows, :] > 0.5
        result = jnp.where(keep, residual[rows, :] + branch, 0.0)
        line.share(piece, result.astype(BF16))
        branch = jnp.where(keep, branch, 0.0)
        sums[0:1, :] += jnp.sum(result * result, axis=0, keepdims=True)
        sums[1:2, :] += jnp.sum(branch * branch, axis=0, keepdims=True)

    def open_tile(start, size):
        rows = pl.ds(start, size)
        load_grad(start // TILE).wait()
        mixed_grad[rows, :] = dot32(branch_grad[rows, :], merge[...]).astype(BF16)
        keys = start + size
        row = lax.broadcasted_iota(jnp.int32, (keys, size), 1) + start
        col = lax.broadcasted_iota(jnp.int32, (keys, size), 0)
        same = segment_row[:keys, :] == segment_col[:, start : start + size]
        mask[:keys, :size] = jnp.where(jnp.logical_and(same, col <= row), 1.0, 0.0)

    def back(start, size, first, pair):
        keys = start + size
        rows, cols = pl.ds(start, size), block(pair, PAIR)
        query = halves(qkv[rows, cols])
        key = qkv[:keys, pl.ds(pl.multiple_of(head_cols + pair * PAIR, PAIR), PAIR)]
        value = qkv[:keys, pl.ds(pl.multiple_of(2 * head_cols + pair * PAIR, PAIR), PAIR)]
        grad = halves(mixed_grad[rows, cols])
        keys_apart = halves(key)
        query_grad = jnp.zeros((size, PAIR), F32)
        key_sum = jnp.zeros((keys, PAIR), F32)
        value_sum = jnp.zeros((keys, PAIR), F32)
        for k in range(2):
            scores = dot_nt(key, query[k]) + slopes[2 * pair + k] * place_col[:keys, :]
            scores = jnp.where(mask[:keys, :size] > 0.5, scores * 0.125, -1000000000.0)
            soft = jnp.exp(scores - totals[pair, k : k + 1, rows])
            grad_probs = dot_nt(value, grad[k])
            row_terms = jnp.sum(soft * grad_probs, axis=0, keepdims=True)
            grad_scores = (soft * (grad_probs - row_terms)).astype(BF16)
            value_sum = value_sum + dot32(soft.astype(BF16), grad[k])
            key_sum = key_sum + dot32(grad_scores, query[k])
            query_grad = query_grad + dot_tn(grad_scores, keys_apart[k])
        triple_grad[rows, cols] = (0.125 * query_grad).astype(BF16)
        if first:
            key_grad[:keys, cols] = key_sum
            value_grad[:keys, cols] = value_sum
        else:
            key_grad[:keys, cols] += key_sum
            value_grad[:keys, cols] += value_sum

    def close_tile(start, size):
        rows = pl.ds(start, size)
        triple_grad[rows, head_cols : 2 * head_cols] = (0.125 * key_grad[rows, :]).astype(BF16)
        triple_grad[rows, 2 * head_cols :] = value_grad[rows, :].astype(BF16)
        column_sums[...] += jnp.sum(triple_grad[rows, :].astype(F32), axis=0, keepdims=True)

    def put(slot, target):
        return pltpu.make_async_copy(stage.at[slot], target, stage_sem.at[slot])

    def job(index, left, right, r, c, shift):
        slot = index % 2
        r, c, to = pl.ds(r, BLOCK), pl.ds(c, BLOCK), pl.ds(c + shift, BLOCK)
        if index >= 2:
            put(slot, weight_out.at[r, to]).wait()
        stage[slot] = dot_tn(left[:, r], right[:, c]).astype(BF16)
        put(slot, weight_out.at[r, to]).start()

    pairs = head_cols // PAIR

    def work(start, size, first, *more):
        return stepped(
            [functools.partial(open_tile, start, size)],
            functools.partial(back, start, size, first),
            pairs,
            [functools.partial(close_tile, start, size), *more],
        )

    products = [
        (branch_grad, mixed, r, c, 3 * head_cols)
        for r in range(0, width, BLOCK)
        for c in range(0, head_cols, BLOCK)
    ] + [
        (norm_in, triple_grad, r, c, 0)
        for r in range(0, width, BLOCK)
        for c in range(0, 3 * head_cols, BLOCK)
    ]
    jobs = [functools.partial(job, k, *product) for k, product in enumerate(products)]
    waits = [load_feed(k).wait for k in range(1, len(tiles))] + [load_norm.wait]
    later = [work(*tile, k == 0, wait) for k, (tile, wait) in enumerate(zip(reversed(tiles), waits))]
    steps = ticks(count, line.pieces)
    drain = spread(jobs, steps - line.pieces)
    paced(lambda step: tick(line, step, finish), tiles, steps, later, drain)
    for slot in range(2):
        put(slot, weight_out.at[pl.ds(0, BLOCK), pl.ds(0, BLOCK)]).wait()

    @pl.loop(0, line.pieces)
    def _(piece):
        line.settle(piece)


def back_call(count, whole, variant, slopes, branch_grad, weights, qkv, mixed, norm_in, totals, segments, feed, residual, valid, vectors):
    rows, width = branch_grad.shape
    head_cols = weights.shape[1] // 4
    merge_spec = pl.BlockSpec((width, head_cols), lambda i: (0, 3), memory_space=pltpu.VMEM)
    pieces = rows // PIECE
    return pl.pallas_call(
        functools.partial(back_kernel, count, head_cols),
        name="back_line",
        out_shape=(
            jax.ShapeDtypeStruct((rows, 3 * head_cols), BF16),
            jax.ShapeDtypeStruct((1, 3 * head_cols), F32),
            jax.ShapeDtypeStruct((whole, width), BF16),
            jax.ShapeDtypeStruct((8, width), F32),
            jax.ShapeDtypeStruct((width, 4 * head_cols), BF16),
        ),
        grid=(1,),
        in_specs=[SMEM, ANY, merge_spec, VMEM, VMEM, ANY] + [VMEM] * 4 + [ANY] * 2 + [VMEM] * 2,
        out_specs=(VMEM, VMEM, ANY, VMEM, ANY),
        scratch_shapes=[
            pltpu.VMEM((rows, width), BF16),
            pltpu.VMEM((rows, width), BF16),
            pltpu.VMEM((rows, width), BF16),
            pltpu.VMEM((rows // count, width), F32),
            pltpu.SemaphoreType.DMA((3, max(2, len(tiles_of(rows))))),
            pltpu.SemaphoreType.DMA((2,)),
            pltpu.VMEM((rows, head_cols), BF16),
            pltpu.VMEM((rows, head_cols), F32),
            pltpu.VMEM((rows, head_cols), F32),
            pltpu.VMEM((PIECE // count, width), F32),
            pltpu.VMEM((rows, TILE), F32),
            pltpu.VMEM((2, BLOCK, BLOCK), BF16),
            pltpu.SemaphoreType.DMA((2,)),
            *Line.scratch(count, pieces, width),
        ],
        compiler_params=params(3, variant),
        cost_estimate=cost(120),
    )(slopes, branch_grad, weights, qkv, mixed, norm_in, totals, *segments[3:], feed, residual, valid, vectors)


def greet_all(groups, count):
    me, group = lax.axis_index("mp"), lax.axis_index("dp")
    barrier = pltpu.get_barrier_semaphore()

    @pl.loop(1, groups)
    def _(away):
        to = lax.rem(group + away, groups)
        pl.semaphore_signal(barrier, inc=1, device_id=(to, me), device_id_type=MESH)

    @pl.loop(1, count)
    def _(away):
        to = lax.rem(me + away, count)
        pl.semaphore_signal(barrier, inc=1, device_id=(group, to), device_id_type=MESH)

    pl.semaphore_wait(barrier, groups + count - 2)


def last_kernel(
    groups, count, triple_grad, triple_hbm, own, residual_grad, front_sums, feed_sums, back_sums, valid,
    column_sums, unit_grad, vectors, first_hbm,
    hidden_grad, all_out, dp_out, first_out,
    mine, theirs, others, pair_sems, chip_sems,
    triple, load_sem, sums, over_dp, cut, all_in, dp_in, own_sum, mp_in, sems, mp_sems, part, acc, *rest,
):
    line = Line(count, part, hidden_grad, *rest)
    me, group = line.me, line.group
    span = own_sum.shape[0]
    blocks = cut.shape[0]
    columns = triple.shape[1]

    def copy_to(src, dst, out, into, to):
        return pltpu.make_async_remote_copy(
            src_ref=src, dst_ref=dst, send_sem=out, recv_sem=into, device_id=to, device_id_type=MESH
        )

    def load(k):
        rows = block(k, BLOCK)
        return pltpu.make_async_copy(
            triple_hbm.at[rows, pl.ds(0, columns)], triple.at[rows], load_sem.at[k]
        )

    for k in range(triple.shape[0] // BLOCK):
        load(k).start()

    chips, depth = mine.shape[0], mine.shape[1]
    parity, chip = lax.rem(group, 2), group // 2
    partner = group + 1 - 2 * parity

    def rows_of(owner):
        return pl.ds(pl.multiple_of(owner * depth, depth), depth)

    def mine_copy(q):
        return pltpu.make_async_copy(first_hbm.at[rows_of(2 * q + parity)], mine.at[q], pair_sems.at[0, q])

    def half_copy(q):
        src = first_hbm.at[rows_of(2 * q + 1 - parity)]
        return copy_to(src, theirs.at[q], pair_sems.at[1, q], pair_sems.at[2, q], (partner, me))

    def chip_copy(away):
        to = lax.rem(chip + away, chips)
        return copy_to(
            mine.at[to], others.at[away], chip_sems.at[0, away], chip_sems.at[1, away], (2 * to + parity, me)
        )

    def add_half(away):
        q = lax.rem(chip + away, chips)
        mine_copy(q).wait()
        half_copy(q).wait_recv()

        @pl.loop(0, depth // 64)
        def _(k):
            rows = block(k, 64)
            mine[q, rows, :] = (mine[q, rows, :].astype(F32) + theirs[q, rows, :].astype(F32)).astype(BF16)

    def send_chip(away):
        add_half(away)
        chip_copy(away).start()

    def add_chips():
        add_half(0)

        @pl.loop(1, chips)
        def _(away):
            chip_copy(away).wait_recv()

        @pl.loop(0, depth // 64)
        def _(k):
            rows = block(k, 64)
            first_out[rows, :] = mine[chip, rows, :].astype(F32)

            @pl.loop(1, chips)
            def _(away):
                first_out[rows, :] += others[away, rows, :].astype(F32)

    greet_all(groups, count)

    @pl.loop(0, chips)
    def _(q):
        mine_copy(q).start()
        half_copy(q).start()

    sums[0:2, :] = jnp.zeros_like(sums[0:2, :])
    sums[2:6, :] = feed_sums[0:4, :]
    sums[6:8, :] = jnp.zeros_like(sums[6:8, :])
    lane = lax.broadcasted_iota(jnp.int32, (1, 128), 1)
    squares = jnp.zeros((1, 128), F32)
    for k, row in enumerate((back_sums[0:1, :], front_sums[0:1, :], back_sums[1:2, :])):
        squares = jnp.where(lane == k, jnp.sum(row, axis=1, keepdims=True), squares)
    tokens = jnp.sum(valid[...], axis=0, keepdims=True)
    squares = jnp.where(lane == 3, tokens, squares)
    over_dp[...] = jnp.zeros_like(over_dp)
    wide = column_sums.shape[1] // 128
    for k in range(wide):
        over_dp[k : k + 1, :] = column_sums[:, 128 * k : 128 * (k + 1)]
    for k in range(unit_grad.shape[1] // 128):
        over_dp[wide + k : wide + k + 1, :] = unit_grad[:, 128 * k : 128 * (k + 1)]

    def dp_copy(away):
        to = lax.rem(group + away, groups)
        return copy_to(over_dp, dp_in.at[away], sems.at[0, away], sems.at[1, away], (to, me))

    def block_copy(away):
        to = lax.rem(group + away, groups)
        src = cut.at[pl.ds(to * blocks // groups, span)]
        return copy_to(src, all_in.at[away], sems.at[2, away], sems.at[3, away], (to, me))

    def mp_copy(away):
        to = lax.rem(me + away, count)
        return copy_to(own_sum, mp_in.at[away], mp_sems.at[0, away], mp_sems.at[1, away], (group, to))

    @pl.loop(1, groups)
    def _(away):
        dp_copy(away).start()

    def send_blocks():
        for k in range(blocks):
            cut[k] = sums[:, 128 * k : 128 * (k + 1)]
            cut[k, 6:7, :] = squares

        @pl.loop(1, groups)
        def _(away):
            block_copy(away).start()

    def add_blocks():
        own_sum[...] = cut[pl.ds(group * blocks // groups, span)]

        @pl.loop(1, groups)
        def _(away):
            block_copy(away).wait_recv()
            own_sum[...] = own_sum[...] + all_in[away]

        @pl.loop(1, count)
        def _(away):
            mp_copy(away).start()

    def add_rest():
        dp_out[...] = over_dp[...]

        @pl.loop(1, groups)
        def _(away):
            dp_copy(away).wait_recv()
            dp_out[...] = dp_out[...] + dp_in[away]

        all_out[...] = own_sum[...]

        @pl.loop(1, count)
        def _(away):
            mp_copy(away).wait_recv()
            all_out[...] = all_out[...] + mp_in[away]

    def finish(piece):
        line.total(piece, acc)
        rows = line.own(piece)
        grad_in = acc[...]
        normed, rate = norm_parts(own[rows, :].astype(F32))
        result = residual_grad[rows, :] + norm_back(grad_in, vectors[0:1, :], normed, rate)
        line.share(piece, result.astype(BF16))
        sums[0:1, :] += jnp.sum(grad_in * normed, axis=0, keepdims=True)
        sums[1:2, :] += jnp.sum(grad_in, axis=0, keepdims=True)

    tiles = tiles_of(part.shape[0])

    def product(start, size, c):
        if start == 0:
            load(c // BLOCK).wait()
        part[pl.ds(start, size), c : c + BLOCK] = dot_nt(
            triple_grad[pl.ds(start, size), :], triple[c : c + BLOCK, :]
        ).astype(BF16)

    def work(start, size):
        return [functools.partial(product, start, size, c) for c in range(0, part.shape[1], BLOCK)]

    for closure in work(*tiles[0]):
        closure()
    later = [work(*tile) for tile in tiles[1:]] + [[]]
    sends = [[] for _ in tiles]
    if chips <= 8:
        for away in range(1, chips):
            sends[0].append(functools.partial(send_chip, away))
    else:

        def send_chips():
            pl.loop(1, chips)(send_chip)

        sends[0].append(send_chips)
    later = [one + two for one, two in zip(later, sends)]
    steps = ticks(count, line.pieces)
    done = LAG * (count - 1) - 1
    drain = [[] for _ in range(steps - line.pieces)]
    drain[done].append(send_blocks)
    drain[done + 2 * LAG].append(add_blocks)
    paced(lambda step: tick(line, step, finish), tiles, steps, later, drain)
    add_rest()
    add_chips()

    @pl.loop(0, line.pieces)
    def _(piece):
        line.settle(piece)

    @pl.loop(0, chips)
    def _(q):
        half_copy(q).wait_send()

    @pl.loop(1, chips)
    def _(away):
        chip_copy(away).wait_send()

    @pl.loop(1, groups)
    def _(away):
        dp_copy(away).wait_send()
        block_copy(away).wait_send()

    @pl.loop(1, count)
    def _(away):
        mp_copy(away).wait_send()


def last_call(groups, count, whole, variant, triple_grad, weights, own, residual_grad, sums, valid, column_sums, unit_grad, vectors, first_grad):
    rows, columns = triple_grad.shape
    width = weights.shape[0]
    apart = (-(-(columns + unit_grad.shape[1]) // 1024) * 8, 128)
    pieces = rows // PIECE
    blocks = width // 128
    span = max(1, blocks // groups)
    chips, depth = groups // 2, width // groups
    return pl.pallas_call(
        functools.partial(last_kernel, groups, count),
        name="last_line",
        out_shape=(
            jax.ShapeDtypeStruct((whole, width), BF16),
            jax.ShapeDtypeStruct((span, 8, 128), F32),
            jax.ShapeDtypeStruct(apart, F32),
            jax.ShapeDtypeStruct((depth, first_grad.shape[1]), F32),
        ),
        in_specs=[VMEM, ANY] + [VMEM] * 9 + [ANY],
        out_specs=(ANY, VMEM, VMEM, VMEM),
        scratch_shapes=[
            *[pltpu.VMEM((chips, depth, first_grad.shape[1]), BF16)] * 3,
            pltpu.SemaphoreType.DMA((3, chips)),
            pltpu.SemaphoreType.DMA((2, chips)),
            pltpu.VMEM((width, columns), BF16),
            pltpu.SemaphoreType.DMA((width // BLOCK,)),
            pltpu.VMEM((8, width), F32),
            pltpu.VMEM(apart, F32),
            pltpu.VMEM((blocks, 8, 128), F32),
            pltpu.VMEM((groups, span, 8, 128), F32),
            pltpu.VMEM((groups, *apart), F32),
            pltpu.VMEM((span, 8, 128), F32),
            pltpu.VMEM((count, span, 8, 128), F32),
            pltpu.SemaphoreType.DMA((4, groups)),
            pltpu.SemaphoreType.DMA((2, count)),
            pltpu.VMEM((rows, width), BF16),
            pltpu.VMEM((PIECE // count, width), F32),
            *Line.scratch(count, pieces, width),
        ],
        compiler_params=params(5, variant),
        cost_estimate=cost(115),
    )(triple_grad, weights, own, residual_grad, *sums, valid, column_sums, unit_grad, vectors, first_grad)


def close_kernel(reduce_hbm, expand_hbm, first_hbm, *rest):
    reduce_out, expand_out, triple_out, merge_out = rest[:4]
    reduce, expand, first, reduce_wide, expand_wide, triple, merge, into, out = rest[4:]

    def copy(src, dst, sem):
        return pltpu.make_async_copy(src, dst, sem)

    ins = [
        copy(reduce_hbm, reduce, into.at[0]),
        copy(expand_hbm, expand, into.at[1]),
        copy(first_hbm, first, into.at[2]),
    ]
    outs = [
        copy(reduce_wide, reduce_out, out.at[0]),
        copy(expand_wide, expand_out, out.at[1]),
        copy(triple, triple_out, out.at[2]),
        copy(merge, merge_out, out.at[3]),
    ]
    for one in ins:
        one.start()

    def widen(src, dst):
        step = 64

        @pl.loop(0, src.shape[0] // step)
        def _(k):
            part = block(k, step)
            dst[part, :] = src[part, :].astype(F32)

    ins[0].wait()
    widen(reduce, reduce_wide)
    outs[0].start()
    ins[1].wait()
    widen(expand, expand_wide)
    outs[1].start()
    ins[2].wait()
    wide = triple.shape[2]
    for k in range(3):
        triple[k] = first[:, k * wide : (k + 1) * wide]
    outs[2].start()
    merge[...] = first[:, 3 * wide :].T
    outs[3].start()
    for one in outs:
        one.wait()


def close_call(reduce_grad, expand_grad, first_grad):
    block_rows, columns = first_grad.shape
    wide = columns // 4
    shapes = [reduce_grad.shape, expand_grad.shape, (3, block_rows, wide), (wide, block_rows)]
    ins = (reduce_grad, expand_grad, first_grad)
    return pl.pallas_call(
        close_kernel,
        name="close",
        out_shape=tuple(jax.ShapeDtypeStruct(shape, F32) for shape in shapes),
        in_specs=[ANY] * 3,
        out_specs=(ANY,) * 4,
        scratch_shapes=[
            *[pltpu.VMEM(array.shape, array.dtype) for array in ins],
            *[pltpu.VMEM(shape, F32) for shape in shapes],
            pltpu.SemaphoreType.DMA((3,)),
            pltpu.SemaphoreType.DMA((4,)),
        ],
        compiler_params=pltpu.CompilerParams(vmem_limit_bytes=63 << 20),
        cost_estimate=cost(6),
    )(*ins)


def unpack_kernel(facts, *rest):
    sources, (held, into, out) = rest[:6], rest[6:]
    packed, swapped, results = sources[0:2], sources[2:4], sources[4:6]
    slots = results[0].shape[0] // SLOT

    def fetch_own(array, slot):
        source = packed[array].at[pl.ds(pl.multiple_of(facts[slot], 16), SLOT)]
        return pltpu.make_async_copy(source, held.at[array, pl.ds(slot * SLOT, SLOT)], into.at[array, slot])

    def fetch_other(array, slot):
        target = held.at[array, pl.ds(slot * SLOT, SLOT)]
        return pltpu.make_async_copy(swapped[array], target, into.at[array, slot])

    def store(array, slot):
        rows = pl.ds(slot * SLOT, SLOT)
        return pltpu.make_async_copy(held.at[array, rows], results[array].at[rows], out.at[array, slot])

    every = [(array, slot) for array in range(2) for slot in range(slots)]
    for array, slot in every:
        @pl.when(facts[slots + slot] == 0)
        def _(array=array, slot=slot):
            fetch_own(array, slot).start()

        @pl.when(facts[slots + slot] != 0)
        def _(array=array, slot=slot):
            fetch_other(array, slot).start()

    for array, slot in every:
        fetch_other(array, slot).wait()
        length = facts[2 * slots + slot]

        @pl.loop(0, SLOT // 64)
        def _(k):
            rows = pl.ds(pl.multiple_of(slot * SLOT + k * 64, 64), 64)
            place = lax.broadcasted_iota(jnp.int32, (64, held.shape[2]), 0) + k * 64
            values = held[array, rows, :].astype(F32)
            held[array, rows, :] = jnp.where(place < length, values, 0.0).astype(BF16)

        store(array, slot).start()
    for array, slot in every:
        store(array, slot).wait()


def unpack_call(facts, packed, swapped):
    rows, width = packed[0].shape
    slots = rows // SLOT
    return pl.pallas_call(
        unpack_kernel,
        name="unpack",
        out_shape=(jax.ShapeDtypeStruct((rows, width), BF16),) * 2,
        in_specs=[SMEM] + [ANY] * 4,
        out_specs=(ANY,) * 2,
        scratch_shapes=[
            pltpu.VMEM((2, rows, width), BF16),
            pltpu.SemaphoreType.DMA((2, slots)),
            pltpu.SemaphoreType.DMA((2, slots)),
        ],
        compiler_params=pltpu.CompilerParams(vmem_limit_bytes=63 << 20),
        cost_estimate=cost(6),
    )(facts, *packed, *swapped)


SIZES = (768, 832, 896, 960)


def make_local(groups, count):
    def local(
        hidden,
        cotangent,
        lengths,
        input_gain,
        input_shift,
        triple_weight,
        triple_bias,
        merge_weight,
        merge_bias,
        middle_gain,
        middle_shift,
        expand_weight,
        expand_bias,
        reduce_weight,
        reduce_bias,
    ):
        rows, width = hidden.shape
        slots = rows // SLOT
        head_cols = triple_weight.shape[2]
        units = expand_weight.shape[1]
        local_heads = head_cols // HEAD_DIM
        me, group = lax.axis_index("mp"), lax.axis_index("dp")
        share = width // groups
        slopes = 2.0 ** (
            -8.0
            * (me * local_heads + jnp.arange(local_heads, dtype=jnp.int32) + 1).astype(F32)
            / HEADS
        )
        bias_pair = triple_bias.astype(F32)
        first = jnp.concatenate([triple_weight.reshape(-1, 3 * head_cols), merge_weight.T], axis=1)
        by_rows = Layout(major_to_minor=(0, 1))
        first = with_layout_constraint(first, by_rows)
        first_full = with_layout_constraint(lax.all_gather(first, "dp", axis=0, tiled=True), by_rows)
        parts = jnp.stack([lengths // 16, lax.rem(lengths, 16)]).reshape(-1)
        parts = jnp.pad(parts, (0, share - 2 * slots)).astype(BF16)
        vectors = jnp.stack(
            [input_gain, input_shift, merge_bias, middle_gain, middle_shift, reduce_bias, parts]
        )
        vectors = lax.all_gather(vectors, "dp", axis=1, tiled=True).astype(F32)
        table = vectors[6].reshape(groups, share)[:, : 2 * slots].astype(jnp.int32)
        table = 16 * table[:, :slots] + table[:, slots:]
        vectors = jnp.pad(vectors, ((0, 1), (0, 0)))

        whole = -(-table // 16) * 16
        if slots == 2 and groups % 2 == 0:
            left, right = whole[0::2], whole[1::2]
            sums = jnp.stack(
                [
                    jnp.maximum(left[:, 0] + left[:, 1], right[:, 0] + right[:, 1]),
                    jnp.maximum(left[:, 0] + right[:, 0], left[:, 1] + right[:, 1]),
                    jnp.maximum(left[:, 0] + right[:, 1], left[:, 1] + right[:, 0]),
                ]
            )
            needed = jnp.max(jnp.min(sums, axis=0))
            choice = jnp.argmin(sums[:, group // 2]).astype(jnp.int32)
            odd = lax.rem(group, 2)
            given = jnp.where((odd == 1) & (choice == 1), 0, 1)
            taken = jnp.where((odd == 0) & (choice == 1), 0, 1)
            swaps = choice > 0
            partners = [(k, k + 1 - 2 * (k % 2)) for k in range(groups)]

            def trade(array):
                return lax.ppermute(array, "dp", partners)

            other_length = table[group + 1 - 2 * odd, taken]
            changed = [swaps & (given == k) for k in range(slots)]
            now = [jnp.where(changed[k], other_length, lengths[k]) for k in range(slots)]

            def enter(array):
                mine = lax.dynamic_slice_in_dim(array, given * SLOT, SLOT, axis=0)
                came = trade(mine)
                return [
                    jnp.where(changed[k], came, array[k * SLOT : (k + 1) * SLOT]) for k in range(slots)
                ]

        else:
            needed = jnp.max(jnp.sum(whole, axis=1))
            changed = [jnp.zeros((), bool)] * slots
            given = jnp.zeros((), jnp.int32)
            now = [lengths[k] for k in range(slots)]

            def trade(array):
                return array

            def enter(array):
                return [array[k * SLOT : (k + 1) * SLOT] for k in range(slots)]

        starts = [jnp.zeros((), jnp.int32)]
        for k in range(slots - 1):
            starts.append(starts[-1] + -(-now[k] // 16) * 16)
        seats = jnp.arange(rows, dtype=jnp.int32)
        segment = sum((seats >= starts[k]).astype(jnp.int32) for k in range(1, slots))
        first_seat = sum(jnp.where(segment == k, starts[k], 0) for k in range(slots))
        length_at = sum(jnp.where(segment == k, now[k], 0) for k in range(slots))
        places = seats - first_seat
        valid = places < length_at

        def pack(pieces):
            packed = jnp.concatenate(pieces, axis=0)
            for k in range(1, slots):
                packed = lax.dynamic_update_slice_in_dim(packed, pieces[k], starts[k], axis=0)
            return packed

        def own_rows(array):
            split = array.reshape(rows // PIECE, count, PIECE // count, -1)
            mine = lax.dynamic_index_in_dim(split, me, axis=1, keepdims=False)
            return mine.reshape(rows // count, -1)

        tokens = pack(enter(hidden))
        grad_feed = jnp.where(valid[:, None], pack(enter(cotangent)), jnp.zeros((), BF16))
        own = own_rows(tokens)
        own_valid = own_rows(valid.astype(F32)[:, None])
        own_grad = own_rows(grad_feed)
        normed, _ = norm_parts(tokens.astype(F32))
        norm_in = (normed * vectors[0] + vectors[1]).astype(BF16)
        as_key = jnp.where(valid, segment, -1)
        as_query = jnp.where(valid, segment, -2)
        spots = places.astype(F32)
        segments = (
            as_query[:, None],
            as_key[None, :],
            spots[None, :],
            as_query[None, :],
            as_key[:, None],
            spots[:, None],
        )
        shift = jnp.concatenate([bias_pair[0], jnp.zeros_like(bias_pair[0]), bias_pair[1]])[None]
        unit_shift = expand_bias.astype(F32)[None]

        def scatter(array, dim):
            return lax.psum_scatter(array, "dp", scatter_dimension=dim, tiled=True)

        def layer(variant, size):
            expand_full = lax.all_gather(expand_weight, "dp", axis=0, tiled=True)
            reduce_full = lax.all_gather(reduce_weight, "dp", axis=1, tiled=True)
            norm_mid, residual, sums_one, qkv, mixed, totals = front_call(
                count, size, variant, slopes, norm_in, first_full, shift, own, own_valid, segments, vectors
            )
            branch_grad, residual_grad, sums_two, unit_grad, feed_part, expand_grad, reduce_grad = feed_call(
                count,
                variant,
                norm_mid,
                expand_full,
                reduce_full,
                grad_feed,
                residual,
                own_grad,
                unit_shift,
                vectors,
            )
            reduce_grad = scatter(reduce_grad, 1)
            expand_grad = scatter(expand_grad, 0)
            grad_triple, column_sums, output, sums_three, first_grad = back_call(
                count,
                rows,
                variant,
                slopes,
                branch_grad,
                first_full,
                qkv,
                mixed,
                norm_in,
                totals,
                segments,
                feed_part,
                residual,
                own_valid,
                vectors,
            )
            hidden_grad, small, dp_small, first_grad = last_call(
                groups,
                count,
                rows,
                variant,
                grad_triple,
                first_full,
                own,
                residual_grad,
                (sums_one, sums_two, sums_three),
                own_valid,
                column_sums,
                unit_grad,
                vectors,
                first_grad,
            )
            return lax.optimization_barrier(
                (output, hidden_grad, small, dp_small, reduce_grad, expand_grad, first_grad)
            )

        sizes = [size for size in SIZES if size < rows] + [rows]

        def branch(variant, size):
            def run():
                return layer(variant, size)

            return run

        index = sum((needed > size).astype(jnp.int32) for size in sizes[:-1])
        output, hidden_grad, small, dp_small, reduce_grad, expand_grad, first_grad = lax.switch(
            index, [branch(k, size) for k, size in enumerate(sizes)]
        )
        at = sum(jnp.where(given == k, starts[k], 0) for k in range(slots))
        swapped = [
            trade(lax.dynamic_slice_in_dim(array, at, SLOT, axis=0)) for array in (output, hidden_grad)
        ]
        facts = jnp.stack([*starts, *[one.astype(jnp.int32) for one in changed], *lengths])
        reduce_grad, expand_grad, triple_grad, merge_grad = close_call(reduce_grad, expand_grad, first_grad)
        output, hidden_grad = unpack_call(facts, (output, hidden_grad), swapped)
        small = small.transpose(1, 0, 2).reshape(8, -1)
        totals = small[6, :4]
        if share < 128:
            place = lax.rem(group * share, 128)
            small = lax.dynamic_slice_in_dim(small, place, share, axis=1)
        flat = dp_small.reshape(-1)
        triple_sums = flat[: 3 * head_cols]
        unit_sums = flat[3 * head_cols : 3 * head_cols + units]
        root_means = jnp.sqrt(totals[:3] / (totals[3] * width))
        pair_grad = jnp.stack([triple_sums[:head_cols], triple_sums[2 * head_cols :]])
        return (
            output,
            hidden_grad,
            small[0],
            small[1],
            triple_grad.transpose(1, 0, 2),
            pair_grad,
            merge_grad,
            small[2],
            small[3],
            small[4],
            expand_grad,
            unit_sums,
            reduce_grad,
            small[5],
            root_means,
        )

    return local


def solution(mesh):
    return jax.shard_map(
        make_local(mesh.shape["dp"], mesh.shape["mp"]),
        mesh=mesh,
        in_specs=(
            P("dp", None),
            P("dp", None),
            P("dp"),
            P("dp"),
            P("dp"),
            P("dp", None, "mp"),
            P(None, "mp"),
            P("mp", "dp"),
            P("dp"),
            P("dp"),
            P("dp"),
            P("dp", "mp"),
            P("mp"),
            P("mp", "dp"),
            P("dp"),
        ),
        out_specs=(
            P("dp", None),
            P("dp", None),
            P("dp"),
            P("dp"),
            P("dp", None, "mp"),
            P(None, "mp"),
            P("mp", "dp"),
            P("dp"),
            P("dp"),
            P("dp"),
            P("dp", "mp"),
            P("mp"),
            P("mp", "dp"),
            P("dp"),
            P(),
        ),
        check_vma=False,
    )
```
